8 devices in a mesh: batch: 1 (over z), col: 2 (over y), row: 4 (over x, core).
Axes of the slice: x: 2, y: 2, z: 1, core: 2. Of those that a mesh axis runs over, the one named last changes fastest.
Arguments:
- lower_cyc: float32 [1536, 1536], P(('batch', 'row'), 'col')
Outputs:
- output: float32 [1536, 1536], P(('batch', 'row'), 'col')
All inputs are finite; a program needn't handle non-finite values.
Results may differ from the reference program's by a relative error of at most 0.001.
Values sent between devices are 32-bit elements.
A program may use at most 1 GiB of HBM per device.

```python
import jax
import jax.numpy as jnp
from jax import lax

N = 1536
DEPTH = 3
BLK = 8
PX = 4
PY = 2


def to_cyclic(matrix):
    blocks6 = matrix.reshape(N // (PX * BLK), PX, BLK, N // (PY * BLK), PY, BLK)
    return blocks6.transpose(1, 0, 2, 4, 3, 5).reshape(N, N)


def to_natural(cyclic):
    blocks6 = cyclic.reshape(PX, N // (PX * BLK), BLK, PY, N // (PY * BLK), BLK)
    return blocks6.transpose(1, 0, 2, 4, 3, 5).reshape(N, N)


def setup_inputs(seed: int = 0, part: int = 0) -> dict:
    base_key = jax.random.fold_in(jax.random.key(seed), part)
    key_diag, key_low = jax.random.split(base_key)
    diag_vals = jax.random.uniform(key_diag, (N,), jnp.float32, 2.0, 4.0)
    low_vals = jax.random.normal(key_low, (N, N), jnp.float32) * (2.0 / N ** 0.5)
    row_ids = jnp.arange(N)[:, None]
    col_ids = jnp.arange(N)[None, :]
    natural = jnp.where(row_ids > col_ids, low_vals, 0.0) + jnp.where(row_ids == col_ids, diag_vals[:, None], 0.0)
    return {"lower_cyc": to_cyclic(natural)}


def highest_dot(left, right):
    return jnp.dot(left, right, precision=lax.Precision.HIGHEST, preferred_element_type=jnp.float32)


def invert_block(mat_block, levels_left):
    block_size = mat_block.shape[0]
    if levels_left == 0:
        identity = jnp.eye(block_size, dtype=jnp.float32)
        return lax.linalg.triangular_solve(mat_block, identity, left_side=True, lower=True)
    half_size = block_size // 2
    inv_upper = invert_block(mat_block[:half_size, :half_size], levels_left - 1)
    inv_lower = invert_block(mat_block[half_size:, half_size:], levels_left - 1)
    temp_prod = highest_dot(mat_block[half_size:, :half_size], inv_upper)
    off_diag = -highest_dot(inv_lower, temp_prod)
    zero_block = jnp.zeros((half_size, half_size), jnp.float32)
    upper_rows = jnp.concatenate([inv_upper, zero_block], axis=1)
    lower_rows = jnp.concatenate([off_diag, inv_lower], axis=1)
    return jnp.concatenate([upper_rows, lower_rows], axis=0)


def reference(lower_cyc):
    return to_cyclic(invert_block(to_natural(lower_cyc), DEPTH))
```

```python
import jax
import jax.numpy as jnp
from jax import lax
from jax.experimental import pallas as pl
from jax.experimental.pallas import tpu as pltpu
from jax.sharding import PartitionSpec as P

MESH = pl.DeviceIdType.MESH
F32 = jnp.float32
AD, AO, BD, BO = range(4)
BLOCKS = (
    ((0, 0), (1, 1), (2, 2)),
    ((1, 0), (2, 0), (2, 1)),
    ((3, 3), (4, 4), (5, 5)),
    ((4, 3), (5, 3), (5, 4)),
)


def hdot(left, right):
    return jnp.dot(left, right, precision=lax.Precision.HIGHEST, preferred_element_type=F32)


def kernel(inp, out, gat, inv, cc, xa, tt, loc_sem, g_send, g_recv, c_send, c_recv, t_send, t_recv):
    row = lax.axis_index("row")
    y = lax.axis_index("col")
    x = row // 2
    c = row % 2
    xo, yo, co = 1 - x, 1 - y, 1 - c
    sib = {"row": 2 * x + co}
    xnb = {"row": 2 * xo + c}
    ynb = {"col": yo}

    def slot(g, sx, sc, sy, lo=0, num=8):
        return gat.at[g, sy, :, sc, pl.ds(lo, num), sx]

    local = {}
    for g in (AD, AO):
        local[g] = []
        for i, (bi, bj) in enumerate(BLOCKS[g]):
            local[g].append(pltpu.make_async_copy(
                inp.at[pl.ds(8 * bi, 8), :, pl.ds(128 * bj, 128)], gat.at[g, y, i, c, :, x], loc_sem.at[g, i]))
    local_c = [pltpu.make_async_copy(
        inp.at[pl.ds(24 + 8 * t, 8), :, pl.ds(0, 384)], cc.at[y, t], loc_sem.at[4, t]) for t in range(3)]
    for g in (BD, BO):
        local[g] = []
        for i, (bi, bj) in enumerate(BLOCKS[g]):
            local[g].append(pltpu.make_async_copy(
                inp.at[pl.ds(8 * bi, 8), :, pl.ds(128 * bj, 128)], gat.at[g, y, i, c, :, x], loc_sem.at[g, i]))
    for g in (AD, AO):
        for cp in local[g]:
            cp.start()
    for cp in local_c:
        cp.start()
    for g in (BD, BO):
        for cp in local[g]:
            cp.start()

    barrier = pltpu.get_barrier_semaphore()
    for nbr in (sib, xnb, ynb):
        pl.semaphore_signal(barrier, inc=1, device_id=nbr, device_id_type=MESH)
    pl.semaphore_wait(barrier, 3)

    sends = []

    def gsend(g, k, ref, dev):
        cp = pltpu.make_async_remote_copy(ref, ref, g_send.at[g, k], g_recv.at[g, k], device_id=dev, device_id_type=MESH)
        cp.start()
        sends.append(cp)

    def gwait(g, k, ref):
        pltpu.make_async_remote_copy(ref, ref, g_send.at[g, k], g_recv.at[g, k], device_id=sib,
                                     device_id_type=MESH).wait_recv()

    def own_x(g):
        gsend(g, 0, slot(g, x, c, y), xnb)

    def own_y(g):
        gsend(g, 1, slot(g, x, c, y), ynb)

    def own_s(g):
        gsend(g, 2, slot(g, x, c, y), sib)

    def wait_local(g):
        for cp in local[g]:
            cp.wait()

    def fwd_x(g):
        gwait(g, 0, slot(g, xo, c, y))
        gsend(g, 3, slot(g, xo, c, y, 0, 4), ynb)
        gsend(g, 5, slot(g, xo, c, y), sib)

    def fwd_y(g):
        gwait(g, 1, slot(g, x, c, yo))
        gsend(g, 4, slot(g, x, c, yo, 4, 4), xnb)
        gsend(g, 6, slot(g, x, c, yo), sib)

    def fwd_d(g):
        gwait(g, 3, slot(g, xo, c, yo, 0, 4))
        gsend(g, 7, slot(g, xo, c, yo, 0, 4), sib)
        gwait(g, 4, slot(g, xo, c, yo, 4, 4))
        gsend(g, 8, slot(g, xo, c, yo, 4, 4), sib)

    def wait_sib(g):
        gwait(g, 2, slot(g, x, co, y))
        gwait(g, 5, slot(g, xo, co, y))
        gwait(g, 6, slot(g, x, co, yo))
        gwait(g, 7, slot(g, xo, co, yo, 0, 4))
        gwait(g, 8, slot(g, xo, co, yo, 4, 4))

    def c_copy(t, q):
        return pltpu.make_async_remote_copy(cc.at[q, t], cc.at[q, t], c_send.at[t], c_recv.at[t], device_id=ynb,
                                            device_id_type=MESH)

    def send_c(t):
        local_c[t].wait()
        cp = c_copy(t, y)
        cp.start()
        sends.append(cp)

    sub = lax.broadcasted_iota(jnp.int32, (8, 128), 0)
    lane = lax.broadcasted_iota(jnp.int32, (8, 128), 1)
    seg = lane // 16

    def base(g, i, dst):
        low = [[None, None] for _ in range(4)]
        for nb in range(4):
            xr, qr = nb // 2, nb % 2
            for qc in range(2):
                acc = gat[g, qc, i, qr, 0, xr]
                for lb in range(1, 8):
                    acc = jnp.where(seg == lb, gat[g, qc, i, qr, lb, xr], acc)
                low[nb][qc] = acc
        rec = []
        for qc in range(2):
            dsum = jnp.zeros((8, 128), F32)
            for xr in range(2):
                here = (sub == lane % 8) & ((lane // 8) % 2 == xr)
                dsum = dsum + jnp.where(here, low[2 * xr + qc][qc], 0.0)
            rec.append(1.0 / jnp.sum(dsum, axis=0, keepdims=True))
        rhs = []
        for nb in range(4):
            for qc in range(2):
                low[nb][qc] = low[nb][qc] * rec[qc]
            rhs.append([jnp.where((sub == lane % 8) & ((lane // 8) % 2 == nb // 2), 1.0, 0.0) if nb % 2 == qc
                        else jnp.zeros((8, 128), F32) for qc in range(2)])
        for k in range(32):
            nk, ek = k // 8, k % 8
            xk, qk = nk // 2, nk % 2
            idx = 16 * seg + (8 * xk + ek)
            for nb in range(nk, 4):
                if nb == nk and ek == 7:
                    continue
                col = jnp.take_along_axis(low[nb][qk], idx, axis=1, mode="promise_in_bounds")
                if nb == nk:
                    col = jnp.where(sub > ek, col, 0.0)
                for qc in range(2):
                    rhs[nb][qc] = rhs[nb][qc] - col * rhs[nk][qc][ek:ek + 1, :]
        for nb in range(4):
            xr, qr = nb // 2, nb % 2
            idx = 16 * seg + 8 * xr + sub
            scale = jnp.take_along_axis(jnp.broadcast_to(rec[qr], (8, 128)), idx, axis=1, mode="promise_in_bounds")
            for qc in range(2):
                val = rhs[nb][qc] * scale
                for lb in range(8):
                    inv[dst, qc, qr, lb, xr] = jnp.where(seg == lb, val, 0.0)

    def both(ref_of):
        return jnp.concatenate([ref_of(0), ref_of(1)], axis=1)

    def inv_full(t):
        return both(lambda qc: inv[t, qc].reshape(256, 128))

    def gat_full(g, i):
        return both(lambda qc: gat[g, qc, i].reshape(256, 128))

    def double(g, w):
        first = 3 * (g // 2)
        odd = [(q, lb0) for q in range(2) for lb0 in range(w, 8, 2 * w)]
        temps = []
        for i in range(3):
            parts = []
            for q, lb0 in odd:
                rows = both(lambda qc: gat[g, qc, i, q, lb0:lb0 + w].reshape(16 * w, 128))
                col = lax.broadcasted_iota(jnp.int32, rows.shape, 1) % 128
                parts.append(jnp.where(col // (16 * w) == lb0 // w - 1, rows, 0.0))
            temps.append(hdot(jnp.concatenate(parts, axis=0), inv_full(first + i)))
        for i in range(3):
            parts = []
            full = []
            at = 0
            for q in range(2):
                for lb0 in range(0, 8, w):
                    if (lb0 // w) % 2 == 1:
                        full.append(temps[i][at:at + 16 * w])
                        at += 16 * w
                    else:
                        full.append(jnp.zeros((16 * w, 256), F32))
            for q, lb0 in odd:
                parts.append(both(lambda qc: inv[first + i, qc, q, lb0:lb0 + w].reshape(16 * w, 128)))
            left = jnp.concatenate(parts, axis=0)
            new = left - hdot(left, jnp.concatenate(full, axis=0))
            at = 0
            for q, lb0 in odd:
                piece = new[at:at + 16 * w]
                at += 16 * w
                for qc in range(2):
                    inv[first + i, qc, q, lb0:lb0 + w] = piece[:, 128 * qc:128 * qc + 128].reshape(w, 2, 8, 128)

    def diag_inverses(g):
        for i in range(3):
            base(g, i, 3 * (g // 2) + i)
        for w in (1, 2, 4):
            double(g, w)

    wait_local(AD)
    own_x(AD)
    own_y(AD)
    own_s(AD)
    wait_local(AO)
    own_x(AO)
    own_y(AO)
    own_s(AO)
    fwd_x(AD)
    fwd_y(AD)
    wait_local(BD)
    own_x(BD)
    send_c(0)
    fwd_x(AO)
    fwd_y(AO)
    wait_local(BO)
    own_x(BO)
    send_c(1)
    send_c(2)
    own_y(BD)
    own_y(BO)
    own_s(BD)
    own_s(BO)
    fwd_d(AD)
    wait_sib(AD)
    diag_inverses(AD)
    fwd_d(AO)
    wait_sib(AO)

    def inv_y(t):
        return inv[t, y].reshape(256, 128)

    x00, x11, x22 = inv_y(0), inv_y(1), inv_y(2)
    xa[0, :, 0:128] = x00
    xa[1, :, 128:256] = x11
    xa[2, :, 256:384] = x22
    x10 = -hdot(inv_full(1), hdot(gat_full(AO, 0), x00))
    xa[1, :, 0:128] = x10
    x1 = jnp.concatenate([x10, x11], axis=1)
    t20 = hdot(gat_full(AO, 2), x1)
    t20 = t20 + jnp.concatenate([hdot(gat_full(AO, 1), x00), jnp.zeros((256, 128), F32)], axis=1)
    xa[2, :, 0:256] = -hdot(inv_full(2), t20)

    def t_ref(t, sx, sc):
        return tt.at[t, sc, :, sx]

    def t_copy(k, t, sx, sc, dev):
        ref = t_ref(t, sx, sc)
        return pltpu.make_async_remote_copy(ref, ref, t_send.at[k, t], t_recv.at[k, t], device_id=dev,
                                            device_id_type=MESH)

    def t_start(k, t, sx, sc, dev):
        cp = t_copy(k, t, sx, sc, dev)
        cp.start()
        sends.append(cp)

    for t in range(3):
        c_copy(t, yo).wait_recv()
        acc = [None] * 3
        for u in range(3):
            left = both(lambda q: cc[q, t, :, :, 128 * u:128 * u + 128].reshape(64, 128))
            prod = hdot(left, xa[u, :, 0:128 * (u + 1)])
            for j in range(u + 1):
                part = prod[:, 128 * j:128 * j + 128]
                acc[j] = part if acc[j] is None else acc[j] + part
        tt[t, c, :, x] = jnp.concatenate(acc, axis=1).reshape(8, 8, 384)
        t_start(0, t, x, c, xnb)
        t_start(1, t, x, c, sib)

    fwd_x(BD)
    fwd_x(BO)
    fwd_y(BD)
    fwd_y(BO)
    fwd_d(BD)
    wait_sib(BD)
    diag_inverses(BD)
    fwd_d(BO)
    for t in range(3):
        t_copy(0, t, xo, c, sib).wait_recv()
        t_start(2, t, xo, c, sib)
    wait_sib(BO)

    def z_diag(t):
        return both(lambda qc: inv[t, qc, c, :, x].reshape(64, 128))

    z22, z33 = z_diag(4), z_diag(5)
    w10 = hdot(gat_full(BO, 0), inv_full(3))
    w20 = hdot(gat_full(BO, 1), inv_full(3))
    w21 = hdot(gat_full(BO, 2), inv_full(4))
    z10 = -hdot(z22, w10)
    v10 = -hdot(inv_full(4), w10)
    z21 = -hdot(z33, w21)
    z20 = -hdot(z33, w20 + hdot(gat_full(BO, 2), v10))
    zrow = ((z_diag(3),), (z10, z22), (z20, z21, z33))

    zero = jnp.zeros((64, 128), F32)
    xa_rows = xa.reshape(3, 2, 8, 2, 8, 384)
    for t in range(3):
        rows_a = xa_rows[t, c, :, x].reshape(64, 384)
        for j in range(3):
            out[64 * t:64 * t + 64, 128 * j:128 * j + 128] = rows_a[:, 128 * j:128 * j + 128] if j <= t else zero
            if j <= t:
                blk = zrow[t][j]
                blk = jnp.where(y == 0, blk[:, 0:128], blk[:, 128:256])
            else:
                blk = zero
            out[192 + 64 * t:256 + 64 * t, 384 + 128 * j:512 + 128 * j] = blk
        out[64 * t:64 * t + 64, 384:768] = jnp.zeros((64, 384), F32)

    acc = [None] * 3
    for t in range(3):
        t_copy(1, t, x, co, sib).wait_recv()
        t_copy(2, t, xo, co, sib).wait_recv()
        left = jnp.concatenate([zrow[s][t] for s in range(t, 3)], axis=0)
        prod = hdot(left, tt[t].reshape(256, 384))
        for s in range(t, 3):
            part = prod[64 * (s - t):64 * (s - t) + 64]
            acc[s] = part if acc[s] is None else acc[s] + part
        out[192 + 64 * t:256 + 64 * t, 0:384] = -acc[t]

    for cp in sends:
        cp.wait_send()


def solution(mesh):
    spec = P(("batch", "row"), "col")

    def body(local_l):
        rows, cols = local_l.shape
        return pl.pallas_call(
            kernel,
            out_shape=jax.ShapeDtypeStruct((rows, cols), F32),
            in_specs=[pl.BlockSpec(memory_space=pl.ANY)],
            out_specs=pl.BlockSpec(memory_space=pltpu.VMEM),
            scratch_shapes=[
                pltpu.VMEM((4, 2, 3, 2, 8, 2, 8, 128), F32),
                pltpu.VMEM((6, 2, 2, 8, 2, 8, 128), F32),
                pltpu.VMEM((2, 3, 8, 8, 384), F32),
                pltpu.VMEM((3, 256, 384), F32),
                pltpu.VMEM((3, 2, 8, 2, 8, 384), F32),
                pltpu.SemaphoreType.DMA((5, 3)),
                pltpu.SemaphoreType.DMA((4, 9)),
                pltpu.SemaphoreType.DMA((4, 9)),
                pltpu.SemaphoreType.DMA((3,)),
                pltpu.SemaphoreType.DMA((3,)),
                pltpu.SemaphoreType.DMA((3, 3)),
                pltpu.SemaphoreType.DMA((3, 3)),
            ],
            compiler_params=pltpu.CompilerParams(
                collective_id=0, has_side_effects=True, vmem_limit_bytes=40 * 1024 * 1024),
        )(local_l.reshape(rows // 8, 8, cols))

    return jax.shard_map(body, mesh=mesh, in_specs=(spec,), out_specs=spec, check_vma=False)
```

```python
import jax
import jax.numpy as jnp
from jax import lax
from jax.experimental import pallas as pl
from jax.experimental.pallas import tpu as pltpu
from jax.sharding import PartitionSpec as P

MESH = pl.DeviceIdType.MESH
F32 = jnp.float32
DIAG = ((5, 4, 3), (2, 1, 0))
OFF = (
    ((5, 4), (5, 3), (4, 3)),
    ((5, 2), (4, 2), (3, 2)),
    ((5, 1), (4, 1), (3, 1)),
    ((2, 1), (5, 0), (4, 0)),
    ((3, 0), (2, 0), (1, 0)),
)
D1, D2, O1, O2, O3, O4, O5 = range(7)
OFF_AT = {blk: 3 * g + i for g, grp in enumerate(OFF) for i, blk in enumerate(grp)}
DIAG_AT = {blk: (g, i) for g, grp in enumerate(DIAG) for i, blk in enumerate(grp)}


def hdot(left, right):
    return jnp.dot(left, right, precision=lax.Precision.HIGHEST, preferred_element_type=F32)


def kernel(inp, out, raw, dpk, dg, goff, inv, loc_sem, g_send, g_recv):
    row = lax.axis_index("row")
    y = lax.axis_index("col")
    x = row // 2
    c = row % 2
    xo, yo, co = 1 - x, 1 - y, 1 - c
    sib = {"row": 2 * x + co}
    xnb = {"row": 2 * xo + c}
    ynb = {"col": yo}

    def take(bi, bj, dst, sem):
        return pltpu.make_async_copy(inp.at[pl.ds(8 * bi, 8), :, pl.ds(128 * bj, 128)], dst, sem)

    local = {}
    for g, grp in enumerate(DIAG):
        local[g] = [take(b, b, raw.at[b], loc_sem.at[b]) for b in grp]
    for g, grp in enumerate(OFF):
        local[2 + g] = [take(bi, bj, goff.at[3 * g + i, y, c, :, x], loc_sem.at[6 + 3 * g + i])
                        for i, (bi, bj) in enumerate(grp)]
    for g in range(7):
        for cp in local[g]:
            cp.start()

    barrier = pltpu.get_barrier_semaphore()
    for nbr in (sib, xnb, ynb):
        pl.semaphore_signal(barrier, inc=1, device_id=nbr, device_id_type=MESH)

    sub = lax.broadcasted_iota(jnp.int32, (8, 128), 0)
    lane = lax.broadcasted_iota(jnp.int32, (8, 128), 1)

    def lanes(shape):
        return lax.broadcasted_iota(jnp.int32, shape, len(shape) - 1)

    def along(tile, idx):
        return jnp.take_along_axis(tile, idx, axis=1, mode="promise_in_bounds")

    def turn(tile, n):
        return along(tile, (lanes(tile.shape) + (128 - n)) & 127)

    def pack(g):
        for cp in local[g]:
            cp.wait()
        for i, b in enumerate(DIAG[g]):
            dpk[g, y, c, x, 5 * i] = raw[b, 7]
            for p in range(3):
                n = 112 - 16 * p
                dpk[g, y, c, x, 5 * i + 1 + p] = jnp.where(lane < n, raw[b, 6 - p], turn(raw[b, p], n))
            dpk[g, y, c, x, 5 * i + 4] = raw[b, 3]

    def unpack(g):
        for i in range(3):
            for qc in range(2):
                for lb in range(8):
                    if lb >= 3:
                        tiles = dpk[g, qc, :, :, 5 * i + 7 - lb]
                    else:
                        tiles = dpk[g, qc, :, :, 5 * i + 1 + lb].reshape(32, 128)
                        tiles = turn(tiles, 16 * (lb + 1)).reshape(2, 2, 8, 128)
                    dg[g, i, qc, :, lb] = tiles

    def slot(g, sx, sc, sy, half=None):
        if g < 2:
            lo, num = (0, 15) if half is None else ((0, 8), (8, 7))[half]
            return dpk.at[g, sy, sc, sx, pl.ds(lo, num)]
        lo, num = (0, 8) if half is None else (4 * half, 4)
        return goff.at[pl.ds(3 * (g - 2), 3), sy, sc, pl.ds(lo, num), sx]

    sends = []

    def gsend(g, k, ref, dev):
        cp = pltpu.make_async_remote_copy(ref, ref, g_send.at[g, k], g_recv.at[g, k], device_id=dev, device_id_type=MESH)
        cp.start()
        sends.append(cp)

    def gwait(g, k, ref):
        pltpu.make_async_remote_copy(ref, ref, g_send.at[g, k], g_recv.at[g, k], device_id=sib,
                                     device_id_type=MESH).wait_recv()

    def own(g):
        if g >= 2:
            for cp in local[g]:
                cp.wait()
        gsend(g, 0, slot(g, x, c, y), xnb)
        gsend(g, 1, slot(g, x, c, y), ynb)
        gsend(g, 2, slot(g, x, c, y), sib)

    def relay(g):
        gwait(g, 0, slot(g, xo, c, y))
        gsend(g, 3, slot(g, xo, c, y, 0), ynb)
        gsend(g, 5, slot(g, xo, c, y), sib)
        gwait(g, 1, slot(g, x, c, yo))
        gsend(g, 4, slot(g, x, c, yo, 1), xnb)
        gsend(g, 6, slot(g, x, c, yo), sib)

    def relay_diag(g):
        for h in range(2):
            gwait(g, 3 + h, slot(g, xo, c, yo, h))
            gsend(g, 7 + h, slot(g, xo, c, yo, h), sib)

    def wait_sib(g):
        gwait(g, 2, slot(g, x, co, y))
        gwait(g, 5, slot(g, xo, co, y))
        gwait(g, 6, slot(g, x, co, yo))
        gwait(g, 7, slot(g, xo, co, yo, 0))
        gwait(g, 8, slot(g, xo, co, yo, 1))

    def base(g):
        sub3 = lax.broadcasted_iota(jnp.int32, (3, 8, 128), 1)
        lane3 = lanes((3, 8, 128))
        seg3 = lane3 >> 4
        seg24 = lanes((24, 128)) & 112
        here = [(sub3 == (lane3 & 7)) & (((lane3 >> 3) & 1) == xr) for xr in range(2)]
        segs = [seg3 == lb for lb in range(8)]
        low = [[None, None] for _ in range(4)]
        for nb in range(4):
            xr, qr = nb // 2, nb % 2
            for qc in range(2):
                acc = dg[g, :, qc, qr, 0, xr]
                for lb in range(1, 8):
                    acc = jnp.where(segs[lb], dg[g, :, qc, qr, lb, xr], acc)
                low[nb][qc] = acc
        rec = []
        for qc in range(2):
            dsum = jnp.where(here[0], low[qc][qc], 0.0) + jnp.where(here[1], low[2 + qc][qc], 0.0)
            rec.append(1.0 / jnp.sum(dsum, axis=1, keepdims=True))
        rhs = []
        for nb in range(4):
            for qc in range(2):
                low[nb][qc] = (low[nb][qc] * rec[qc]).reshape(24, 128)
            rhs.append([jnp.where(here[nb // 2], 1.0, 0.0) if nb % 2 == qc else jnp.zeros((3, 8, 128), F32)
                        for qc in range(2)])
        below = [sub3 > ek for ek in range(7)]
        for k in range(32):
            nk, ek = k // 8, k % 8
            xk, qk = nk // 2, nk % 2
            idx = seg24 + (8 * xk + ek)
            pivot = [rhs[nk][qc][:, ek:ek + 1, :] for qc in range(2)]
            for nb in range(nk, 4):
                if nb == nk and ek == 7:
                    continue
                col = along(low[nb][qk], idx).reshape(3, 8, 128)
                if nb == nk:
                    col = jnp.where(below[ek], col, 0.0)
                for qc in range(2):
                    rhs[nb][qc] = rhs[nb][qc] - col * pivot[qc]
        for nb in range(4):
            xr, qr = nb // 2, nb % 2
            idx = (seg3 * 16 + 8 * xr + sub3).reshape(24, 128)
            scale = along(jnp.broadcast_to(rec[qr], (3, 8, 128)).reshape(24, 128), idx).reshape(3, 8, 128)
            for qc in range(2):
                val = rhs[nb][qc] * scale
                for lb in range(8):
                    inv[g, :, qc, qr, lb, xr] = jnp.where(segs[lb], val, 0.0)

    def both(ref_of):
        return jnp.concatenate([ref_of(0), ref_of(1)], axis=1)

    def inv_full(b):
        return both(lambda qc: inv[(*DIAG_AT[b], qc)].reshape(256, 128))

    def low_block(k, j):
        return both(lambda qc: goff[OFF_AT[k, j], qc].reshape(256, 128))

    def rows_of(tiles):
        return jnp.concatenate(tiles, axis=0)

    def double(blocks, w):
        pairs = range(4 // w)
        shape = (2, w, 2, 8, 128)
        half = lanes(shape) >> {1: 4, 2: 5, 4: 6}[w]
        even = [half == 2 * p for p in pairs]
        zero = jnp.zeros(shape, F32)
        odd_rows = [pl.ds((2 * p + 1) * w, w) for p in pairs]
        temps = []
        for b in blocks:
            at = DIAG_AT[b]

            def left(qc):
                acc = zero
                for p in pairs:
                    acc = jnp.where(even[p], dg[(*at, qc, slice(None), odd_rows[p])], acc)
                return acc.reshape(32 * w, 128)
            temps.append(hdot(both(left), inv_full(b)))
        for b, temp in zip(blocks, temps):
            at = DIAG_AT[b]

            def left(qc):
                acc = inv[(*at, qc, slice(None), odd_rows[0])]
                for p in pairs[1:]:
                    acc = acc + inv[(*at, qc, slice(None), odd_rows[p])]
                return acc.reshape(32 * w, 128)

            def right(qc):
                mine = temp[:, 128 * qc:128 * qc + 128].reshape(shape)
                parts = []
                for p in pairs:
                    parts += [zero, jnp.where(even[p], mine, 0.0)]
                return jnp.concatenate(parts, axis=1).reshape(256, 128)
            prod = -hdot(both(left), both(right))
            for qc in range(2):
                piece = prod[:, 128 * qc:128 * qc + 128].reshape(shape)
                for p in pairs:
                    ref = (*at, qc, slice(None), odd_rows[p])
                    inv[ref] = jnp.where(even[p], piece, inv[ref])

    def diag_inverses(g):
        unpack(g)
        base(g)
        for w in (1, 2, 4):
            double(DIAG[g], w)

    zst = [None] * 6

    def z_diag(j):
        return both(lambda qc: inv[(*DIAG_AT[j], qc, c, slice(None), x)].reshape(64, 128))

    def emit(i, j, blk):
        out[64 * i:64 * i + 64, 128 * j:128 * j + 128] = blk

    def add_terms(j, ks, acc):
        for k in ks:
            prod = hdot(zst[k], low_block(k, j))
            for i in range(k, 6):
                part = prod[64 * (i - k):64 * (i - k) + 64]
                acc[i] = part if acc[i] is None else acc[i] + part

    def finish(j, acc):
        emit(j, j, inv[(*DIAG_AT[j], y, c, slice(None), x)].reshape(64, 128))
        if j == 5:
            zst[5] = z_diag(5)
            return
        terms = rows_of(acc[j + 1:])
        if j == 0:
            res = -hdot(terms, inv[(*DIAG_AT[0], y)].reshape(256, 128))
            for i in range(1, 6):
                emit(i, 0, res[64 * (i - 1):64 * i])
            return
        res = -hdot(terms, inv_full(j))
        zst[j] = rows_of([z_diag(j), res])
        mine = jnp.where(y == 0, res[:, 0:128], res[:, 128:256])
        for i in range(j + 1, 6):
            emit(i, j, mine[64 * (i - j - 1):64 * (i - j)])

    pack(D1)
    pl.semaphore_wait(barrier, 3)
    own(D1)
    pack(D2)
    own(D2)
    own(O1)
    for i in range(6):
        if i < 5:
            out[64 * i:64 * i + 64, 128 * (i + 1):768] = jnp.zeros((64, 128 * (5 - i)), F32)
    relay(D1)
    own(O2)
    relay(D2)
    own(O3)
    relay(O1)
    own(O4)
    relay_diag(D1)
    wait_sib(D1)
    relay(O2)
    own(O5)
    relay_diag(D2)
    diag_inverses(D1)
    relay(O3)
    relay_diag(O1)
    wait_sib(D2)
    diag_inverses(D2)
    relay(O4)
    relay_diag(O2)
    wait_sib(O1)
    finish(5, None)
    acc = [None] * 6
    add_terms(4, (5,), acc)
    finish(4, acc)
    acc = [None] * 6
    add_terms(3, (5, 4), acc)
    finish(3, acc)
    relay(O5)
    relay_diag(O3)
    wait_sib(O2)
    acc = [None] * 6
    add_terms(2, (5, 4, 3), acc)
    finish(2, acc)
    relay_diag(O4)
    wait_sib(O3)
    acc = [None] * 6
    add_terms(1, (5, 4, 3), acc)
    relay_diag(O5)
    wait_sib(O4)
    add_terms(1, (2,), acc)
    finish(1, acc)
    acc = [None] * 6
    add_terms(0, (5, 4), acc)
    wait_sib(O5)
    add_terms(0, (3, 2, 1), acc)
    finish(0, acc)

    for cp in sends:
        cp.wait_send()


def solution(mesh):
    spec = P(("batch", "row"), "col")

    def body(local_l):
        rows, cols = local_l.shape
        return pl.pallas_call(
            kernel,
            out_shape=jax.ShapeDtypeStruct((rows, cols), F32),
            in_specs=[pl.BlockSpec(memory_space=pl.ANY)],
            out_specs=pl.BlockSpec(memory_space=pltpu.VMEM),
            scratch_shapes=[
                pltpu.VMEM((6, 8, 8, 128), F32),
                pltpu.VMEM((2, 2, 2, 2, 15, 8, 128), F32),
                pltpu.VMEM((2, 3, 2, 2, 8, 2, 8, 128), F32),
                pltpu.VMEM((15, 2, 2, 8, 2, 8, 128), F32),
                pltpu.VMEM((2, 3, 2, 2, 8, 2, 8, 128), F32),
                pltpu.SemaphoreType.DMA((21,)),
                pltpu.SemaphoreType.DMA((7, 9)),
                pltpu.SemaphoreType.DMA((7, 9)),
            ],
            compiler_params=pltpu.CompilerParams(
                collective_id=0, has_side_effects=True, vmem_limit_bytes=60 * 1024 * 1024),
        )(local_l.reshape(rows // 8, 8, cols))

    return jax.shard_map(body, mesh=mesh, in_specs=(spec,), out_specs=spec, check_vma=False)
```

```python
import jax
import jax.numpy as jnp
from jax import lax
from jax.experimental import pallas as pl
from jax.experimental.pallas import tpu as pltpu
from jax.sharding import PartitionSpec as P

MESH = pl.DeviceIdType.MESH
F32 = jnp.float32
OFF = (
    ((5, 4), (4, 3), (5, 3)),
    ((3, 2), (4, 2), (5, 2)),
    ((2, 1), (3, 1), (4, 1), (5, 1)),
    ((1, 0), (2, 0)),
    ((3, 0), (4, 0)),
    ((5, 0),),
)
DG, O1, O2, O3, O4, O5, O6 = range(7)
OFF_LIST = [blk for grp in OFF for blk in grp]
OFF_AT = {blk: n for n, blk in enumerate(OFF_LIST)}
START = [OFF_AT[grp[0]] for grp in OFF]


def hdot(left, right):
    return jnp.dot(left, right, precision=lax.Precision.HIGHEST, preferred_element_type=F32)


def kernel(inp, out, raw, dpk, dg, goff, inv, loc_sem, g_send, g_recv):
    row = lax.axis_index("row")
    y = lax.axis_index("col")
    x = row // 2
    c = row % 2
    xo, yo, co = 1 - x, 1 - y, 1 - c
    sib = {"row": 2 * x + co}
    xnb = {"row": 2 * xo + c}
    ynb = {"col": yo}

    def take(bi, bj, dst, sem):
        return pltpu.make_async_copy(inp.at[pl.ds(8 * bi, 8), :, pl.ds(128 * bj, 128)], dst, sem)

    local = [[take(b, b, raw.at[b], loc_sem.at[b]) for b in range(6)]]
    for grp in OFF:
        local.append([take(bi, bj, goff.at[OFF_AT[bi, bj], y, c, :, x], loc_sem.at[6 + OFF_AT[bi, bj]])
                      for bi, bj in grp])
    for grp in local:
        for cp in grp:
            cp.start()

    barrier = pltpu.get_barrier_semaphore()
    for nbr in (sib, xnb, ynb):
        pl.semaphore_signal(barrier, inc=1, device_id=nbr, device_id_type=MESH)

    sub = lax.broadcasted_iota(jnp.int32, (8, 128), 0)
    lane = lax.broadcasted_iota(jnp.int32, (8, 128), 1)

    def lanes(shape):
        return lax.broadcasted_iota(jnp.int32, shape, len(shape) - 1)

    def along(tile, idx):
        return jnp.take_along_axis(tile, idx, axis=1, mode="promise_in_bounds")

    def turn(tile, n):
        return along(tile, (lanes(tile.shape) + (128 - n)) & 127)

    def pack():
        for b in range(6):
            local[DG][b].wait()
            dpk[y, c, x, 5 * b] = raw[b, 7]
            for p in range(3):
                n = 112 - 16 * p
                dpk[y, c, x, 5 * b + 1 + p] = jnp.where(lane < n, raw[b, 6 - p], turn(raw[b, p], n))
            dpk[y, c, x, 5 * b + 4] = raw[b, 3]

    def unpack():
        for b in range(6):
            for qc in range(2):
                for lb in range(8):
                    if lb >= 3:
                        tiles = dpk[qc, :, :, 5 * b + 7 - lb]
                    else:
                        tiles = dpk[qc, :, :, 5 * b + 1 + lb].reshape(32, 128)
                        tiles = turn(tiles, 16 * (lb + 1)).reshape(2, 2, 8, 128)
                    dg[b, qc, :, lb] = tiles

    def slot(g, sx, sc, sy, half=None):
        if g == DG:
            lo, num = (0, 30) if half is None else (15 * half, 15)
            return dpk.at[sy, sc, sx, pl.ds(lo, num)]
        lo, num = (0, 8) if half is None else (4 * half, 4)
        return goff.at[pl.ds(START[g - 1], len(OFF[g - 1])), sy, sc, pl.ds(lo, num), sx]

    sends = []

    def gsend(g, k, ref, dev):
        cp = pltpu.make_async_remote_copy(ref, ref, g_send.at[g, k], g_recv.at[g, k], device_id=dev, device_id_type=MESH)
        cp.start()
        sends.append(cp)

    def gwait(g, k, ref):
        pltpu.make_async_remote_copy(ref, ref, g_send.at[g, k], g_recv.at[g, k], device_id=sib,
                                     device_id_type=MESH).wait_recv()

    def own(g):
        if g != DG:
            for cp in local[g]:
                cp.wait()
        gsend(g, 0, slot(g, x, c, y), xnb)
        gsend(g, 1, slot(g, x, c, y), ynb)
        gsend(g, 2, slot(g, x, c, y), sib)

    def relay(g):
        gwait(g, 0, slot(g, xo, c, y))
        gsend(g, 3, slot(g, xo, c, y, 0), ynb)
        gsend(g, 5, slot(g, xo, c, y), sib)
        gwait(g, 1, slot(g, x, c, yo))
        gsend(g, 4, slot(g, x, c, yo, 1), xnb)
        gsend(g, 6, slot(g, x, c, yo), sib)

    def relay_diag(g):
        for h in range(2):
            gwait(g, 3 + h, slot(g, xo, c, yo, h))
            gsend(g, 7 + h, slot(g, xo, c, yo, h), sib)

    def wait_sib(g):
        gwait(g, 2, slot(g, x, co, y))
        gwait(g, 5, slot(g, xo, co, y))
        gwait(g, 6, slot(g, x, co, yo))
        gwait(g, 7, slot(g, xo, co, yo, 0))
        gwait(g, 8, slot(g, xo, co, yo, 1))

    def base(at):
        sub3 = lax.broadcasted_iota(jnp.int32, (3, 8, 128), 1)
        lane3 = lanes((3, 8, 128))
        seg3 = lane3 >> 4
        seg24 = lanes((24, 128)) & 112
        here = [(sub3 == (lane3 & 7)) & (((lane3 >> 3) & 1) == xr) for xr in range(2)]
        segs = [seg3 == lb for lb in range(8)]
        low = [[None, None] for _ in range(4)]
        for nb in range(4):
            xr, qr = nb // 2, nb % 2
            for qc in range(2):
                acc = dg[at:at + 3, qc, qr, 0, xr]
                for lb in range(1, 8):
                    acc = jnp.where(segs[lb], dg[at:at + 3, qc, qr, lb, xr], acc)
                low[nb][qc] = acc
        rec = []
        for qc in range(2):
            dsum = jnp.where(here[0], low[qc][qc], 0.0) + jnp.where(here[1], low[2 + qc][qc], 0.0)
            rec.append(1.0 / jnp.sum(dsum, axis=1, keepdims=True))
        rhs = []
        for nb in range(4):
            for qc in range(2):
                low[nb][qc] = (low[nb][qc] * rec[qc]).reshape(24, 128)
            rhs.append([jnp.where(here[nb // 2], 1.0, 0.0) if nb % 2 == qc else jnp.zeros((3, 8, 128), F32)
                        for qc in range(2)])
        below = [sub3 > ek for ek in range(7)]
        for k in range(32):
            nk, ek = k // 8, k % 8
            xk, qk = nk // 2, nk % 2
            idx = seg24 + (8 * xk + ek)
            pivot = [rhs[nk][qc][:, ek:ek + 1, :] for qc in range(2)]
            for nb in range(nk, 4):
                if nb == nk and ek == 7:
                    continue
                col = along(low[nb][qk], idx).reshape(3, 8, 128)
                if nb == nk:
                    col = jnp.where(below[ek], col, 0.0)
                for qc in range(2):
                    rhs[nb][qc] = rhs[nb][qc] - col * pivot[qc]
        for nb in range(4):
            xr, qr = nb // 2, nb % 2
            idx = (seg3 * 16 + 8 * xr + sub3).reshape(24, 128)
            scale = along(jnp.broadcast_to(rec[qr], (3, 8, 128)).reshape(24, 128), idx).reshape(3, 8, 128)
            for qc in range(2):
                val = rhs[nb][qc] * scale
                for lb in range(8):
                    inv[at:at + 3, qc, qr, lb, xr] = jnp.where(segs[lb], val, 0.0)

    def both(ref_of):
        return jnp.concatenate([ref_of(0), ref_of(1)], axis=1)

    def inv_full(b):
        return both(lambda qc: inv[b, qc].reshape(256, 128))

    def low_block(k, j):
        return both(lambda qc: goff[OFF_AT[k, j], qc].reshape(256, 128))

    def rows_of(tiles):
        return jnp.concatenate(tiles, axis=0)

    def double(w):
        pairs = range(4 // w)
        n = 16 * w
        shift = {1: 4, 2: 5, 4: 6}[w]
        shape = (2, w, 2, 8, 128)
        part = lanes(shape) >> shift
        even = [part == 2 * p for p in pairs]
        pair = [(lanes((w, 2, 8, 128)) >> (shift + 1)) == p for p in pairs]
        zero = jnp.zeros(shape, F32)
        first = (lanes((n, 128)) & n) == 0
        hole = jnp.zeros((128, 128), F32)

        def rows(p, odd):
            return pl.ds((2 * p + odd) * w, w)

        def twin(one, two):
            return rows_of([both(lambda h: (one, hole)[h]), both(lambda h: (hole, two)[h])])

        def low_left(b):
            acc = [zero, zero]
            for qc in range(2):
                for p in pairs:
                    acc[qc] = jnp.where(even[p], dg[b, qc, :, rows(p, 1)], acc[qc])
            return acc[0].reshape(2 * n, 128) + turn(acc[1].reshape(2 * n, 128), n)

        def up_inv(b):
            parts = []
            for p in pairs:
                for q in range(2):
                    one, two = (inv[b, qc, q, rows(p, 0)].reshape(n, 128) for qc in range(2))
                    parts.append(jnp.where(first, one, turn(two, n)))
            return rows_of(parts)

        def low_inv(b):
            acc = [inv[b, qc, :, rows(0, 1)] for qc in range(2)]
            for qc in range(2):
                for p in pairs[1:]:
                    acc[qc] = acc[qc] + inv[b, qc, :, rows(p, 1)]
            return turn(acc[0].reshape(2 * n, 128), -n) + acc[1].reshape(2 * n, 128)

        def temp_rows(temp):
            temp = temp.reshape(shape)
            return rows_of([jnp.where(pair[p], temp[q], 0.0).reshape(n, 128) for p in pairs for q in range(2)])

        two_blocks = ((5, 4), (3, 2), (1, 0))
        temps = [hdot(both(lambda h: low_left(bs[h])), twin(up_inv(bs[0]), up_inv(bs[1]))) for bs in two_blocks]
        for bs, temp in zip(two_blocks, temps):
            prod = -hdot(both(lambda h: low_inv(bs[h])), twin(temp_rows(temp[:, 0:128]), temp_rows(temp[:, 128:256])))
            for h, b in enumerate(bs):
                piece = prod[:, 128 * h:128 * h + 128]
                for qc, val in enumerate((piece, turn(piece, -n))):
                    val = val.reshape(shape)
                    for p in pairs:
                        inv[b, qc, :, rows(p, 1)] = jnp.where(even[p], val, inv[b, qc, :, rows(p, 1)])

    zst = [None] * 6

    def z_diag(j):
        return both(lambda qc: inv[j, qc, c, :, x].reshape(64, 128))

    def emit(i, j, blk):
        out[64 * i:64 * i + 64, 128 * j:128 * j + 128] = blk

    def add_terms(j, ks, acc):
        for k in ks:
            prod = hdot(zst[k], low_block(k, j))
            for i in range(k, 6):
                part = prod[64 * (i - k):64 * (i - k) + 64]
                acc[i] = part if acc[i] is None else acc[i] + part

    def finish(j, acc):
        emit(j, j, inv[j, y, c, :, x].reshape(64, 128))
        if j == 5:
            zst[5] = z_diag(5)
            return
        res = -hdot(rows_of(acc[j + 1:]), inv_full(j))
        zst[j] = rows_of([z_diag(j), res])
        mine = jnp.where(y == 0, res[:, 0:128], res[:, 128:256])
        for i in range(j + 1, 6):
            emit(i, j, mine[64 * (i - j - 1):64 * (i - j)])

    def finish_first(acc, lo, hi):
        res = -hdot(rows_of(acc[lo:hi]), inv[0, y].reshape(256, 128))
        for i in range(lo, hi):
            emit(i, 0, res[64 * (i - lo):64 * (i - lo) + 64])

    pack()
    pl.semaphore_wait(barrier, 3)
    own(DG)
    own(O1)
    for i in range(5):
        out[64 * i:64 * i + 64, 128 * (i + 1):768] = jnp.zeros((64, 128 * (5 - i)), F32)
    relay(DG)
    own(O2)
    relay(O1)
    own(O3)
    relay_diag(DG)
    wait_sib(DG)
    unpack()
    base(0)
    base(3)
    relay(O2)
    own(O4)
    double(1)
    double(2)
    relay_diag(O1)
    double(4)
    relay(O3)
    own(O5)
    own(O6)
    wait_sib(O1)
    finish(5, None)
    acc = [None] * 6
    add_terms(4, (5,), acc)
    finish(4, acc)
    acc = [None] * 6
    add_terms(3, (5, 4), acc)
    finish(3, acc)
    relay_diag(O2)
    wait_sib(O2)
    acc = [None] * 6
    add_terms(2, (5, 4, 3), acc)
    finish(2, acc)
    relay(O4)
    relay_diag(O3)
    wait_sib(O3)
    acc = [None] * 6
    add_terms(1, (5, 4, 3, 2), acc)
    finish(1, acc)
    emit(0, 0, inv[0, y, c, :, x].reshape(64, 128))
    relay(O5)
    relay(O6)
    relay_diag(O4)
    wait_sib(O4)
    acc = [None] * 6
    add_terms(0, (1, 2), acc)
    relay_diag(O5)
    relay_diag(O6)
    wait_sib(O5)
    add_terms(0, (3, 4), acc)
    finish_first(acc, 1, 5)
    wait_sib(O6)
    add_terms(0, (5,), acc)
    finish_first(acc, 5, 6)

    for cp in sends:
        cp.wait_send()


def solution(mesh):
    spec = P(("batch", "row"), "col")

    def body(local_l):
        rows, cols = local_l.shape
        return pl.pallas_call(
            kernel,
            out_shape=jax.ShapeDtypeStruct((rows, cols), F32),
            in_specs=[pl.BlockSpec(memory_space=pltpu.HBM)],
            out_specs=pl.BlockSpec(memory_space=pltpu.VMEM),
            scratch_shapes=[
                pltpu.VMEM((6, 8, 8, 128), F32),
                pltpu.VMEM((2, 2, 2, 30, 8, 128), F32),
                pltpu.VMEM((6, 2, 2, 8, 2, 8, 128), F32),
                pltpu.VMEM((15, 2, 2, 8, 2, 8, 128), F32),
                pltpu.VMEM((6, 2, 2, 8, 2, 8, 128), F32),
                pltpu.SemaphoreType.DMA((21,)),
                pltpu.SemaphoreType.DMA((7, 9)),
                pltpu.SemaphoreType.DMA((7, 9)),
            ],
            compiler_params=pltpu.CompilerParams(
                collective_id=0, has_side_effects=True, vmem_limit_bytes=40 * 1024 * 1024),
        )(pltpu.with_memory_space_constraint(local_l.reshape(rows // 8, 8, cols), pltpu.HBM))

    return jax.shard_map(body, mesh=mesh, in_specs=(spec,), out_specs=spec, check_vma=False)
```

```python
import jax
import jax.numpy as jnp
from jax import lax
from jax.experimental import pallas as pl
from jax.experimental.pallas import tpu as pltpu
from jax.sharding import PartitionSpec as P

MESH = pl.DeviceIdType.MESH
F32 = jnp.float32
OFF = (
    ((5, 4),),
    ((4, 3), (5, 3)),
    ((3, 2), (4, 2), (5, 2)),
    ((2, 1), (3, 1), (4, 1), (5, 1)),
    ((1, 0), (2, 0)),
    ((3, 0), (4, 0)),
    ((5, 0),),
)
DG, O1, O2, O3, O4, O5, O6, O7 = range(8)
OFF_LIST = [blk for grp in OFF for blk in grp]
OFF_AT = {blk: n for n, blk in enumerate(OFF_LIST)}
START = [OFF_AT[grp[0]] for grp in OFF]


def hdot(left, right):
    return jnp.dot(left, right, precision=lax.Precision.HIGHEST, preferred_element_type=F32)


def kernel(inp, out, raw, dpk, dg, goff, inv, loc_sem, g_send, g_recv):
    row = lax.axis_index("row")
    y = lax.axis_index("col")
    x = row // 2
    c = row % 2
    xo, yo, co = 1 - x, 1 - y, 1 - c
    sib = {"row": 2 * x + co}
    xnb = {"row": 2 * xo + c}
    ynb = {"col": yo}

    def take(bi, bj, dst, sem):
        return pltpu.make_async_copy(inp.at[pl.ds(8 * bi, 8), :, pl.ds(128 * bj, 128)], dst, sem)

    local = [[take(b, b, raw.at[b], loc_sem.at[b]) for b in range(6)]]
    for grp in OFF:
        local.append([take(bi, bj, goff.at[OFF_AT[bi, bj], y, c, :, x], loc_sem.at[6 + OFF_AT[bi, bj]])
                      for bi, bj in grp])
    for g in (O1, DG, O2, O3, O4, O5, O6, O7):
        for cp in local[g]:
            cp.start()

    barrier = pltpu.get_barrier_semaphore()
    for nbr in (sib, xnb, ynb):
        pl.semaphore_signal(barrier, inc=1, device_id=nbr, device_id_type=MESH)

    sub = lax.broadcasted_iota(jnp.int32, (8, 128), 0)
    lane = lax.broadcasted_iota(jnp.int32, (8, 128), 1)

    def lanes(shape):
        return lax.broadcasted_iota(jnp.int32, shape, len(shape) - 1)

    def along(tile, idx):
        return jnp.take_along_axis(tile, idx, axis=1, mode="promise_in_bounds")

    def turn(tile, n):
        return along(tile, (lanes(tile.shape) + (128 - n)) & 127)

    def pack():
        for b in range(6):
            local[DG][b].wait()
        for b in range(6):
            dpk[y, c, x, 5 * b] = raw[b, 7]
            for p in range(3):
                n = 112 - 16 * p
                dpk[y, c, x, 5 * b + 1 + p] = jnp.where(lane < n, raw[b, 6 - p], turn(raw[b, p], n))
            dpk[y, c, x, 5 * b + 4] = raw[b, 3]

    def unpack():
        for b in range(6):
            for qc in range(2):
                for lb in range(8):
                    if lb >= 3:
                        tiles = dpk[qc, :, :, 5 * b + 7 - lb]
                    else:
                        tiles = dpk[qc, :, :, 5 * b + 1 + lb].reshape(32, 128)
                        tiles = turn(tiles, 16 * (lb + 1)).reshape(2, 2, 8, 128)
                    dg[b, qc, :, lb] = tiles

    def slot(g, sx, sc, sy, half=None):
        if g == DG:
            lo, num = (0, 30) if half is None else (15 * half, 15)
            return dpk.at[sy, sc, sx, pl.ds(lo, num)]
        lo, num = (0, 8) if half is None else (4 * half, 4)
        return goff.at[pl.ds(START[g - 1], len(OFF[g - 1])), sy, sc, pl.ds(lo, num), sx]

    sends = []

    def gsend(g, k, ref, dev):
        cp = pltpu.make_async_remote_copy(ref, ref, g_send.at[g, k], g_recv.at[g, k], device_id=dev, device_id_type=MESH)
        cp.start()
        sends.append(cp)

    def gwait(g, k, ref):
        pltpu.make_async_remote_copy(ref, ref, g_send.at[g, k], g_recv.at[g, k], device_id=sib,
                                     device_id_type=MESH).wait_recv()

    def own(g):
        if g != DG:
            for cp in local[g]:
                cp.wait()
        gsend(g, 0, slot(g, x, c, y), xnb)
        gsend(g, 1, slot(g, x, c, y), ynb)
        gsend(g, 2, slot(g, x, c, y), sib)

    def relay(g):
        gwait(g, 0, slot(g, xo, c, y))
        gsend(g, 3, slot(g, xo, c, y, 0), ynb)
        gsend(g, 5, slot(g, xo, c, y), sib)
        gwait(g, 1, slot(g, x, c, yo))
        gsend(g, 4, slot(g, x, c, yo, 1), xnb)
        gsend(g, 6, slot(g, x, c, yo), sib)

    def relay_diag(g):
        for h in range(2):
            gwait(g, 3 + h, slot(g, xo, c, yo, h))
            gsend(g, 7 + h, slot(g, xo, c, yo, h), sib)

    def wait_sib(g):
        gwait(g, 2, slot(g, x, co, y))
        gwait(g, 5, slot(g, xo, co, y))
        gwait(g, 6, slot(g, x, co, yo))
        gwait(g, 7, slot(g, xo, co, yo, 0))
        gwait(g, 8, slot(g, xo, co, yo, 1))

    def base(at):
        sub3 = lax.broadcasted_iota(jnp.int32, (3, 8, 128), 1)
        lane3 = lanes((3, 8, 128))
        seg3 = lane3 >> 4
        seg24 = lanes((24, 128)) & 112
        here = [(sub3 == (lane3 & 7)) & (((lane3 >> 3) & 1) == xr) for xr in range(2)]
        segs = [seg3 == lb for lb in range(8)]
        low = [[None, None] for _ in range(4)]
        for nb in range(4):
            xr, qr = nb // 2, nb % 2
            for qc in range(2):
                acc = dg[at:at + 3, qc, qr, 0, xr]
                for lb in range(1, 8):
                    acc = jnp.where(segs[lb], dg[at:at + 3, qc, qr, lb, xr], acc)
                low[nb][qc] = acc
        rec = []
        for qc in range(2):
            dsum = jnp.where(here[0], low[qc][qc], 0.0) + jnp.where(here[1], low[2 + qc][qc], 0.0)
            rec.append(1.0 / jnp.sum(dsum, axis=1, keepdims=True))
        rhs = []
        for nb in range(4):
            for qc in range(2):
                low[nb][qc] = (low[nb][qc] * rec[qc]).reshape(24, 128)
            rhs.append([jnp.where(here[nb // 2], 1.0, 0.0) if nb % 2 == qc else jnp.zeros((3, 8, 128), F32)
                        for qc in range(2)])
        below = [sub3 > ek for ek in range(7)]
        for k in range(32):
            nk, ek = k // 8, k % 8
            xk, qk = nk // 2, nk % 2
            idx = seg24 + (8 * xk + ek)
            pivot = [rhs[nk][qc][:, ek:ek + 1, :] for qc in range(2)]
            for nb in range(nk, 4):
                if nb == nk and ek == 7:
                    continue
                col = along(low[nb][qk], idx).reshape(3, 8, 128)
                if nb == nk:
                    col = jnp.where(below[ek], col, 0.0)
                for qc in range(2):
                    rhs[nb][qc] = rhs[nb][qc] - col * pivot[qc]
        for nb in range(4):
            xr, qr = nb // 2, nb % 2
            idx = (seg3 * 16 + 8 * xr + sub3).reshape(24, 128)
            scale = along(jnp.broadcast_to(rec[qr], (3, 8, 128)).reshape(24, 128), idx).reshape(3, 8, 128)
            for qc in range(2):
                val = rhs[nb][qc] * scale
                for lb in range(8):
                    inv[at:at + 3, qc, qr, lb, xr] = jnp.where(segs[lb], val, 0.0)

    def both(ref_of):
        return jnp.concatenate([ref_of(0), ref_of(1)], axis=1)

    def inv_full(b):
        return both(lambda qc: inv[b, qc].reshape(256, 128))

    def low_block(k, j):
        return both(lambda qc: goff[OFF_AT[k, j], qc].reshape(256, 128))

    def rows_of(tiles):
        return jnp.concatenate(tiles, axis=0)

    def double(w):
        pairs = range(4 // w)
        n = 16 * w
        shift = {1: 4, 2: 5, 4: 6}[w]
        shape = (2, w, 2, 8, 128)
        part = lanes(shape) >> shift
        even = [part == 2 * p for p in pairs]
        pair = [(lanes((w, 2, 8, 128)) >> (shift + 1)) == p for p in pairs]
        zero = jnp.zeros(shape, F32)
        first = (lanes((n, 128)) & n) == 0
        hole = jnp.zeros((128, 128), F32)

        def rows(p, odd):
            return pl.ds((2 * p + odd) * w, w)

        def twin(one, two):
            return rows_of([both(lambda h: (one, hole)[h]), both(lambda h: (hole, two)[h])])

        def low_left(b):
            acc = [zero, zero]
            for qc in range(2):
                for p in pairs:
                    acc[qc] = jnp.where(even[p], dg[b, qc, :, rows(p, 1)], acc[qc])
            return acc[0].reshape(2 * n, 128) + turn(acc[1].reshape(2 * n, 128), n)

        def up_inv(b):
            parts = []
            for p in pairs:
                for q in range(2):
                    one, two = (inv[b, qc, q, rows(p, 0)].reshape(n, 128) for qc in range(2))
                    parts.append(jnp.where(first, one, turn(two, n)))
            return rows_of(parts)

        def low_inv(b):
            acc = [inv[b, qc, :, rows(0, 1)] for qc in range(2)]
            for qc in range(2):
                for p in pairs[1:]:
                    acc[qc] = acc[qc] + inv[b, qc, :, rows(p, 1)]
            return turn(acc[0].reshape(2 * n, 128), -n) + acc[1].reshape(2 * n, 128)

        def temp_rows(temp):
            temp = temp.reshape(shape)
            return rows_of([jnp.where(pair[p], temp[q], 0.0).reshape(n, 128) for p in pairs for q in range(2)])

        two_blocks = ((5, 4), (3, 2), (1, 0))
        temps = [hdot(both(lambda h: low_left(bs[h])), twin(up_inv(bs[0]), up_inv(bs[1]))) for bs in two_blocks]
        for bs, temp in zip(two_blocks, temps):
            prod = -hdot(both(lambda h: low_inv(bs[h])), twin(temp_rows(temp[:, 0:128]), temp_rows(temp[:, 128:256])))
            for h, b in enumerate(bs):
                piece = prod[:, 128 * h:128 * h + 128]
                for qc, val in enumerate((piece, turn(piece, -n))):
                    val = val.reshape(shape)
                    for p in pairs:
                        inv[b, qc, :, rows(p, 1)] = jnp.where(even[p], val, inv[b, qc, :, rows(p, 1)])

    zst = [None] * 6

    def z_diag(j):
        return both(lambda qc: inv[j, qc, c, :, x].reshape(64, 128))

    def emit(i, j, blk):
        out[64 * i:64 * i + 64, 128 * j:128 * j + 128] = blk

    def add_terms(j, ks, acc):
        for k in ks:
            prod = hdot(zst[k], low_block(k, j))
            for i in range(k, 6):
                part = prod[64 * (i - k):64 * (i - k) + 64]
                acc[i] = part if acc[i] is None else acc[i] + part

    def finish(j, acc):
        emit(j, j, inv[j, y, c, :, x].reshape(64, 128))
        if j == 5:
            zst[5] = z_diag(5)
            return
        res = -hdot(rows_of(acc[j + 1:]), inv_full(j))
        zst[j] = rows_of([z_diag(j), res])
        mine = jnp.where(y == 0, res[:, 0:128], res[:, 128:256])
        for i in range(j + 1, 6):
            emit(i, j, mine[64 * (i - j - 1):64 * (i - j)])

    def finish_first(acc, lo, hi):
        res = -hdot(rows_of(acc[lo:hi]), inv[0, y].reshape(256, 128))
        for i in range(lo, hi):
            emit(i, 0, res[64 * (i - lo):64 * (i - lo) + 64])

    pl.semaphore_wait(barrier, 3)
    own(O1)
    pack()
    own(DG)
    own(O2)
    for i in range(5):
        out[64 * i:64 * i + 64, 128 * (i + 1):768] = jnp.zeros((64, 128 * (5 - i)), F32)
    relay(O1)
    relay(DG)
    own(O3)
    relay(O2)
    own(O4)
    relay_diag(O1)
    relay_diag(DG)
    wait_sib(DG)
    unpack()
    base(0)
    base(3)
    relay(O3)
    own(O5)
    double(1)
    double(2)
    relay_diag(O2)
    double(4)
    wait_sib(O1)
    finish(5, None)
    acc = [None] * 6
    add_terms(4, (5,), acc)
    finish(4, acc)
    relay(O4)
    own(O6)
    own(O7)
    wait_sib(O2)
    acc = [None] * 6
    add_terms(3, (5, 4), acc)
    finish(3, acc)
    relay_diag(O3)
    relay(O5)
    wait_sib(O3)
    acc = [None] * 6
    add_terms(2, (5, 4, 3), acc)
    finish(2, acc)
    emit(0, 0, inv[0, y, c, :, x].reshape(64, 128))
    relay_diag(O4)
    relay(O6)
    wait_sib(O4)
    acc = [None] * 6
    add_terms(1, (5, 4), acc)
    relay(O7)
    add_terms(1, (3, 2), acc)
    relay_diag(O5)
    finish(1, acc)
    relay_diag(O6)
    relay_diag(O7)
    wait_sib(O5)
    acc = [None] * 6
    add_terms(0, (1, 2), acc)
    wait_sib(O6)
    add_terms(0, (3, 4), acc)
    finish_first(acc, 1, 5)
    wait_sib(O7)
    add_terms(0, (5,), acc)
    finish_first(acc, 5, 6)

    for cp in sends:
        cp.wait_send()


def solution(mesh):
    spec = P(("batch", "row"), "col")

    def body(local_l):
        rows, cols = local_l.shape
        return pl.pallas_call(
            kernel,
            out_shape=jax.ShapeDtypeStruct((rows, cols), F32),
            in_specs=[pl.BlockSpec(memory_space=pltpu.HBM)],
            out_specs=pl.BlockSpec(memory_space=pltpu.VMEM),
            scratch_shapes=[
                pltpu.VMEM((6, 8, 8, 128), F32),
                pltpu.VMEM((2, 2, 2, 30, 8, 128), F32),
                pltpu.VMEM((6, 2, 2, 8, 2, 8, 128), F32),
                pltpu.VMEM((15, 2, 2, 8, 2, 8, 128), F32),
                pltpu.VMEM((6, 2, 2, 8, 2, 8, 128), F32),
                pltpu.SemaphoreType.DMA((21,)),
                pltpu.SemaphoreType.DMA((8, 9)),
                pltpu.SemaphoreType.DMA((8, 9)),
            ],
            compiler_params=pltpu.CompilerParams(
                collective_id=0, has_side_effects=True, vmem_limit_bytes=40 * 1024 * 1024),
        )(pltpu.with_memory_space_constraint(local_l.reshape(rows // 8, 8, cols), pltpu.HBM))

    return jax.shard_map(body, mesh=mesh, in_specs=(spec,), out_specs=spec, check_vma=False)
```

```python
import jax
import jax.numpy as jnp
from jax import lax
from jax.experimental import pallas as pl
from jax.experimental.pallas import tpu as pltpu
from jax.sharding import PartitionSpec as P

MESH = pl.DeviceIdType.MESH
F32 = jnp.float32
DB, DA, BO, AO = range(4)
DIAG = {DB: (5, 4, 3), DA: (2, 1, 0)}
OFF = {BO: ((5, 4), (4, 3), (5, 3)), AO: ((2, 1), (1, 0), (2, 0))}
OFF_AT = {blk: 3 * (g - 2) + i for g, grp in OFF.items() for i, blk in enumerate(grp)}


def hdot(left, right):
    return jnp.dot(left, right, precision=lax.Precision.HIGHEST, preferred_element_type=F32)


def kernel(inp, out, raw, dpk, dg, goff, cbuf, ubuf, inv, loc_sem, g_send, g_recv, c_send, c_recv, u_send, u_recv):
    row = lax.axis_index("row")
    y = lax.axis_index("col")
    x = row // 2
    c = row % 2
    xo, yo, co = 1 - x, 1 - y, 1 - c
    sib = {"row": 2 * x + co}
    xnb = {"row": 2 * xo + c}
    ynb = {"col": yo}

    def take(bi, bj, dst, sem):
        return pltpu.make_async_copy(inp.at[pl.ds(8 * bi, 8), :, pl.ds(128 * bj, 128)], dst, sem)

    local = {g: [take(b, b, raw.at[b], loc_sem.at[b]) for b in DIAG[g]] for g in DIAG}
    for g in OFF:
        local[g] = [take(bi, bj, goff.at[OFF_AT[bi, bj], y, c, :, x], loc_sem.at[6 + OFF_AT[bi, bj]]) for bi, bj in OFF[g]]
    local_c = [[take(3 + k, j, cbuf.at[j, k, c, :, x], loc_sem.at[12 + 3 * j + k]) for k in range(3)] for j in range(3)]
    for grp in (local[DB], local[BO], local[DA], local_c[2], local_c[1], local_c[0], local[AO]):
        for cp in grp:
            cp.start()

    barrier = pltpu.get_barrier_semaphore()
    for nbr in (sib, xnb, ynb):
        pl.semaphore_signal(barrier, inc=1, device_id=nbr, device_id_type=MESH)

    sub = lax.broadcasted_iota(jnp.int32, (8, 128), 0)
    lane = lax.broadcasted_iota(jnp.int32, (8, 128), 1)

    def lanes(shape):
        return lax.broadcasted_iota(jnp.int32, shape, len(shape) - 1)

    def along(tile, idx):
        return jnp.take_along_axis(tile, idx, axis=1, mode="promise_in_bounds")

    def turn(tile, n):
        return along(tile, (lanes(tile.shape) + (128 - n)) & 127)

    def pack(g):
        for cp in local[g]:
            cp.wait()
        for i, b in enumerate(DIAG[g]):
            dpk[g, y, c, x, 5 * i] = raw[b, 7]
            for p in range(3):
                n = 112 - 16 * p
                dpk[g, y, c, x, 5 * i + 1 + p] = jnp.where(lane < n, raw[b, 6 - p], turn(raw[b, p], n))
            dpk[g, y, c, x, 5 * i + 4] = raw[b, 3]

    def unpack(g):
        for i, b in enumerate(DIAG[g]):
            for qc in range(2):
                for lb in range(8):
                    if lb >= 3:
                        tiles = dpk[g, qc, :, :, 5 * i + 7 - lb]
                    else:
                        tiles = dpk[g, qc, :, :, 5 * i + 1 + lb].reshape(32, 128)
                        tiles = turn(tiles, 16 * (lb + 1)).reshape(2, 2, 8, 128)
                    dg[b, qc, :, lb] = tiles

    def slot(g, sx, sc, sy):
        if g in DIAG:
            return dpk.at[g, sy, sc, sx]
        return goff.at[pl.ds(3 * (g - 2), 3), sy, sc, :, sx]

    sends = []

    def copy(ref, send, recv, dev):
        return pltpu.make_async_remote_copy(ref, ref, send, recv, device_id=dev, device_id_type=MESH)

    def start(cp):
        cp.start()
        sends.append(cp)

    def gsend(g, k, ref, dev):
        start(copy(ref, g_send.at[g, k], g_recv.at[g, k], dev))

    def gwait(g, k, ref):
        copy(ref, g_send.at[g, k], g_recv.at[g, k], sib).wait_recv()

    def own(g, to):
        for k, dev in enumerate((xnb, ynb, sib)):
            if "xys"[k] in to:
                gsend(g, k, slot(g, x, c, y), dev)

    def ready(g):
        for cp in local[g]:
            cp.wait()

    def from_x(g):
        gwait(g, 0, slot(g, xo, c, y))
        if g != AO:
            gsend(g, 3, slot(g, xo, c, y), ynb)
        gsend(g, 4, slot(g, xo, c, y), sib)

    def from_y(g):
        gwait(g, 1, slot(g, x, c, yo))
        if g == AO:
            gsend(g, 3, slot(g, x, c, yo), xnb)
        gsend(g, 5, slot(g, x, c, yo), sib)

    def from_diag(g):
        gwait(g, 3, slot(g, xo, c, yo))
        gsend(g, 6, slot(g, xo, c, yo), sib)

    def wait_sib(g):
        gwait(g, 2, slot(g, x, co, y))
        gwait(g, 4, slot(g, xo, co, y))
        gwait(g, 5, slot(g, x, co, yo))
        gwait(g, 6, slot(g, xo, co, yo))

    def c_slot(j, sx, sc):
        return cbuf.at[j, :, sc, :, sx]

    def c_own(j):
        for cp in local_c[j]:
            cp.wait()
        for k, dev in enumerate((xnb, sib)):
            start(copy(c_slot(j, x, c), c_send.at[j, k], c_recv.at[j, k], dev))

    def c_relay(j):
        copy(c_slot(j, xo, c), c_send.at[j, 0], c_recv.at[j, 0], sib).wait_recv()
        start(copy(c_slot(j, xo, c), c_send.at[j, 2], c_recv.at[j, 2], sib))

    def c_wait(j):
        copy(c_slot(j, x, co), c_send.at[j, 1], c_recv.at[j, 1], sib).wait_recv()
        copy(c_slot(j, xo, co), c_send.at[j, 2], c_recv.at[j, 2], sib).wait_recv()

    def u_send_to(j):
        start(copy(ubuf.at[j, y], u_send.at[j], u_recv.at[j], ynb))

    def u_wait(j):
        copy(ubuf.at[j, yo], u_send.at[j], u_recv.at[j], ynb).wait_recv()

    def base(at):
        sub3 = lax.broadcasted_iota(jnp.int32, (3, 8, 128), 1)
        lane3 = lanes((3, 8, 128))
        seg3 = lane3 >> 4
        seg24 = lanes((24, 128)) & 112
        here = [(sub3 == (lane3 & 7)) & (((lane3 >> 3) & 1) == xr) for xr in range(2)]
        segs = [seg3 == lb for lb in range(8)]
        low = [[None, None] for _ in range(4)]
        for nb in range(4):
            xr, qr = nb // 2, nb % 2
            for qc in range(2):
                acc = dg[at:at + 3, qc, qr, 0, xr]
                for lb in range(1, 8):
                    acc = jnp.where(segs[lb], dg[at:at + 3, qc, qr, lb, xr], acc)
                low[nb][qc] = acc
        rec = []
        for qc in range(2):
            dsum = jnp.where(here[0], low[qc][qc], 0.0) + jnp.where(here[1], low[2 + qc][qc], 0.0)
            rec.append(1.0 / jnp.sum(dsum, axis=1, keepdims=True))
        rhs = []
        for nb in range(4):
            for qc in range(2):
                low[nb][qc] = (low[nb][qc] * rec[qc]).reshape(24, 128)
            rhs.append([jnp.where(here[nb // 2], 1.0, 0.0) if nb % 2 == qc else jnp.zeros((3, 8, 128), F32)
                        for qc in range(2)])
        below = [sub3 > ek for ek in range(7)]
        for k in range(32):
            nk, ek = k // 8, k % 8
            xk, qk = nk // 2, nk % 2
            idx = seg24 + (8 * xk + ek)
            pivot = [rhs[nk][qc][:, ek:ek + 1, :] for qc in range(2)]
            for nb in range(nk, 4):
                if nb == nk and ek == 7:
                    continue
                col = along(low[nb][qk], idx).reshape(3, 8, 128)
                if nb == nk:
                    col = jnp.where(below[ek], col, 0.0)
                for qc in range(2):
                    rhs[nb][qc] = rhs[nb][qc] - col * pivot[qc]
        for nb in range(4):
            xr, qr = nb // 2, nb % 2
            idx = (seg3 * 16 + 8 * xr + sub3).reshape(24, 128)
            scale = along(jnp.broadcast_to(rec[qr], (3, 8, 128)).reshape(24, 128), idx).reshape(3, 8, 128)
            for qc in range(2):
                val = rhs[nb][qc] * scale
                for lb in range(8):
                    inv[at:at + 3, qc, qr, lb, xr] = jnp.where(segs[lb], val, 0.0)

    def both(ref_of):
        return jnp.concatenate([ref_of(0), ref_of(1)], axis=1)

    def inv_full(b):
        return both(lambda qc: inv[b, qc].reshape(256, 128))

    def low_block(k, j):
        return both(lambda qc: goff[OFF_AT[k, j], qc].reshape(256, 128))

    def rows_of(tiles):
        return jnp.concatenate(tiles, axis=0)

    def double(group, w):
        pairs = range(4 // w)
        n = 16 * w
        shift = {1: 4, 2: 5, 4: 6}[w]
        shape = (2, w, 2, 8, 128)
        part = lanes(shape) >> shift
        even = [part == 2 * p for p in pairs]
        pair = [(lanes((w, 2, 8, 128)) >> (shift + 1)) == p for p in pairs]
        zero = jnp.zeros(shape, F32)
        first = (lanes((n, 128)) & n) == 0
        hole = jnp.zeros((128, 128), F32)

        def rows(p, odd):
            return pl.ds((2 * p + odd) * w, w)

        def twin(one, two):
            return rows_of([both(lambda h: (one, hole)[h]), both(lambda h: (hole, two)[h])])

        def low_left(b):
            acc = [zero, zero]
            for qc in range(2):
                for p in pairs:
                    acc[qc] = jnp.where(even[p], dg[b, qc, :, rows(p, 1)], acc[qc])
            return acc[0].reshape(2 * n, 128) + turn(acc[1].reshape(2 * n, 128), n)

        def up_inv(b):
            parts = []
            for p in pairs:
                for q in range(2):
                    one, two = (inv[b, qc, q, rows(p, 0)].reshape(n, 128) for qc in range(2))
                    parts.append(jnp.where(first, one, turn(two, n)))
            return rows_of(parts)

        def low_inv(b):
            acc = [inv[b, qc, :, rows(0, 1)] for qc in range(2)]
            for qc in range(2):
                for p in pairs[1:]:
                    acc[qc] = acc[qc] + inv[b, qc, :, rows(p, 1)]
            return turn(acc[0].reshape(2 * n, 128), -n) + acc[1].reshape(2 * n, 128)

        def temp_rows(temp):
            temp = temp.reshape(shape)
            return rows_of([jnp.where(pair[p], temp[q], 0.0).reshape(n, 128) for p in pairs for q in range(2)])

        def product(lefts, rights):
            if len(lefts) == 1:
                return hdot(lefts[0], rights[0])
            return hdot(jnp.concatenate(lefts, axis=1), twin(*rights))

        two_blocks = (group[:2], group[2:])
        temps = [product([low_left(b) for b in bs], [up_inv(b) for b in bs]) for bs in two_blocks]
        for bs, temp in zip(two_blocks, temps):
            prod = -product([low_inv(b) for b in bs],
                            [temp_rows(temp[:, 128 * h:128 * h + 128]) for h in range(len(bs))])
            for h, b in enumerate(bs):
                piece = prod[:, 128 * h:128 * h + 128]
                for qc, val in enumerate((piece, turn(piece, -n))):
                    val = val.reshape(shape)
                    for p in pairs:
                        inv[b, qc, :, rows(p, 1)] = jnp.where(even[p], val, inv[b, qc, :, rows(p, 1)])

    zst = [None] * 6

    def z_diag(j):
        return both(lambda qc: inv[j, qc, c, :, x].reshape(64, 128))

    def emit(i, j, blk):
        out[64 * i:64 * i + 64, 128 * j:128 * j + 128] = blk

    def add_terms(j, ks, acc):
        for k in ks:
            prod = hdot(zst[k], low_block(k, j))
            for i in range(k, 6):
                part = prod[64 * (i - k):64 * (i - k) + 64]
                acc[i] = part if acc[i] is None else acc[i] + part

    def finish(j, acc):
        emit(j, j, inv[j, y, c, :, x].reshape(64, 128))
        if j == 5:
            zst[5] = z_diag(5)
            return
        res = -hdot(rows_of(acc[j + 1:]), inv_full(j))
        zst[j] = rows_of([z_diag(j), res])
        mine = jnp.where(y == 0, res[:, 0:128], res[:, 128:256])
        for i in range(j + 1, 6):
            emit(i, j, mine[64 * (i - j - 1):64 * (i - j)])

    def finish_first(acc, lo, hi):
        res = -hdot(rows_of(acc[lo:hi]), inv[0, y].reshape(256, 128))
        for i in range(lo, hi):
            emit(i, 0, res[64 * (i - lo):64 * (i - lo) + 64])

    def inverses(g):
        unpack(g)
        base(min(DIAG[g]))
        for w in (1, 2, 4):
            double(DIAG[g], w)

    def u_compute(j):
        acc = [None] * 6
        for k in (3, 4, 5):
            prod = hdot(zst[k], cbuf[j, k - 3].reshape(256, 128))
            for i in range(k, 6):
                part = prod[64 * (i - k):64 * (i - k) + 64]
                acc[i] = part if acc[i] is None else acc[i] + part
        for i in (3, 4, 5):
            ubuf[j, y, 64 * (i - 3):64 * (i - 3) + 64] = acc[i]

    def u_add(j, acc):
        for i in (3, 4, 5):
            part = both(lambda q: ubuf[j, q, 64 * (i - 3):64 * (i - 3) + 64])
            acc[i] = part if acc[i] is None else acc[i] + part

    pack(DB)
    pl.semaphore_wait(barrier, 3)
    own(DB, "xys")
    ready(BO)
    own(BO, "xys")
    pack(DA)
    own(DA, "xs")
    c_own(2)
    for i in range(5):
        out[64 * i:64 * i + 64, 128 * (i + 1):768] = jnp.zeros((64, 128 * (5 - i)), F32)
    from_x(DB)
    from_y(DB)
    c_own(1)
    c_own(0)
    from_x(BO)
    own(DA, "y")
    from_y(BO)
    ready(AO)
    own(AO, "xys")
    from_x(DA)
    from_diag(DB)
    wait_sib(DB)
    inverses(DB)
    from_diag(BO)
    c_relay(2)
    from_y(DA)
    wait_sib(BO)
    finish(5, None)
    acc = [None] * 6
    add_terms(4, (5,), acc)
    finish(4, acc)
    acc = [None] * 6
    add_terms(3, (5, 4), acc)
    finish(3, acc)
    c_wait(2)
    c_relay(1)
    u_compute(2)
    u_send_to(2)
    c_wait(1)
    from_y(AO)
    u_compute(1)
    u_send_to(1)
    c_relay(0)
    from_diag(DA)
    c_wait(0)
    u_compute(0)
    u_send_to(0)
    from_x(AO)
    wait_sib(DA)
    inverses(DA)
    from_diag(AO)
    emit(0, 0, inv[0, y, c, :, x].reshape(64, 128))
    u_wait(2)
    acc = [None] * 6
    u_add(2, acc)
    finish(2, acc)
    wait_sib(AO)
    acc = [None] * 6
    add_terms(1, (2,), acc)
    u_wait(1)
    u_add(1, acc)
    finish(1, acc)
    acc = [None] * 6
    add_terms(0, (2, 1), acc)
    finish_first(acc, 1, 3)
    u_wait(0)
    u_add(0, acc)
    finish_first(acc, 3, 6)

    for cp in sends:
        cp.wait_send()


def solution(mesh):
    spec = P(("batch", "row"), "col")

    def body(local_l):
        rows, cols = local_l.shape
        return pl.pallas_call(
            kernel,
            out_shape=jax.ShapeDtypeStruct((rows, cols), F32),
            in_specs=[pl.BlockSpec(memory_space=pltpu.HBM)],
            out_specs=pl.BlockSpec(memory_space=pltpu.VMEM),
            scratch_shapes=[
                pltpu.VMEM((6, 8, 8, 128), F32),
                pltpu.VMEM((2, 2, 2, 2, 15, 8, 128), F32),
                pltpu.VMEM((6, 2, 2, 8, 2, 8, 128), F32),
                pltpu.VMEM((6, 2, 2, 8, 2, 8, 128), F32),
                pltpu.VMEM((3, 3, 2, 8, 2, 8, 128), F32),
                pltpu.VMEM((3, 2, 192, 128), F32),
                pltpu.VMEM((6, 2, 2, 8, 2, 8, 128), F32),
                pltpu.SemaphoreType.DMA((21,)),
                pltpu.SemaphoreType.DMA((4, 7)),
                pltpu.SemaphoreType.DMA((4, 7)),
                pltpu.SemaphoreType.DMA((3, 3)),
                pltpu.SemaphoreType.DMA((3, 3)),
                pltpu.SemaphoreType.DMA((3,)),
                pltpu.SemaphoreType.DMA((3,)),
            ],
            compiler_params=pltpu.CompilerParams(
                collective_id=0, has_side_effects=True, vmem_limit_bytes=40 * 1024 * 1024),
        )(pltpu.with_memory_space_constraint(local_l.reshape(rows // 8, 8, cols), pltpu.HBM))

    return jax.shard_map(body, mesh=mesh, in_specs=(spec,), out_specs=spec, check_vma=False)
```

```python
import jax
import jax.numpy as jnp
from jax import lax
from jax.experimental import pallas as pl
from jax.experimental.pallas import tpu as pltpu
from jax.sharding import PartitionSpec as P

MESH = pl.DeviceIdType.MESH
F32 = jnp.float32
DB, DA, BO, AO = range(4)
DIAG = {DB: (5, 4, 3), DA: (2, 1, 0)}
OFF = {BO: ((5, 4), (4, 3), (5, 3)), AO: ((2, 1), (1, 0), (2, 0))}
OFF_AT = {blk: 3 * (g - 2) + i for g, grp in OFF.items() for i, blk in enumerate(grp)}


def hdot(left, right):
    return jnp.dot(left, right, precision=lax.Precision.HIGHEST, preferred_element_type=F32)


def kernel(inp, out, raw, dpk, dg, goff, cbuf, ubuf, inv, loc_sem, g_send, g_recv, c_send, c_recv, u_send, u_recv):
    row = lax.axis_index("row")
    y = lax.axis_index("col")
    x = row // 2
    c = row % 2
    xo, yo, co = 1 - x, 1 - y, 1 - c
    sib = {"row": 2 * x + co}
    xnb = {"row": 2 * xo + c}
    ynb = {"col": yo}

    def take(bi, bj, dst, sem):
        return pltpu.make_async_copy(inp.at[pl.ds(8 * bi, 8), :, pl.ds(128 * bj, 128)], dst, sem)

    local = {g: [take(b, b, raw.at[b], loc_sem.at[b]) for b in DIAG[g]] for g in DIAG}
    for g in OFF:
        local[g] = [take(bi, bj, goff.at[OFF_AT[bi, bj], y, c, :, x], loc_sem.at[6 + OFF_AT[bi, bj]]) for bi, bj in OFF[g]]
    local_c = [[take(3 + k, j, cbuf.at[j, k, c, :, x], loc_sem.at[12 + 3 * j + k]) for k in range(3)] for j in range(3)]
    for grp in (local[DB], local[BO], local[DA], local_c[2], local_c[1], local_c[0], local[AO]):
        for cp in grp:
            cp.start()

    barrier = pltpu.get_barrier_semaphore()
    for nbr in (sib, xnb, ynb):
        pl.semaphore_signal(barrier, inc=1, device_id=nbr, device_id_type=MESH)

    sub = lax.broadcasted_iota(jnp.int32, (8, 128), 0)
    lane = lax.broadcasted_iota(jnp.int32, (8, 128), 1)

    def lanes(shape):
        return lax.broadcasted_iota(jnp.int32, shape, len(shape) - 1)

    def along(tile, idx):
        return jnp.take_along_axis(tile, idx, axis=1, mode="promise_in_bounds")

    def turn(tile, n):
        return along(tile, (lanes(tile.shape) + (128 - n)) & 127)

    def pack(g):
        for cp in local[g]:
            cp.wait()
        for i, b in enumerate(DIAG[g]):
            dpk[g, y, c, x, 5 * i] = raw[b, 7]
            for p in range(3):
                n = 112 - 16 * p
                dpk[g, y, c, x, 5 * i + 1 + p] = jnp.where(lane < n, raw[b, 6 - p], turn(raw[b, p], n))
            dpk[g, y, c, x, 5 * i + 4] = raw[b, 3]

    def unpack(g):
        for i, b in enumerate(DIAG[g]):
            for qc in range(2):
                for lb in range(8):
                    if lb >= 3:
                        tiles = dpk[g, qc, :, :, 5 * i + 7 - lb]
                    else:
                        tiles = dpk[g, qc, :, :, 5 * i + 1 + lb].reshape(32, 128)
                        tiles = turn(tiles, 16 * (lb + 1)).reshape(2, 2, 8, 128)
                    dg[b, qc, :, lb] = tiles

    def slot(g, sx, sc, sy):
        if g in DIAG:
            return dpk.at[g, sy, sc, sx]
        return goff.at[pl.ds(3 * (g - 2), 3), sy, sc, :, sx]

    sends = []

    def copy(ref, send, recv, dev):
        return pltpu.make_async_remote_copy(ref, ref, send, recv, device_id=dev, device_id_type=MESH)

    def start(cp):
        cp.start()
        sends.append(cp)

    def gsend(g, k, ref, dev):
        start(copy(ref, g_send.at[g, k], g_recv.at[g, k], dev))

    def gwait(g, k, ref):
        copy(ref, g_send.at[g, k], g_recv.at[g, k], sib).wait_recv()

    def own(g, to):
        for k, dev in enumerate((xnb, ynb, sib)):
            if "xys"[k] in to:
                gsend(g, k, slot(g, x, c, y), dev)

    def ready(g):
        for cp in local[g]:
            cp.wait()

    def from_x(g):
        gwait(g, 0, slot(g, xo, c, y))
        if g != AO:
            gsend(g, 3, slot(g, xo, c, y), ynb)
        gsend(g, 4, slot(g, xo, c, y), sib)

    def from_y(g):
        gwait(g, 1, slot(g, x, c, yo))
        if g == AO:
            gsend(g, 3, slot(g, x, c, yo), xnb)
        gsend(g, 5, slot(g, x, c, yo), sib)

    def from_diag(g):
        gwait(g, 3, slot(g, xo, c, yo))
        gsend(g, 6, slot(g, xo, c, yo), sib)

    def wait_sib(g):
        gwait(g, 2, slot(g, x, co, y))
        gwait(g, 4, slot(g, xo, co, y))
        gwait(g, 5, slot(g, x, co, yo))
        gwait(g, 6, slot(g, xo, co, yo))

    def c_slot(j, sx, sc):
        return cbuf.at[j, :, sc, :, sx]

    def c_own(j):
        for cp in local_c[j]:
            cp.wait()
        for k, dev in enumerate((xnb, sib)):
            start(copy(c_slot(j, x, c), c_send.at[j, k], c_recv.at[j, k], dev))

    def c_relay(j):
        copy(c_slot(j, xo, c), c_send.at[j, 0], c_recv.at[j, 0], sib).wait_recv()
        start(copy(c_slot(j, xo, c), c_send.at[j, 2], c_recv.at[j, 2], sib))

    def c_wait(j):
        copy(c_slot(j, x, co), c_send.at[j, 1], c_recv.at[j, 1], sib).wait_recv()
        copy(c_slot(j, xo, co), c_send.at[j, 2], c_recv.at[j, 2], sib).wait_recv()

    def u_send_to(j):
        start(copy(ubuf.at[j, y], u_send.at[j], u_recv.at[j], ynb))

    def u_wait(j):
        copy(ubuf.at[j, yo], u_send.at[j], u_recv.at[j], ynb).wait_recv()

    def base(at):
        sub3 = lax.broadcasted_iota(jnp.int32, (3, 8, 128), 1)
        lane3 = lanes((3, 8, 128))
        seg3 = lane3 >> 4
        seg24 = lanes((24, 128)) & 112
        here = [(sub3 == (lane3 & 7)) & (((lane3 >> 3) & 1) == xr) for xr in range(2)]
        segs = [seg3 == lb for lb in range(8)]
        low = [[None, None] for _ in range(4)]
        for nb in range(4):
            xr, qr = nb // 2, nb % 2
            for qc in range(2):
                acc = dg[at:at + 3, qc, qr, 0, xr]
                for lb in range(1, 8):
                    acc = jnp.where(segs[lb], dg[at:at + 3, qc, qr, lb, xr], acc)
                low[nb][qc] = acc
        rec = []
        for qc in range(2):
            dsum = jnp.where(here[0], low[qc][qc], 0.0) + jnp.where(here[1], low[2 + qc][qc], 0.0)
            rec.append(1.0 / jnp.sum(dsum, axis=1, keepdims=True))
        rhs = []
        for nb in range(4):
            for qc in range(2):
                low[nb][qc] = (low[nb][qc] * rec[qc]).reshape(24, 128)
            rhs.append([jnp.where(here[nb // 2], 1.0, 0.0) if nb % 2 == qc else jnp.zeros((3, 8, 128), F32)
                        for qc in range(2)])
        below = [sub3 > ek for ek in range(7)]
        for k in range(32):
            nk, ek = k // 8, k % 8
            xk, qk = nk // 2, nk % 2
            idx = seg24 + (8 * xk + ek)
            pivot = [rhs[nk][qc][:, ek:ek + 1, :] for qc in range(2)]
            for nb in range(nk, 4):
                if nb == nk and ek == 7:
                    continue
                col = along(low[nb][qk], idx).reshape(3, 8, 128)
                if nb == nk:
                    col = jnp.where(below[ek], col, 0.0)
                for qc in range(2):
                    rhs[nb][qc] = rhs[nb][qc] - col * pivot[qc]
        for nb in range(4):
            xr, qr = nb // 2, nb % 2
            idx = (seg3 * 16 + 8 * xr + sub3).reshape(24, 128)
            scale = along(jnp.broadcast_to(rec[qr], (3, 8, 128)).reshape(24, 128), idx).reshape(3, 8, 128)
            for qc in range(2):
                val = rhs[nb][qc] * scale
                for lb in range(8):
                    inv[at:at + 3, qc, qr, lb, xr] = jnp.where(segs[lb], val, 0.0)

    def both(ref_of):
        return jnp.concatenate([ref_of(0), ref_of(1)], axis=1)

    def inv_full(b):
        return both(lambda qc: inv[b, qc].reshape(256, 128))

    def low_block(k, j):
        return both(lambda qc: goff[OFF_AT[k, j], qc].reshape(256, 128))

    def rows_of(tiles):
        return jnp.concatenate(tiles, axis=0)

    def double(group, w):
        pairs = range(4 // w)
        n = 16 * w
        shift = {1: 4, 2: 5, 4: 6}[w]
        shape = (2, w, 2, 8, 128)
        part = lanes(shape) >> shift
        even = [part == 2 * p for p in pairs]
        pair = [(lanes((w, 2, 8, 128)) >> (shift + 1)) == p for p in pairs]
        zero = jnp.zeros(shape, F32)
        first = (lanes((n, 128)) & n) == 0
        hole = jnp.zeros((128, 128), F32)

        def rows(p, odd):
            return pl.ds((2 * p + odd) * w, w)

        def twin(one, two):
            return rows_of([both(lambda h: (one, hole)[h]), both(lambda h: (hole, two)[h])])

        def low_left(b):
            acc = [zero, zero]
            for qc in range(2):
                for p in pairs:
                    acc[qc] = jnp.where(even[p], dg[b, qc, :, rows(p, 1)], acc[qc])
            return acc[0].reshape(2 * n, 128) + turn(acc[1].reshape(2 * n, 128), n)

        def up_inv(b):
            parts = []
            for p in pairs:
                for q in range(2):
                    one, two = (inv[b, qc, q, rows(p, 0)].reshape(n, 128) for qc in range(2))
                    parts.append(jnp.where(first, one, turn(two, n)))
            return rows_of(parts)

        def low_inv(b):
            acc = [inv[b, qc, :, rows(0, 1)] for qc in range(2)]
            for qc in range(2):
                for p in pairs[1:]:
                    acc[qc] = acc[qc] + inv[b, qc, :, rows(p, 1)]
            return turn(acc[0].reshape(2 * n, 128), -n) + acc[1].reshape(2 * n, 128)

        def temp_rows(temp):
            temp = temp.reshape(shape)
            return rows_of([jnp.where(pair[p], temp[q], 0.0).reshape(n, 128) for p in pairs for q in range(2)])

        def product(lefts, rights):
            if len(lefts) == 1:
                return hdot(lefts[0], rights[0])
            return hdot(jnp.concatenate(lefts, axis=1), twin(*rights))

        two_blocks = (group[:2], group[2:])
        temps = [product([low_left(b) for b in bs], [up_inv(b) for b in bs]) for bs in two_blocks]
        for bs, temp in zip(two_blocks, temps):
            prod = -product([low_inv(b) for b in bs],
                            [temp_rows(temp[:, 128 * h:128 * h + 128]) for h in range(len(bs))])
            for h, b in enumerate(bs):
                piece = prod[:, 128 * h:128 * h + 128]
                for qc, val in enumerate((piece, turn(piece, -n))):
                    val = val.reshape(shape)
                    for p in pairs:
                        inv[b, qc, :, rows(p, 1)] = jnp.where(even[p], val, inv[b, qc, :, rows(p, 1)])

    zst = [None] * 6

    def z_diag(j):
        return both(lambda qc: inv[j, qc, c, :, x].reshape(64, 128))

    def emit(i, j, blk):
        out[64 * i:64 * i + 64, 128 * j:128 * j + 128] = blk

    def add_terms(j, ks, acc):
        for k in ks:
            prod = hdot(zst[k], low_block(k, j))
            for i in range(k, 6):
                part = prod[64 * (i - k):64 * (i - k) + 64]
                acc[i] = part if acc[i] is None else acc[i] + part

    def finish(j, acc):
        emit(j, j, inv[j, y, c, :, x].reshape(64, 128))
        if j == 5:
            zst[5] = z_diag(5)
            return
        res = -hdot(rows_of(acc[j + 1:]), inv_full(j))
        zst[j] = rows_of([z_diag(j), res])
        mine = jnp.where(y == 0, res[:, 0:128], res[:, 128:256])
        for i in range(j + 1, 6):
            emit(i, j, mine[64 * (i - j - 1):64 * (i - j)])

    def finish_first(acc, lo, hi):
        res = -hdot(rows_of(acc[lo:hi]), inv[0, y].reshape(256, 128))
        for i in range(lo, hi):
            emit(i, 0, res[64 * (i - lo):64 * (i - lo) + 64])

    def inverses(g):
        unpack(g)
        base(min(DIAG[g]))
        for w in (1, 2, 4):
            double(DIAG[g], w)

    def u_compute(j):
        acc = [None] * 6
        for k in (3, 4, 5):
            prod = hdot(zst[k], cbuf[j, k - 3].reshape(256, 128))
            for i in range(k, 6):
                part = prod[64 * (i - k):64 * (i - k) + 64]
                acc[i] = part if acc[i] is None else acc[i] + part
        for i in (3, 4, 5):
            ubuf[j, y, 64 * (i - 3):64 * (i - 3) + 64] = acc[i]

    def u_add(j, acc):
        for i in (3, 4, 5):
            part = both(lambda q: ubuf[j, q, 64 * (i - 3):64 * (i - 3) + 64])
            acc[i] = part if acc[i] is None else acc[i] + part

    pack(DB)
    pl.semaphore_wait(barrier, 3)
    own(DB, "xys")
    ready(BO)
    own(BO, "xys")
    pack(DA)
    own(DA, "xs")
    c_own(2)
    for i in range(5):
        out[64 * i:64 * i + 64, 128 * (i + 1):768] = jnp.zeros((64, 128 * (5 - i)), F32)
    from_x(DB)
    own(DA, "y")
    from_y(DB)
    c_own(1)
    c_own(0)
    from_x(BO)
    from_y(BO)
    from_x(DA)
    ready(AO)
    own(AO, "xys")
    from_diag(DB)
    wait_sib(DB)
    unpack(DB)
    base(3)
    from_y(DA)
    c_relay(2)
    double(DIAG[DB], 1)
    from_diag(BO)
    double(DIAG[DB], 2)
    c_relay(1)
    double(DIAG[DB], 4)
    from_diag(DA)
    wait_sib(BO)
    finish(5, None)
    acc = [None] * 6
    add_terms(4, (5,), acc)
    finish(4, acc)
    acc = [None] * 6
    add_terms(3, (5, 4), acc)
    finish(3, acc)
    c_relay(0)
    wait_sib(DA)
    c_wait(2)
    unpack(DA)
    u_compute(2)
    base(0)
    u_send_to(2)
    c_wait(1)
    u_compute(1)
    double(DIAG[DA], 1)
    u_send_to(1)
    from_y(AO)
    c_wait(0)
    u_compute(0)
    double(DIAG[DA], 2)
    u_send_to(0)
    from_x(AO)
    double(DIAG[DA], 4)
    from_diag(AO)
    emit(0, 0, inv[0, y, c, :, x].reshape(64, 128))
    u_wait(2)
    acc = [None] * 6
    u_add(2, acc)
    finish(2, acc)
    wait_sib(AO)
    acc = [None] * 6
    add_terms(1, (2,), acc)
    u_wait(1)
    u_add(1, acc)
    finish(1, acc)
    acc = [None] * 6
    add_terms(0, (2, 1), acc)
    finish_first(acc, 1, 3)
    u_wait(0)
    u_add(0, acc)
    finish_first(acc, 3, 6)

    for cp in sends:
        cp.wait_send()


def solution(mesh):
    spec = P(("batch", "row"), "col")

    def body(local_l):
        rows, cols = local_l.shape
        return pl.pallas_call(
            kernel,
            out_shape=jax.ShapeDtypeStruct((rows, cols), F32),
            in_specs=[pl.BlockSpec(memory_space=pltpu.HBM)],
            out_specs=pl.BlockSpec(memory_space=pltpu.VMEM),
            scratch_shapes=[
                pltpu.VMEM((6, 8, 8, 128), F32),
                pltpu.VMEM((2, 2, 2, 2, 15, 8, 128), F32),
                pltpu.VMEM((6, 2, 2, 8, 2, 8, 128), F32),
                pltpu.VMEM((6, 2, 2, 8, 2, 8, 128), F32),
                pltpu.VMEM((3, 3, 2, 8, 2, 8, 128), F32),
                pltpu.VMEM((3, 2, 192, 128), F32),
                pltpu.VMEM((6, 2, 2, 8, 2, 8, 128), F32),
                pltpu.SemaphoreType.DMA((21,)),
                pltpu.SemaphoreType.DMA((4, 7)),
                pltpu.SemaphoreType.DMA((4, 7)),
                pltpu.SemaphoreType.DMA((3, 3)),
                pltpu.SemaphoreType.DMA((3, 3)),
                pltpu.SemaphoreType.DMA((3,)),
                pltpu.SemaphoreType.DMA((3,)),
            ],
            compiler_params=pltpu.CompilerParams(
                collective_id=0, has_side_effects=True, vmem_limit_bytes=40 * 1024 * 1024),
        )(pltpu.with_memory_space_constraint(local_l.reshape(rows // 8, 8, cols), pltpu.HBM))

    return jax.shard_map(body, mesh=mesh, in_specs=(spec,), out_specs=spec, check_vma=False)
```

```python
import jax
import jax.numpy as jnp
from jax import lax
from jax.experimental import pallas as pl
from jax.experimental.pallas import tpu as pltpu
from jax.sharding import PartitionSpec as P

MESH = pl.DeviceIdType.MESH
F32 = jnp.float32
DB, DA, BO, AO = range(4)
DIAG = {DB: (5, 4, 3), DA: (2, 1, 0)}
OFF = {BO: ((5, 4), (4, 3), (5, 3)), AO: ((2, 1), (1, 0), (2, 0))}
OFF_AT = {blk: 3 * (g - 2) + i for g, grp in OFF.items() for i, blk in enumerate(grp)}


CGRP = [[(4, j), (5, j)] for j in range(3)] + [[(3, j) for j in range(3)]]


def c_at(k, j):
    return 6 + j if k == 3 else 2 * j + k - 4


def hdot(left, right):
    return jnp.dot(left, right, precision=lax.Precision.HIGHEST, preferred_element_type=F32)


def kernel(inp, out, raw, dpk, dg, goff, cbuf, utop, ubuf, inv, loc_sem, g_send, g_recv, c_send, c_recv, u_send, u_recv):
    row = lax.axis_index("row")
    y = lax.axis_index("col")
    x = row // 2
    c = row % 2
    xo, yo, co = 1 - x, 1 - y, 1 - c
    sib = {"row": 2 * x + co}
    xnb = {"row": 2 * xo + c}
    ynb = {"col": yo}

    def take(bi, bj, dst, sem):
        return pltpu.make_async_copy(inp.at[pl.ds(8 * bi, 8), :, pl.ds(128 * bj, 128)], dst, sem)

    local = {g: [take(b, b, raw.at[b], loc_sem.at[b]) for b in DIAG[g]] for g in DIAG}
    for g in OFF:
        local[g] = [take(bi, bj, goff.at[OFF_AT[bi, bj], y, c, :, x], loc_sem.at[6 + OFF_AT[bi, bj]]) for bi, bj in OFF[g]]
    local_c = [[take(bi, bj, cbuf.at[c_at(bi, bj), c, :, x], loc_sem.at[12 + c_at(bi, bj)]) for bi, bj in grp] for grp in CGRP]
    for grp in (local[BO], local[DB], local[DA], local_c[3], local_c[1], local_c[2], local[AO], local_c[0]):
        for cp in grp:
            cp.start()

    barrier = pltpu.get_barrier_semaphore()
    for nbr in (sib, xnb, ynb):
        pl.semaphore_signal(barrier, inc=1, device_id=nbr, device_id_type=MESH)

    sub = lax.broadcasted_iota(jnp.int32, (8, 128), 0)
    lane = lax.broadcasted_iota(jnp.int32, (8, 128), 1)

    def lanes(shape):
        return lax.broadcasted_iota(jnp.int32, shape, len(shape) - 1)

    def along(tile, idx):
        return jnp.take_along_axis(tile, idx, axis=1, mode="promise_in_bounds")

    def turn(tile, n):
        return along(tile, (lanes(tile.shape) + (128 - n)) & 127)

    def pack(g):
        for cp in local[g]:
            cp.wait()
        for i, b in enumerate(DIAG[g]):
            dpk[g, y, c, x, 5 * i] = raw[b, 7]
            for p in range(3):
                n = 112 - 16 * p
                dpk[g, y, c, x, 5 * i + 1 + p] = jnp.where(lane < n, raw[b, 6 - p], turn(raw[b, p], n))
            dpk[g, y, c, x, 5 * i + 4] = raw[b, 3]

    def unpack(g):
        for i, b in enumerate(DIAG[g]):
            for qc in range(2):
                for lb in range(8):
                    if lb >= 3:
                        tiles = dpk[g, qc, :, :, 5 * i + 7 - lb]
                    else:
                        tiles = dpk[g, qc, :, :, 5 * i + 1 + lb].reshape(32, 128)
                        tiles = turn(tiles, 16 * (lb + 1)).reshape(2, 2, 8, 128)
                    dg[b, qc, :, lb] = tiles

    def slot(g, sx, sc, sy):
        if g in DIAG:
            return dpk.at[g, sy, sc, sx]
        return goff.at[pl.ds(3 * (g - 2), 3), sy, sc, :, sx]

    sends = []

    def copy(ref, send, recv, dev):
        return pltpu.make_async_remote_copy(ref, ref, send, recv, device_id=dev, device_id_type=MESH)

    def start(cp):
        cp.start()
        sends.append(cp)

    def gsend(g, k, ref, dev):
        start(copy(ref, g_send.at[g, k], g_recv.at[g, k], dev))

    def gwait(g, k, ref):
        copy(ref, g_send.at[g, k], g_recv.at[g, k], sib).wait_recv()

    def own(g, to):
        for k, dev in enumerate((xnb, ynb, sib)):
            if "xys"[k] in to:
                gsend(g, k, slot(g, x, c, y), dev)

    def ready(g):
        for cp in local[g]:
            cp.wait()

    def from_x(g):
        gwait(g, 0, slot(g, xo, c, y))
        if g != AO:
            gsend(g, 3, slot(g, xo, c, y), ynb)
        gsend(g, 4, slot(g, xo, c, y), sib)

    def from_y(g):
        gwait(g, 1, slot(g, x, c, yo))
        if g == AO:
            gsend(g, 3, slot(g, x, c, yo), xnb)
        gsend(g, 5, slot(g, x, c, yo), sib)

    def from_diag(g):
        gwait(g, 3, slot(g, xo, c, yo))
        gsend(g, 6, slot(g, xo, c, yo), sib)

    def wait_sib(g):
        gwait(g, 2, slot(g, x, co, y))
        gwait(g, 4, slot(g, xo, co, y))
        gwait(g, 5, slot(g, x, co, yo))
        gwait(g, 6, slot(g, xo, co, yo))

    def c_slot(g, sx, sc):
        return cbuf.at[pl.ds(c_at(*CGRP[g][0]), len(CGRP[g])), sc, :, sx]

    def c_own(g):
        for cp in local_c[g]:
            cp.wait()
        for k, dev in enumerate((xnb, sib)):
            start(copy(c_slot(g, x, c), c_send.at[g, k], c_recv.at[g, k], dev))

    def c_relay(g):
        copy(c_slot(g, xo, c), c_send.at[g, 0], c_recv.at[g, 0], sib).wait_recv()
        start(copy(c_slot(g, xo, c), c_send.at[g, 2], c_recv.at[g, 2], sib))

    def c_wait(g):
        copy(c_slot(g, x, co), c_send.at[g, 1], c_recv.at[g, 1], sib).wait_recv()
        copy(c_slot(g, xo, co), c_send.at[g, 2], c_recv.at[g, 2], sib).wait_recv()

    def u_slot(g, sy):
        return utop.at[sy] if g == 3 else ubuf.at[g, sy]

    def u_send_to(g):
        start(copy(u_slot(g, y), u_send.at[g], u_recv.at[g], ynb))

    def u_wait(g):
        copy(u_slot(g, yo), u_send.at[g], u_recv.at[g], ynb).wait_recv()

    def base(at):
        sub3 = lax.broadcasted_iota(jnp.int32, (3, 8, 128), 1)
        lane3 = lanes((3, 8, 128))
        seg3 = lane3 >> 4
        seg24 = lanes((24, 128)) & 112
        here = [(sub3 == (lane3 & 7)) & (((lane3 >> 3) & 1) == xr) for xr in range(2)]
        segs = [seg3 == lb for lb in range(8)]
        low = [[None, None] for _ in range(4)]
        for nb in range(4):
            xr, qr = nb // 2, nb % 2
            for qc in range(2):
                acc = dg[at:at + 3, qc, qr, 0, xr]
                for lb in range(1, 8):
                    acc = jnp.where(segs[lb], dg[at:at + 3, qc, qr, lb, xr], acc)
                low[nb][qc] = acc
        rec = []
        for qc in range(2):
            dsum = jnp.where(here[0], low[qc][qc], 0.0) + jnp.where(here[1], low[2 + qc][qc], 0.0)
            rec.append(1.0 / jnp.sum(dsum, axis=1, keepdims=True))
        rhs = []
        for nb in range(4):
            for qc in range(2):
                low[nb][qc] = (low[nb][qc] * rec[qc]).reshape(24, 128)
            rhs.append([jnp.where(here[nb // 2], 1.0, 0.0) if nb % 2 == qc else jnp.zeros((3, 8, 128), F32)
                        for qc in range(2)])
        below = [sub3 > ek for ek in range(7)]
        for k in range(32):
            nk, ek = k // 8, k % 8
            xk, qk = nk // 2, nk % 2
            idx = seg24 + (8 * xk + ek)
            pivot = [rhs[nk][qc][:, ek:ek + 1, :] for qc in range(2)]
            for nb in range(nk, 4):
                if nb == nk and ek == 7:
                    continue
                col = along(low[nb][qk], idx).reshape(3, 8, 128)
                if nb == nk:
                    col = jnp.where(below[ek], col, 0.0)
                for qc in range(2):
                    rhs[nb][qc] = rhs[nb][qc] - col * pivot[qc]
        for nb in range(4):
            xr, qr = nb // 2, nb % 2
            idx = (seg3 * 16 + 8 * xr + sub3).reshape(24, 128)
            scale = along(jnp.broadcast_to(rec[qr], (3, 8, 128)).reshape(24, 128), idx).reshape(3, 8, 128)
            for qc in range(2):
                val = rhs[nb][qc] * scale
                for lb in range(8):
                    inv[at:at + 3, qc, qr, lb, xr] = jnp.where(segs[lb], val, 0.0)

    def both(ref_of):
        return jnp.concatenate([ref_of(0), ref_of(1)], axis=1)

    def inv_full(b):
        return both(lambda qc: inv[b, qc].reshape(256, 128))

    def low_block(k, j):
        return both(lambda qc: goff[OFF_AT[k, j], qc].reshape(256, 128))

    def rows_of(tiles):
        return jnp.concatenate(tiles, axis=0)

    def double(group, w):
        pairs = range(4 // w)
        n = 16 * w
        shift = {1: 4, 2: 5, 4: 6}[w]
        shape = (2, w, 2, 8, 128)
        part = lanes(shape) >> shift
        even = [part == 2 * p for p in pairs]
        pair = [(lanes((w, 2, 8, 128)) >> (shift + 1)) == p for p in pairs]
        zero = jnp.zeros(shape, F32)
        first = (lanes((n, 128)) & n) == 0
        hole = jnp.zeros((128, 128), F32)

        def rows(p, odd):
            return pl.ds((2 * p + odd) * w, w)

        def twin(one, two):
            return rows_of([both(lambda h: (one, hole)[h]), both(lambda h: (hole, two)[h])])

        def low_left(b):
            acc = [zero, zero]
            for qc in range(2):
                for p in pairs:
                    acc[qc] = jnp.where(even[p], dg[b, qc, :, rows(p, 1)], acc[qc])
            return acc[0].reshape(2 * n, 128) + turn(acc[1].reshape(2 * n, 128), n)

        def up_inv(b):
            parts = []
            for p in pairs:
                for q in range(2):
                    one, two = (inv[b, qc, q, rows(p, 0)].reshape(n, 128) for qc in range(2))
                    parts.append(jnp.where(first, one, turn(two, n)))
            return rows_of(parts)

        def low_inv(b):
            acc = [inv[b, qc, :, rows(0, 1)] for qc in range(2)]
            for qc in range(2):
                for p in pairs[1:]:
                    acc[qc] = acc[qc] + inv[b, qc, :, rows(p, 1)]
            return turn(acc[0].reshape(2 * n, 128), -n) + acc[1].reshape(2 * n, 128)

        def temp_rows(temp):
            temp = temp.reshape(shape)
            return rows_of([jnp.where(pair[p], temp[q], 0.0).reshape(n, 128) for p in pairs for q in range(2)])

        def product(lefts, rights):
            if len(lefts) == 1:
                return hdot(lefts[0], rights[0])
            return hdot(jnp.concatenate(lefts, axis=1), twin(*rights))

        two_blocks = (group[:2], group[2:])
        temps = [product([low_left(b) for b in bs], [up_inv(b) for b in bs]) for bs in two_blocks]
        for bs, temp in zip(two_blocks, temps):
            prod = -product([low_inv(b) for b in bs],
                            [temp_rows(temp[:, 128 * h:128 * h + 128]) for h in range(len(bs))])
            for h, b in enumerate(bs):
                piece = prod[:, 128 * h:128 * h + 128]
                for qc, val in enumerate((piece, turn(piece, -n))):
                    val = val.reshape(shape)
                    for p in pairs:
                        inv[b, qc, :, rows(p, 1)] = jnp.where(even[p], val, inv[b, qc, :, rows(p, 1)])

    zst = [None] * 6

    def z_diag(j):
        return both(lambda qc: inv[j, qc, c, :, x].reshape(64, 128))

    def emit(i, j, blk):
        out[64 * i:64 * i + 64, 128 * j:128 * j + 128] = blk

    def add_terms(j, ks, acc):
        for k in ks:
            prod = hdot(zst[k], low_block(k, j))
            for i in range(k, 6):
                part = prod[64 * (i - k):64 * (i - k) + 64]
                acc[i] = part if acc[i] is None else acc[i] + part

    def finish(j, acc):
        emit(j, j, inv[j, y, c, :, x].reshape(64, 128))
        if j == 5:
            zst[5] = z_diag(5)
            return
        res = -hdot(rows_of(acc[j + 1:]), inv_full(j))
        zst[j] = rows_of([z_diag(j), res])
        mine = jnp.where(y == 0, res[:, 0:128], res[:, 128:256])
        for i in range(j + 1, 6):
            emit(i, j, mine[64 * (i - j - 1):64 * (i - j)])

    def finish_first(acc, lo, hi):
        res = -hdot(rows_of(acc[lo:hi]), inv[0, y].reshape(256, 128))
        for i in range(lo, hi):
            emit(i, 0, res[64 * (i - lo):64 * (i - lo) + 64])

    def inverses(g):
        unpack(g)
        base(min(DIAG[g]))
        for w in (1, 2, 4):
            double(DIAG[g], w)

    def c_block(k, j):
        return cbuf[c_at(k, j)].reshape(256, 128)

    def u_compute_top():
        prod = hdot(z_diag(3), jnp.concatenate([c_block(3, j) for j in range(3)], axis=1))
        for j in range(3):
            utop[y, j] = prod[:, 128 * j:128 * j + 128]

    def u_compute(j):
        both_rows = hdot(zst[3][64:192], c_block(3, j)) + hdot(zst[4], c_block(4, j))
        ubuf[j, y, 0:64] = both_rows[0:64]
        ubuf[j, y, 64:128] = both_rows[64:128] + hdot(zst[5], c_block(5, j))

    def u_add(j, acc):
        parts = {3: both(lambda q: utop[q, j]), 4: both(lambda q: ubuf[j, q, 0:64]), 5: both(lambda q: ubuf[j, q, 64:128])}
        for i, part in parts.items():
            acc[i] = part if acc[i] is None else acc[i] + part

    ready(BO)
    pl.semaphore_wait(barrier, 3)
    own(BO, "y")
    pack(DB)
    own(DB, "xy")
    own(BO, "x")
    pack(DA)
    for i in range(5):
        out[64 * i:64 * i + 64, 128 * (i + 1):768] = jnp.zeros((64, 128 * (5 - i)), F32)
    own(DB, "s")
    from_x(DB)
    own(DA, "xs")
    own(BO, "s")
    c_own(3)
    own(DA, "y")
    from_y(BO)
    from_x(BO)
    from_y(DB)
    from_diag(DB)
    c_own(1)
    from_x(DA)
    c_own(2)
    ready(AO)
    own(AO, "ys")
    wait_sib(DB)
    unpack(DB)
    base(3)
    c_own(0)
    double(DIAG[DB], 1)
    c_relay(3)
    double(DIAG[DB], 2)
    from_diag(BO)
    double(DIAG[DB], 4)
    c_wait(3)
    from_y(DA)
    own(AO, "x")
    u_compute_top()
    u_send_to(3)
    from_diag(DA)
    c_relay(2)
    wait_sib(BO)
    c_relay(1)
    finish(5, None)
    acc = [None] * 6
    add_terms(4, (5,), acc)
    finish(4, acc)
    acc = [None] * 6
    add_terms(3, (5, 4), acc)
    finish(3, acc)
    wait_sib(DA)
    c_wait(2)
    c_relay(0)
    from_y(AO)
    unpack(DA)
    u_compute(2)
    base(0)
    u_send_to(2)
    c_wait(1)
    u_compute(1)
    double(DIAG[DA], 1)
    u_send_to(1)
    c_wait(0)
    from_x(AO)
    u_compute(0)
    double(DIAG[DA], 2)
    u_send_to(0)
    double(DIAG[DA], 4)
    from_diag(AO)
    emit(0, 0, inv[0, y, c, :, x].reshape(64, 128))
    u_wait(3)
    u_wait(2)
    acc = [None] * 6
    u_add(2, acc)
    finish(2, acc)
    wait_sib(AO)
    acc = [None] * 6
    add_terms(1, (2,), acc)
    first = [None] * 6
    add_terms(0, (2,), first)
    u_wait(1)
    u_add(1, acc)
    finish(1, acc)
    add_terms(0, (1,), first)
    u_wait(0)
    u_add(0, first)
    finish_first(first, 1, 6)

    for cp in sends:
        cp.wait_send()


def solution(mesh):
    spec = P(("batch", "row"), "col")

    def body(local_l):
        rows, cols = local_l.shape
        return pl.pallas_call(
            kernel,
            out_shape=jax.ShapeDtypeStruct((rows, cols), F32),
            in_specs=[pl.BlockSpec(memory_space=pltpu.HBM)],
            out_specs=pl.BlockSpec(memory_space=pltpu.VMEM),
            scratch_shapes=[
                pltpu.VMEM((6, 8, 8, 128), F32),
                pltpu.VMEM((2, 2, 2, 2, 15, 8, 128), F32),
                pltpu.VMEM((6, 2, 2, 8, 2, 8, 128), F32),
                pltpu.VMEM((6, 2, 2, 8, 2, 8, 128), F32),
                pltpu.VMEM((9, 2, 8, 2, 8, 128), F32),
                pltpu.VMEM((2, 3, 64, 128), F32),
                pltpu.VMEM((3, 2, 128, 128), F32),
                pltpu.VMEM((6, 2, 2, 8, 2, 8, 128), F32),
                pltpu.SemaphoreType.DMA((21,)),
                pltpu.SemaphoreType.DMA((4, 7)),
                pltpu.SemaphoreType.DMA((4, 7)),
                pltpu.SemaphoreType.DMA((4, 3)),
                pltpu.SemaphoreType.DMA((4, 3)),
                pltpu.SemaphoreType.DMA((4,)),
                pltpu.SemaphoreType.DMA((4,)),
            ],
            compiler_params=pltpu.CompilerParams(
                collective_id=0, has_side_effects=True, vmem_limit_bytes=40 * 1024 * 1024),
        )(pltpu.with_memory_space_constraint(local_l.reshape(rows // 8, 8, cols), pltpu.HBM))

    return jax.shard_map(body, mesh=mesh, in_specs=(spec,), out_specs=spec, check_vma=False)
```

```python
import jax
import jax.numpy as jnp
from jax import lax
from jax.experimental import pallas as pl
from jax.experimental.pallas import tpu as pltpu
from jax.sharding import PartitionSpec as P

MESH = pl.DeviceIdType.MESH
F32 = jnp.float32
DB, DA, BO, A1, A2 = range(5)
DIAG = {DB: (5, 4, 3), DA: (2, 1, 0)}
OFF = {BO: ((5, 4), (4, 3), (5, 3)), A1: ((2, 1),), A2: ((1, 0), (2, 0))}
OFF_AT = {blk: n for n, blk in enumerate(blk for grp in OFF.values() for blk in grp)}
VIA = {DB: "y", DA: "y", BO: "y", A1: "x", A2: "x"}


CGRP = [[(4, j), (5, j)] for j in range(3)] + [[(3, j) for j in range(3)]]


def c_at(k, j):
    return 6 + j if k == 3 else 2 * j + k - 4


def hdot(left, right):
    return jnp.dot(left, right, precision=lax.Precision.HIGHEST, preferred_element_type=F32)


def kernel(inp, out, raw, dpk, dg, goff, cbuf, utop, ubuf, inv, loc_sem, g_send, g_recv, c_send, c_recv, u_send, u_recv):
    row = lax.axis_index("row")
    y = lax.axis_index("col")
    x = row // 2
    c = row % 2
    xo, yo, co = 1 - x, 1 - y, 1 - c
    sib = {"row": 2 * x + co}
    xnb = {"row": 2 * xo + c}
    ynb = {"col": yo}

    def take(bi, bj, dst, sem):
        return pltpu.make_async_copy(inp.at[pl.ds(8 * bi, 8), :, pl.ds(128 * bj, 128)], dst, sem)

    local = {g: [take(b, b, raw.at[b], loc_sem.at[b]) for b in DIAG[g]] for g in DIAG}
    for g in OFF:
        local[g] = [take(bi, bj, goff.at[OFF_AT[bi, bj], y, c, :, x], loc_sem.at[6 + OFF_AT[bi, bj]]) for bi, bj in OFF[g]]
    local_c = [[take(bi, bj, cbuf.at[c_at(bi, bj), c, :, x], loc_sem.at[12 + c_at(bi, bj)]) for bi, bj in grp] for grp in CGRP]
    for grp in (local[DB], local[BO], local[DA], local_c[3], local_c[2], local[A1], local_c[1], local_c[0], local[A2]):
        for cp in grp:
            cp.start()

    barrier = pltpu.get_barrier_semaphore()
    for nbr in (sib, xnb, ynb):
        pl.semaphore_signal(barrier, inc=1, device_id=nbr, device_id_type=MESH)

    sub = lax.broadcasted_iota(jnp.int32, (8, 128), 0)
    lane = lax.broadcasted_iota(jnp.int32, (8, 128), 1)

    def lanes(shape):
        return lax.broadcasted_iota(jnp.int32, shape, len(shape) - 1)

    def along(tile, idx):
        return jnp.take_along_axis(tile, idx, axis=1, mode="promise_in_bounds")

    def turn(tile, n):
        return along(tile, (lanes(tile.shape) + (128 - n)) & 127)

    def pack(g):
        for cp in local[g]:
            cp.wait()
        for i, b in enumerate(DIAG[g]):
            dpk[g, y, c, x, 5 * i] = raw[b, 7]
            for p in range(3):
                n = 112 - 16 * p
                dpk[g, y, c, x, 5 * i + 1 + p] = jnp.where(lane < n, raw[b, 6 - p], turn(raw[b, p], n))
            dpk[g, y, c, x, 5 * i + 4] = raw[b, 3]

    def unpack(g):
        for i, b in enumerate(DIAG[g]):
            for qc in range(2):
                for lb in range(8):
                    if lb >= 3:
                        tiles = dpk[g, qc, :, :, 5 * i + 7 - lb]
                    else:
                        tiles = dpk[g, qc, :, :, 5 * i + 1 + lb].reshape(32, 128)
                        tiles = turn(tiles, 16 * (lb + 1)).reshape(2, 2, 8, 128)
                    dg[b, qc, :, lb] = tiles

    def slot(g, sx, sc, sy, half=None):
        if g in DIAG:
            lo, num = (0, 15) if half is None else ((0, 8), (8, 7))[half]
            return dpk.at[g, sy, sc, sx, pl.ds(lo, num)]
        lo, num = (0, 8) if half is None else (4 * half, 4)
        return goff.at[pl.ds(OFF_AT[OFF[g][0]], len(OFF[g])), sy, sc, pl.ds(lo, num), sx]

    sends = []

    def copy(ref, send, recv, dev):
        return pltpu.make_async_remote_copy(ref, ref, send, recv, device_id=dev, device_id_type=MESH)

    def start(cp):
        cp.start()
        sends.append(cp)

    def gsend(g, k, ref, dev):
        start(copy(ref, g_send.at[g, k], g_recv.at[g, k], dev))

    def gwait(g, k, ref):
        copy(ref, g_send.at[g, k], g_recv.at[g, k], sib).wait_recv()

    def own(g, to):
        for k, dev in enumerate((xnb, ynb, sib)):
            if "xys"[k] in to:
                gsend(g, k, slot(g, x, c, y), dev)

    def ready(g):
        for cp in local[g]:
            cp.wait()

    def from_x(g):
        gwait(g, 0, slot(g, xo, c, y))
        if VIA[g] != "x":
            gsend(g, 3, slot(g, xo, c, y, 0 if VIA[g] == "h" else None), ynb)
        gsend(g, 4, slot(g, xo, c, y), sib)

    def from_y(g):
        gwait(g, 1, slot(g, x, c, yo))
        if VIA[g] == "x":
            gsend(g, 3, slot(g, x, c, yo), xnb)
        elif VIA[g] == "h":
            gsend(g, 7, slot(g, x, c, yo, 1), xnb)
        gsend(g, 5, slot(g, x, c, yo), sib)

    def diag_parts(g):
        return ((3, 6, 0), (7, 8, 1)) if VIA[g] == "h" else ((3, 6, None),)

    def from_diag(g):
        for got, to, half in diag_parts(g):
            gwait(g, got, slot(g, xo, c, yo, half))
            gsend(g, to, slot(g, xo, c, yo, half), sib)

    def wait_sib(g):
        gwait(g, 2, slot(g, x, co, y))
        gwait(g, 4, slot(g, xo, co, y))
        gwait(g, 5, slot(g, x, co, yo))
        for got, to, half in diag_parts(g):
            gwait(g, to, slot(g, xo, co, yo, half))

    def c_slot(g, sx, sc):
        return cbuf.at[pl.ds(c_at(*CGRP[g][0]), len(CGRP[g])), sc, :, sx]

    def c_own(g):
        for cp in local_c[g]:
            cp.wait()
        for k, dev in enumerate((xnb, sib)):
            start(copy(c_slot(g, x, c), c_send.at[g, k], c_recv.at[g, k], dev))

    def c_relay(g):
        copy(c_slot(g, xo, c), c_send.at[g, 0], c_recv.at[g, 0], sib).wait_recv()
        start(copy(c_slot(g, xo, c), c_send.at[g, 2], c_recv.at[g, 2], sib))

    def c_wait(g):
        copy(c_slot(g, x, co), c_send.at[g, 1], c_recv.at[g, 1], sib).wait_recv()
        copy(c_slot(g, xo, co), c_send.at[g, 2], c_recv.at[g, 2], sib).wait_recv()

    def u_slot(g, sy):
        return utop.at[sy] if g == 3 else ubuf.at[g, sy]

    def u_send_to(g):
        start(copy(u_slot(g, y), u_send.at[g], u_recv.at[g], ynb))

    def u_wait(g):
        copy(u_slot(g, yo), u_send.at[g], u_recv.at[g], ynb).wait_recv()

    def base(at):
        sub3 = lax.broadcasted_iota(jnp.int32, (3, 8, 128), 1)
        lane3 = lanes((3, 8, 128))
        seg3 = lane3 >> 4
        seg24 = lanes((24, 128)) & 112
        here = [(sub3 == (lane3 & 7)) & (((lane3 >> 3) & 1) == xr) for xr in range(2)]
        segs = [seg3 == lb for lb in range(8)]
        low = [[None, None] for _ in range(4)]
        for nb in range(4):
            xr, qr = nb // 2, nb % 2
            for qc in range(2):
                acc = dg[at:at + 3, qc, qr, 0, xr]
                for lb in range(1, 8):
                    acc = jnp.where(segs[lb], dg[at:at + 3, qc, qr, lb, xr], acc)
                low[nb][qc] = acc
        rec = []
        for qc in range(2):
            dsum = jnp.where(here[0], low[qc][qc], 0.0) + jnp.where(here[1], low[2 + qc][qc], 0.0)
            rec.append(1.0 / jnp.sum(dsum, axis=1, keepdims=True))
        rhs = []
        for nb in range(4):
            for qc in range(2):
                low[nb][qc] = (low[nb][qc] * rec[qc]).reshape(24, 128)
            rhs.append([jnp.where(here[nb // 2], 1.0, 0.0) if nb % 2 == qc else jnp.zeros((3, 8, 128), F32)
                        for qc in range(2)])
        below = [sub3 > ek for ek in range(7)]
        for k in range(32):
            nk, ek = k // 8, k % 8
            xk, qk = nk // 2, nk % 2
            idx = seg24 + (8 * xk + ek)
            pivot = [rhs[nk][qc][:, ek:ek + 1, :] for qc in range(2)]
            for nb in range(nk, 4):
                if nb == nk and ek == 7:
                    continue
                col = along(low[nb][qk], idx).reshape(3, 8, 128)
                if nb == nk:
                    col = jnp.where(below[ek], col, 0.0)
                for qc in range(2):
                    rhs[nb][qc] = rhs[nb][qc] - col * pivot[qc]
        for nb in range(4):
            xr, qr = nb // 2, nb % 2
            idx = (seg3 * 16 + 8 * xr + sub3).reshape(24, 128)
            scale = along(jnp.broadcast_to(rec[qr], (3, 8, 128)).reshape(24, 128), idx).reshape(3, 8, 128)
            for qc in range(2):
                val = rhs[nb][qc] * scale
                for lb in range(8):
                    inv[at:at + 3, qc, qr, lb, xr] = jnp.where(segs[lb], val, 0.0)

    def both(ref_of):
        return jnp.concatenate([ref_of(0), ref_of(1)], axis=1)

    def inv_full(b):
        return both(lambda qc: inv[b, qc].reshape(256, 128))

    def low_block(k, j):
        return both(lambda qc: goff[OFF_AT[k, j], qc].reshape(256, 128))

    def rows_of(tiles):
        return jnp.concatenate(tiles, axis=0)

    def double(group, w):
        pairs = range(4 // w)
        n = 16 * w
        shift = {1: 4, 2: 5, 4: 6}[w]
        shape = (2, w, 2, 8, 128)
        part = lanes(shape) >> shift
        even = [part == 2 * p for p in pairs]
        pair = [(lanes((w, 2, 8, 128)) >> (shift + 1)) == p for p in pairs]
        zero = jnp.zeros(shape, F32)
        first = (lanes((n, 128)) & n) == 0
        hole = jnp.zeros((128, 128), F32)

        def rows(p, odd):
            return pl.ds((2 * p + odd) * w, w)

        def twin(one, two):
            return rows_of([both(lambda h: (one, hole)[h]), both(lambda h: (hole, two)[h])])

        def low_left(b):
            acc = [zero, zero]
            for qc in range(2):
                for p in pairs:
                    acc[qc] = jnp.where(even[p], dg[b, qc, :, rows(p, 1)], acc[qc])
            return acc[0].reshape(2 * n, 128) + turn(acc[1].reshape(2 * n, 128), n)

        def up_inv(b):
            parts = []
            for p in pairs:
                for q in range(2):
                    one, two = (inv[b, qc, q, rows(p, 0)].reshape(n, 128) for qc in range(2))
                    parts.append(jnp.where(first, one, turn(two, n)))
            return rows_of(parts)

        def low_inv(b):
            acc = [inv[b, qc, :, rows(0, 1)] for qc in range(2)]
            for qc in range(2):
                for p in pairs[1:]:
                    acc[qc] = acc[qc] + inv[b, qc, :, rows(p, 1)]
            return turn(acc[0].reshape(2 * n, 128), -n) + acc[1].reshape(2 * n, 128)

        def temp_rows(temp):
            temp = temp.reshape(shape)
            return rows_of([jnp.where(pair[p], temp[q], 0.0).reshape(n, 128) for p in pairs for q in range(2)])

        def product(lefts, rights):
            if len(lefts) == 1:
                return hdot(lefts[0], rights[0])
            return hdot(jnp.concatenate(lefts, axis=1), twin(*rights))

        here = [(lanes((w, 2, 8, 128)) >> shift) == 2 * p for p in pairs]

        def wide_rows(temp):
            temp = [temp[:, 128 * qc:128 * qc + 128].reshape(shape) for qc in range(2)]
            return rows_of([both(lambda qc: jnp.where(here[p], temp[qc][q], 0.0).reshape(n, 128))
                            for p in pairs for q in range(2)])

        if w < 4:
            temps = [hdot(low_left(b), rows_of([both(lambda qc: inv[b, qc, q, rows(p, 0)].reshape(n, 128))
                                                for p in pairs for q in range(2)])) for b in group]
            for b, temp in zip(group, temps):
                prod = -hdot(low_inv(b), wide_rows(temp))
                for qc in range(2):
                    val = prod[:, 128 * qc:128 * qc + 128].reshape(shape)
                    for p in pairs:
                        inv[b, qc, :, rows(p, 1)] = jnp.where(even[p], val, inv[b, qc, :, rows(p, 1)])
            return
        two_blocks = (group[:2], group[2:])
        temps = [product([low_left(b) for b in bs], [up_inv(b) for b in bs]) for bs in two_blocks]
        for bs, temp in zip(two_blocks, temps):
            prod = -product([low_inv(b) for b in bs],
                            [temp_rows(temp[:, 128 * h:128 * h + 128]) for h in range(len(bs))])
            for h, b in enumerate(bs):
                piece = prod[:, 128 * h:128 * h + 128]
                for qc, val in enumerate((piece, turn(piece, -n))):
                    val = val.reshape(shape)
                    for p in pairs:
                        inv[b, qc, :, rows(p, 1)] = jnp.where(even[p], val, inv[b, qc, :, rows(p, 1)])

    zst = [None] * 6

    def z_diag(j):
        return both(lambda qc: inv[j, qc, c, :, x].reshape(64, 128))

    def emit(i, j, blk):
        out[64 * i:64 * i + 64, 128 * j:128 * j + 128] = blk

    def add_terms(j, ks, acc):
        for k in ks:
            prod = hdot(zst[k], low_block(k, j))
            for i in range(k, 6):
                part = prod[64 * (i - k):64 * (i - k) + 64]
                acc[i] = part if acc[i] is None else acc[i] + part

    def finish(j, acc):
        emit(j, j, inv[j, y, c, :, x].reshape(64, 128))
        if j == 5:
            zst[5] = z_diag(5)
            return
        res = -hdot(rows_of(acc[j + 1:]), inv_full(j))
        zst[j] = rows_of([z_diag(j), res])
        mine = jnp.where(y == 0, res[:, 0:128], res[:, 128:256])
        for i in range(j + 1, 6):
            emit(i, j, mine[64 * (i - j - 1):64 * (i - j)])

    def finish_first(acc, lo, hi):
        res = -hdot(rows_of(acc[lo:hi]), inv[0, y].reshape(256, 128))
        for i in range(lo, hi):
            emit(i, 0, res[64 * (i - lo):64 * (i - lo) + 64])

    def c_block(k, j):
        return cbuf[c_at(k, j)].reshape(256, 128)

    def u_compute_top():
        prod = hdot(z_diag(3), jnp.concatenate([c_block(3, j) for j in range(3)], axis=1))
        for j in range(3):
            utop[y, j] = prod[:, 128 * j:128 * j + 128]

    def u_compute(j):
        both_rows = hdot(zst[3][64:192], c_block(3, j)) + hdot(zst[4], c_block(4, j))
        ubuf[j, y, 0:64] = both_rows[0:64]
        ubuf[j, y, 64:128] = both_rows[64:128] + hdot(zst[5], c_block(5, j))

    def u_add(j, acc):
        parts = {3: both(lambda q: utop[q, j]), 4: both(lambda q: ubuf[j, q, 0:64]), 5: both(lambda q: ubuf[j, q, 64:128])}
        for i, part in parts.items():
            acc[i] = part if acc[i] is None else acc[i] + part

    pack(DB)
    pl.semaphore_wait(barrier, 3)
    own(DB, "xy")
    ready(BO)
    own(BO, "sx")
    pack(DA)
    own(DA, "x")
    for i in range(5):
        out[64 * i:64 * i + 64, 128 * (i + 1):768] = jnp.zeros((64, 128 * (5 - i)), F32)
    own(DA, "s")
    ready(A1)
    own(A1, "s")
    c_own(3)
    own(BO, "y")
    own(DB, "s")
    c_own(2)
    from_x(DB)
    from_y(DB)
    own(DA, "y")
    from_y(BO)
    ready(A2)
    own(A2, "s")
    from_x(BO)
    from_diag(DB)
    c_own(1)
    own(A1, "x")
    c_own(0)
    from_x(DA)
    wait_sib(DB)
    unpack(DB)
    base(3)
    own(A2, "x")
    own(A1, "y")
    double(DIAG[DB], 1)
    own(A2, "y")
    c_relay(3)
    double(DIAG[DB], 2)
    from_diag(BO)
    double(DIAG[DB], 4)
    c_wait(3)
    from_y(DA)
    u_compute_top()
    u_send_to(3)
    wait_sib(BO)
    from_diag(DA)
    c_relay(2)
    c_relay(1)
    finish(5, None)
    acc = [None] * 6
    add_terms(4, (5,), acc)
    finish(4, acc)
    acc = [None] * 6
    add_terms(3, (5, 4), acc)
    finish(3, acc)
    wait_sib(DA)
    c_wait(2)
    unpack(DA)
    u_compute(2)
    base(0)
    u_send_to(2)
    from_y(A1)
    c_wait(1)
    from_x(A1)
    c_relay(0)
    from_y(A2)
    u_compute(1)
    double(DIAG[DA], 1)
    u_send_to(1)
    c_wait(0)
    u_compute(0)
    double(DIAG[DA], 2)
    from_x(A2)
    from_diag(A1)
    u_send_to(0)
    double(DIAG[DA], 4)
    emit(0, 0, inv[0, y, c, :, x].reshape(64, 128))
    u_wait(3)
    u_wait(2)
    acc = [None] * 6
    u_add(2, acc)
    finish(2, acc)
    from_diag(A2)
    wait_sib(A1)
    acc = [None] * 6
    add_terms(1, (2,), acc)
    u_wait(1)
    u_add(1, acc)
    finish(1, acc)
    wait_sib(A2)
    acc = [None] * 6
    add_terms(0, (2, 1), acc)
    acc[3] = acc[3] + both(lambda q: utop[q, 0])
    finish_first(acc, 1, 4)
    u_wait(0)
    u_add(0, acc)
    finish_first(acc, 4, 6)

    for cp in sends:
        cp.wait_send()


def solution(mesh):
    spec = P(("batch", "row"), "col")

    def body(local_l):
        rows, cols = local_l.shape
        return pl.pallas_call(
            kernel,
            out_shape=jax.ShapeDtypeStruct((rows, cols), F32),
            in_specs=[pl.BlockSpec(memory_space=pltpu.HBM)],
            out_specs=pl.BlockSpec(memory_space=pltpu.VMEM),
            scratch_shapes=[
                pltpu.VMEM((6, 8, 8, 128), F32),
                pltpu.VMEM((2, 2, 2, 2, 15, 8, 128), F32),
                pltpu.VMEM((6, 2, 2, 8, 2, 8, 128), F32),
                pltpu.VMEM((6, 2, 2, 8, 2, 8, 128), F32),
                pltpu.VMEM((9, 2, 8, 2, 8, 128), F32),
                pltpu.VMEM((2, 3, 64, 128), F32),
                pltpu.VMEM((3, 2, 128, 128), F32),
                pltpu.VMEM((6, 2, 2, 8, 2, 8, 128), F32),
                pltpu.SemaphoreType.DMA((21,)),
                pltpu.SemaphoreType.DMA((5, 9)),
                pltpu.SemaphoreType.DMA((5, 9)),
                pltpu.SemaphoreType.DMA((4, 3)),
                pltpu.SemaphoreType.DMA((4, 3)),
                pltpu.SemaphoreType.DMA((4,)),
                pltpu.SemaphoreType.DMA((4,)),
            ],
            compiler_params=pltpu.CompilerParams(
                collective_id=0, has_side_effects=True, vmem_limit_bytes=40 * 1024 * 1024),
        )(pltpu.with_memory_space_constraint(local_l.reshape(rows // 8, 8, cols), pltpu.HBM))

    return jax.shard_map(body, mesh=mesh, in_specs=(spec,), out_specs=spec, check_vma=False)
```

```python
import jax
import jax.numpy as jnp
from jax import lax
from jax.experimental import pallas as pl
from jax.experimental.pallas import tpu as pltpu
from jax.sharding import PartitionSpec as P

MESH = pl.DeviceIdType.MESH
F32 = jnp.float32
DB, DA, BO, A1, A2 = range(5)
DIAG = {DB: (5, 4, 3), DA: (2, 1, 0)}
OFF = {BO: ((5, 4), (4, 3), (5, 3)), A1: ((2, 1), (2, 0)), A2: ((1, 0),)}
OFF_AT = {blk: n for n, blk in enumerate(blk for grp in OFF.values() for blk in grp)}
LAST_X = (A1, A2,)


CGRP = [[(4, j), (5, j)] for j in range(3)] + [[(3, j) for j in range(3)]]


def c_at(k, j):
    return 6 + j if k == 3 else 2 * j + k - 4


def hdot(left, right):
    return jnp.dot(left, right, precision=lax.Precision.HIGHEST, preferred_element_type=F32)


def kernel(inp, out, raw, dpk, dg, goff, cbuf, utop, ubuf, inv, loc_sem, g_send, g_recv, c_send, c_recv, u_send, u_recv):
    row = lax.axis_index("row")
    y = lax.axis_index("col")
    x = row // 2
    c = row % 2
    xo, yo, co = 1 - x, 1 - y, 1 - c
    sib = {"row": 2 * x + co}
    xnb = {"row": 2 * xo + c}
    ynb = {"col": yo}

    def take(bi, bj, dst, sem):
        return pltpu.make_async_copy(inp.at[pl.ds(8 * bi, 8), :, pl.ds(128 * bj, 128)], dst, sem)

    local = {g: [take(b, b, raw.at[b], loc_sem.at[b]) for b in DIAG[g]] for g in DIAG}
    for g in OFF:
        local[g] = [take(bi, bj, goff.at[OFF_AT[bi, bj], y, c, :, x], loc_sem.at[6 + OFF_AT[bi, bj]]) for bi, bj in OFF[g]]
    local_c = [[take(bi, bj, cbuf.at[c_at(bi, bj), c, :, x], loc_sem.at[12 + c_at(bi, bj)]) for bi, bj in grp] for grp in CGRP]
    for grp in (local[DB], local[BO], local[DA], local_c[3], local_c[2], local[A1], local_c[1], local_c[0], local[A2]):
        for cp in grp:
            cp.start()

    barrier = pltpu.get_barrier_semaphore()
    for nbr in (sib, xnb, ynb):
        pl.semaphore_signal(barrier, inc=1, device_id=nbr, device_id_type=MESH)

    sub = lax.broadcasted_iota(jnp.int32, (8, 128), 0)
    lane = lax.broadcasted_iota(jnp.int32, (8, 128), 1)

    def lanes(shape):
        return lax.broadcasted_iota(jnp.int32, shape, len(shape) - 1)

    def along(tile, idx):
        return jnp.take_along_axis(tile, idx, axis=1, mode="promise_in_bounds")

    def turn(tile, n):
        return along(tile, (lanes(tile.shape) + (128 - n)) & 127)

    def pack(g):
        for cp in local[g]:
            cp.wait()
        for i, b in enumerate(DIAG[g]):
            dpk[g, y, c, x, 5 * i] = raw[b, 7]
            for p in range(3):
                n = 112 - 16 * p
                dpk[g, y, c, x, 5 * i + 1 + p] = jnp.where(lane < n, raw[b, 6 - p], turn(raw[b, p], n))
            dpk[g, y, c, x, 5 * i + 4] = raw[b, 3]

    def unpack(g):
        for i, b in enumerate(DIAG[g]):
            for qc in range(2):
                for lb in range(8):
                    if lb >= 3:
                        tiles = dpk[g, qc, :, :, 5 * i + 7 - lb]
                    else:
                        tiles = dpk[g, qc, :, :, 5 * i + 1 + lb].reshape(32, 128)
                        tiles = turn(tiles, 16 * (lb + 1)).reshape(2, 2, 8, 128)
                    dg[b, qc, :, lb] = tiles

    def slot(g, sx, sc, sy):
        if g in DIAG:
            return dpk.at[g, sy, sc, sx]
        return goff.at[pl.ds(OFF_AT[OFF[g][0]], len(OFF[g])), sy, sc, :, sx]

    sends = []

    def copy(ref, send, recv, dev):
        return pltpu.make_async_remote_copy(ref, ref, send, recv, device_id=dev, device_id_type=MESH)

    def start(cp):
        cp.start()
        sends.append(cp)

    def gsend(g, k, ref, dev):
        start(copy(ref, g_send.at[g, k], g_recv.at[g, k], dev))

    def gwait(g, k, ref):
        copy(ref, g_send.at[g, k], g_recv.at[g, k], sib).wait_recv()

    def own(g, to):
        for k, dev in enumerate((xnb, ynb, sib)):
            if "xys"[k] in to:
                gsend(g, k, slot(g, x, c, y), dev)

    def ready(g):
        for cp in local[g]:
            cp.wait()

    def from_x(g):
        gwait(g, 0, slot(g, xo, c, y))
        if g not in LAST_X:
            gsend(g, 3, slot(g, xo, c, y), ynb)
        gsend(g, 4, slot(g, xo, c, y), sib)

    def from_y(g):
        gwait(g, 1, slot(g, x, c, yo))
        if g in LAST_X:
            gsend(g, 3, slot(g, x, c, yo), xnb)
        gsend(g, 5, slot(g, x, c, yo), sib)

    def from_diag(g):
        gwait(g, 3, slot(g, xo, c, yo))
        gsend(g, 6, slot(g, xo, c, yo), sib)

    def wait_sib(g):
        for k, ref in ((2, slot(g, x, co, y)), (4, slot(g, xo, co, y)), (5, slot(g, x, co, yo)), (6, slot(g, xo, co, yo))):
            gwait(g, k, ref)

    def c_slot(g, sx, sc):
        return cbuf.at[pl.ds(c_at(*CGRP[g][0]), len(CGRP[g])), sc, :, sx]

    def c_own(g):
        for cp in local_c[g]:
            cp.wait()
        for k, dev in enumerate((xnb, sib)):
            start(copy(c_slot(g, x, c), c_send.at[g, k], c_recv.at[g, k], dev))

    def c_relay(g):
        copy(c_slot(g, xo, c), c_send.at[g, 0], c_recv.at[g, 0], sib).wait_recv()
        start(copy(c_slot(g, xo, c), c_send.at[g, 2], c_recv.at[g, 2], sib))

    def c_wait(g):
        copy(c_slot(g, x, co), c_send.at[g, 1], c_recv.at[g, 1], sib).wait_recv()
        copy(c_slot(g, xo, co), c_send.at[g, 2], c_recv.at[g, 2], sib).wait_recv()

    def u_slot(g, sy):
        return utop.at[sy] if g == 3 else ubuf.at[g, sy]

    def u_send_to(g):
        start(copy(u_slot(g, y), u_send.at[g], u_recv.at[g], ynb))

    def u_wait(g):
        copy(u_slot(g, yo), u_send.at[g], u_recv.at[g], ynb).wait_recv()

    def base(at):
        sub3 = lax.broadcasted_iota(jnp.int32, (3, 8, 128), 1)
        lane3 = lanes((3, 8, 128))
        seg3 = lane3 >> 4
        seg24 = lanes((24, 128)) & 112
        here = [(sub3 == (lane3 & 7)) & (((lane3 >> 3) & 1) == xr) for xr in range(2)]
        segs = [seg3 == lb for lb in range(8)]
        low = [[None, None] for _ in range(4)]
        for nb in range(4):
            xr, qr = nb // 2, nb % 2
            for qc in range(2):
                acc = dg[at:at + 3, qc, qr, 0, xr]
                for lb in range(1, 8):
                    acc = jnp.where(segs[lb], dg[at:at + 3, qc, qr, lb, xr], acc)
                low[nb][qc] = acc
        rec = []
        for qc in range(2):
            dsum = jnp.where(here[0], low[qc][qc], 0.0) + jnp.where(here[1], low[2 + qc][qc], 0.0)
            rec.append(1.0 / jnp.sum(dsum, axis=1, keepdims=True))
        rhs = []
        for nb in range(4):
            for qc in range(2):
                low[nb][qc] = (low[nb][qc] * rec[qc]).reshape(24, 128)
            rhs.append([jnp.where(here[nb // 2], 1.0, 0.0) if nb % 2 == qc else jnp.zeros((3, 8, 128), F32)
                        for qc in range(2)])
        below = [sub3 > ek for ek in range(7)]
        for k in range(32):
            nk, ek = k // 8, k % 8
            xk, qk = nk // 2, nk % 2
            idx = seg24 + (8 * xk + ek)
            pivot = [rhs[nk][qc][:, ek:ek + 1, :] for qc in range(2)]
            for nb in range(nk, 4):
                if nb == nk and ek == 7:
                    continue
                col = along(low[nb][qk], idx).reshape(3, 8, 128)
                if nb == nk:
                    col = jnp.where(below[ek], col, 0.0)
                for qc in range(2):
                    rhs[nb][qc] = rhs[nb][qc] - col * pivot[qc]
        for nb in range(4):
            xr, qr = nb // 2, nb % 2
            idx = (seg3 * 16 + 8 * xr + sub3).reshape(24, 128)
            scale = along(jnp.broadcast_to(rec[qr], (3, 8, 128)).reshape(24, 128), idx).reshape(3, 8, 128)
            for qc in range(2):
                val = rhs[nb][qc] * scale
                for lb in range(8):
                    inv[at:at + 3, qc, qr, lb, xr] = jnp.where(segs[lb], val, 0.0)

    def both(ref_of):
        return jnp.concatenate([ref_of(0), ref_of(1)], axis=1)

    def inv_full(b):
        return both(lambda qc: inv[b, qc].reshape(256, 128))

    def low_block(k, j):
        return both(lambda qc: goff[OFF_AT[k, j], qc].reshape(256, 128))

    def rows_of(tiles):
        return jnp.concatenate(tiles, axis=0)

    def double(group, w):
        pairs = range(4 // w)
        n = 16 * w
        shift = {1: 4, 2: 5, 4: 6}[w]
        shape = (2, w, 2, 8, 128)
        part = lanes(shape) >> shift
        even = [part == 2 * p for p in pairs]
        pair = [(lanes((w, 2, 8, 128)) >> (shift + 1)) == p for p in pairs]
        zero = jnp.zeros(shape, F32)
        first = (lanes((n, 128)) & n) == 0
        hole = jnp.zeros((128, 128), F32)

        def rows(p, odd):
            return pl.ds((2 * p + odd) * w, w)

        def twin(one, two):
            return rows_of([both(lambda h: (one, hole)[h]), both(lambda h: (hole, two)[h])])

        def low_left(b):
            acc = [zero, zero]
            for qc in range(2):
                for p in pairs:
                    acc[qc] = jnp.where(even[p], dg[b, qc, :, rows(p, 1)], acc[qc])
            return acc[0].reshape(2 * n, 128) + turn(acc[1].reshape(2 * n, 128), n)

        def up_inv(b):
            parts = []
            for p in pairs:
                for q in range(2):
                    one, two = (inv[b, qc, q, rows(p, 0)].reshape(n, 128) for qc in range(2))
                    parts.append(jnp.where(first, one, turn(two, n)))
            return rows_of(parts)

        def low_inv(b):
            acc = [inv[b, qc, :, rows(0, 1)] for qc in range(2)]
            for qc in range(2):
                for p in pairs[1:]:
                    acc[qc] = acc[qc] + inv[b, qc, :, rows(p, 1)]
            return turn(acc[0].reshape(2 * n, 128), -n) + acc[1].reshape(2 * n, 128)

        def temp_rows(temp):
            temp = temp.reshape(shape)
            return rows_of([jnp.where(pair[p], temp[q], 0.0).reshape(n, 128) for p in pairs for q in range(2)])

        def product(lefts, rights):
            if len(lefts) == 1:
                return hdot(lefts[0], rights[0])
            return hdot(jnp.concatenate(lefts, axis=1), twin(*rights))

        here = [(lanes((w, 2, 8, 128)) >> shift) == 2 * p for p in pairs]

        def wide_rows(temp):
            temp = [temp[:, 128 * qc:128 * qc + 128].reshape(shape) for qc in range(2)]
            return rows_of([both(lambda qc: jnp.where(here[p], temp[qc][q], 0.0).reshape(n, 128))
                            for p in pairs for q in range(2)])

        if w < 4:
            temps = [hdot(low_left(b), rows_of([both(lambda qc: inv[b, qc, q, rows(p, 0)].reshape(n, 128))
                                                for p in pairs for q in range(2)])) for b in group]
            for b, temp in zip(group, temps):
                prod = -hdot(low_inv(b), wide_rows(temp))
                for qc in range(2):
                    val = prod[:, 128 * qc:128 * qc + 128].reshape(shape)
                    for p in pairs:
                        inv[b, qc, :, rows(p, 1)] = jnp.where(even[p], val, inv[b, qc, :, rows(p, 1)])
            return
        two_blocks = (group[:2], group[2:])
        temps = [product([low_left(b) for b in bs], [up_inv(b) for b in bs]) for bs in two_blocks]
        for bs, temp in zip(two_blocks, temps):
            prod = -product([low_inv(b) for b in bs],
                            [temp_rows(temp[:, 128 * h:128 * h + 128]) for h in range(len(bs))])
            for h, b in enumerate(bs):
                piece = prod[:, 128 * h:128 * h + 128]
                for qc, val in enumerate((piece, turn(piece, -n))):
                    val = val.reshape(shape)
                    for p in pairs:
                        inv[b, qc, :, rows(p, 1)] = jnp.where(even[p], val, inv[b, qc, :, rows(p, 1)])

    zst = [None] * 6

    def z_diag(j):
        return both(lambda qc: inv[j, qc, c, :, x].reshape(64, 128))

    def emit(i, j, blk):
        out[64 * i:64 * i + 64, 128 * j:128 * j + 128] = blk

    def add_terms(j, ks, acc):
        for k in ks:
            prod = hdot(zst[k], low_block(k, j))
            for i in range(k, 6):
                part = prod[64 * (i - k):64 * (i - k) + 64]
                acc[i] = part if acc[i] is None else acc[i] + part

    def finish(j, acc):
        emit(j, j, inv[j, y, c, :, x].reshape(64, 128))
        if j == 5:
            zst[5] = z_diag(5)
            return
        res = -hdot(rows_of(acc[j + 1:]), inv_full(j))
        zst[j] = rows_of([z_diag(j), res])
        mine = jnp.where(y == 0, res[:, 0:128], res[:, 128:256])
        for i in range(j + 1, 6):
            emit(i, j, mine[64 * (i - j - 1):64 * (i - j)])

    def empty():
        return [None] * 6

    def finish_first(acc):
        res = -hdot(rows_of(acc[1:]), inv[0, y].reshape(256, 128))
        for i in range(1, 6):
            emit(i, 0, res[64 * (i - 1):64 * i])

    def c_block(k, j):
        return cbuf[c_at(k, j)].reshape(256, 128)

    def u_compute_top():
        prod = hdot(z_diag(3), jnp.concatenate([c_block(3, j) for j in range(3)], axis=1))
        for j in range(3):
            utop[y, j] = prod[:, 128 * j:128 * j + 128]

    def u_compute(j):
        both_rows = hdot(zst[3][64:192], c_block(3, j)) + hdot(zst[4], c_block(4, j))
        ubuf[j, y, 0:64] = both_rows[0:64]
        ubuf[j, y, 64:128] = both_rows[64:128] + hdot(zst[5], c_block(5, j))

    def u_add(j, acc):
        parts = {3: both(lambda q: utop[q, j]), 4: both(lambda q: ubuf[j, q, 0:64]), 5: both(lambda q: ubuf[j, q, 64:128])}
        for i, part in parts.items():
            acc[i] = part if acc[i] is None else acc[i] + part

    pack(DB)
    pl.semaphore_wait(barrier, 3)
    own(DB, "yx")
    ready(BO)
    own(BO, "sx")
    own(DB, "s")
    own(BO, "y")
    from_x(DB)
    pack(DA)
    own(DA, "yx")
    from_y(DB)
    c_own(3)
    from_x(BO)
    c_own(2)
    own(DA, "s")
    c_own(0)
    for i in range(5):
        out[64 * i:64 * i + 64, 128 * (i + 1):768] = jnp.zeros((64, 128 * (5 - i)), F32)
    from_diag(DB)
    wait_sib(DB)
    from_y(DA)
    from_x(DA)
    unpack(DB)
    base(3)
    c_own(1)
    double(DIAG[DB], 1)
    ready(A1)
    own(A1, "y")
    from_y(BO)
    c_relay(3)
    double(DIAG[DB], 2)
    own(A1, "x")
    from_diag(BO)
    ready(A2)
    own(A2, "xy")
    double(DIAG[DB], 4)
    c_wait(3)
    u_compute_top()
    u_send_to(3)
    from_diag(DA)
    wait_sib(BO)
    c_relay(2)
    finish(5, None)
    acc = empty()
    add_terms(4, (5,), acc)
    finish(4, acc)
    acc = empty()
    add_terms(3, (5, 4), acc)
    finish(3, acc)
    c_relay(1)
    from_y(A1)
    c_relay(0)
    wait_sib(DA)
    c_wait(2)
    unpack(DA)
    u_compute(2)
    base(0)
    u_send_to(2)
    own(A1, "s")
    own(A2, "s")
    from_y(A2)
    c_wait(1)
    u_compute(1)
    double(DIAG[DA], 1)
    u_send_to(1)
    c_wait(0)
    from_x(A2)
    from_x(A1)
    u_compute(0)
    double(DIAG[DA], 2)
    u_send_to(0)
    from_diag(A1)
    double(DIAG[DA], 4)
    emit(0, 0, inv[0, y, c, :, x].reshape(64, 128))
    from_diag(A2)
    u_wait(3)
    u_wait(2)
    acc = empty()
    u_add(2, acc)
    finish(2, acc)
    wait_sib(A1)
    acc = empty()
    add_terms(1, (2,), acc)
    first = empty()
    add_terms(0, (2,), first)
    u_wait(1)
    wait_sib(A2)
    u_add(1, acc)
    finish(1, acc)
    add_terms(0, (1,), first)
    u_wait(0)
    u_add(0, first)
    finish_first(first)

    for cp in sends:
        cp.wait_send()


def solution(mesh):
    spec = P(("batch", "row"), "col")

    def body(local_l):
        rows, cols = local_l.shape
        return pl.pallas_call(
            kernel,
            out_shape=jax.ShapeDtypeStruct((rows, cols), F32),
            in_specs=[pl.BlockSpec(memory_space=pltpu.HBM)],
            out_specs=pl.BlockSpec(memory_space=pltpu.VMEM),
            scratch_shapes=[
                pltpu.VMEM((6, 8, 8, 128), F32),
                pltpu.VMEM((2, 2, 2, 2, 15, 8, 128), F32),
                pltpu.VMEM((6, 2, 2, 8, 2, 8, 128), F32),
                pltpu.VMEM((6, 2, 2, 8, 2, 8, 128), F32),
                pltpu.VMEM((9, 2, 8, 2, 8, 128), F32),
                pltpu.VMEM((2, 3, 64, 128), F32),
                pltpu.VMEM((3, 2, 128, 128), F32),
                pltpu.VMEM((6, 2, 2, 8, 2, 8, 128), F32),
                pltpu.SemaphoreType.DMA((21,)),
                pltpu.SemaphoreType.DMA((5, 7)),
                pltpu.SemaphoreType.DMA((5, 7)),
                pltpu.SemaphoreType.DMA((4, 3)),
                pltpu.SemaphoreType.DMA((4, 3)),
                pltpu.SemaphoreType.DMA((4,)),
                pltpu.SemaphoreType.DMA((4,)),
            ],
            compiler_params=pltpu.CompilerParams(
                collective_id=0, has_side_effects=True, vmem_limit_bytes=40 * 1024 * 1024),
        )(pltpu.with_memory_space_constraint(local_l.reshape(rows // 8, 8, cols), pltpu.HBM))

    return jax.shard_map(body, mesh=mesh, in_specs=(spec,), out_specs=spec, check_vma=False)
```

```python
import jax
import jax.numpy as jnp
from jax import lax
from jax.experimental import pallas as pl
from jax.experimental.pallas import tpu as pltpu
from jax.sharding import PartitionSpec as P

MESH = pl.DeviceIdType.MESH
F32 = jnp.float32
DB, DA, BO, A1, A2 = range(5)
DIAG = {DB: (5, 4, 3), DA: (2, 1, 0)}
OFF = {BO: ((5, 4), (4, 3), (5, 3)), A1: ((2, 1), (2, 0)), A2: ((1, 0),)}
OFF_AT = {blk: n for n, blk in enumerate(blk for grp in OFF.values() for blk in grp)}
LAST_X = (A1, A2,)


CGRP = [[(4, j), (5, j)] for j in range(3)] + [[(3, j) for j in range(3)]]


def c_at(k, j):
    return 6 + j if k == 3 else 2 * j + k - 4


def hdot(left, right):
    return jnp.dot(left, right, precision=lax.Precision.HIGHEST, preferred_element_type=F32)


def kernel(inp, out, raw, dpk, dg, goff, cbuf, utop, ubuf, inv, loc_sem, g_send, g_recv, c_send, c_recv, u_send, u_recv):
    row = lax.axis_index("row")
    y = lax.axis_index("col")
    x = row // 2
    c = row % 2
    xo, yo, co = 1 - x, 1 - y, 1 - c
    sib = {"row": 2 * x + co}
    xnb = {"row": 2 * xo + c}
    ynb = {"col": yo}

    barrier = pltpu.get_barrier_semaphore()
    for nbr in (sib, xnb, ynb):
        pl.semaphore_signal(barrier, inc=1, device_id=nbr, device_id_type=MESH)

    def take(bi, bj, dst, sem):
        return pltpu.make_async_copy(inp.at[pl.ds(8 * bi, 8), :, pl.ds(128 * bj, 128)], dst, sem)

    local = {g: [take(b, b, raw.at[b], loc_sem.at[b]) for b in DIAG[g]] for g in DIAG}
    for g in OFF:
        local[g] = [take(bi, bj, goff.at[OFF_AT[bi, bj], y, c, :, x], loc_sem.at[6 + OFF_AT[bi, bj]]) for bi, bj in OFF[g]]
    local_c = [[take(bi, bj, cbuf.at[c_at(bi, bj), c, :, x], loc_sem.at[12 + c_at(bi, bj)]) for bi, bj in grp] for grp in CGRP]
    for grp in (local[DB], local[BO], local[DA], local_c[3], local_c[2], local[A1], local_c[1], local_c[0], local[A2]):
        for cp in grp:
            cp.start()

    sub = lax.broadcasted_iota(jnp.int32, (8, 128), 0)
    lane = lax.broadcasted_iota(jnp.int32, (8, 128), 1)

    def lanes(shape):
        return lax.broadcasted_iota(jnp.int32, shape, len(shape) - 1)

    def along(tile, idx):
        return jnp.take_along_axis(tile, idx, axis=1, mode="promise_in_bounds")

    def turn(tile, n):
        return along(tile, (lanes(tile.shape) + (128 - n)) & 127)

    def pack(g):
        for cp in local[g]:
            cp.wait()
        for i, b in enumerate(DIAG[g]):
            dpk[g, y, c, x, 5 * i] = raw[b, 7]
            for p in range(3):
                n = 112 - 16 * p
                dpk[g, y, c, x, 5 * i + 1 + p] = jnp.where(lane < n, raw[b, 6 - p], turn(raw[b, p], n))
            dpk[g, y, c, x, 5 * i + 4] = raw[b, 3]

    def unpack(g):
        for i, b in enumerate(DIAG[g]):
            for qc in range(2):
                for lb in range(8):
                    if lb >= 3:
                        tiles = dpk[g, qc, :, :, 5 * i + 7 - lb]
                    else:
                        tiles = dpk[g, qc, :, :, 5 * i + 1 + lb].reshape(32, 128)
                        tiles = turn(tiles, 16 * (lb + 1)).reshape(2, 2, 8, 128)
                    dg[b, qc, :, lb] = tiles

    def slot(g, sx, sc, sy):
        if g in DIAG:
            return dpk.at[g, sy, sc, sx]
        return goff.at[pl.ds(OFF_AT[OFF[g][0]], len(OFF[g])), sy, sc, :, sx]

    sends = []

    def copy(ref, send, recv, dev):
        return pltpu.make_async_remote_copy(ref, ref, send, recv, device_id=dev, device_id_type=MESH)

    def start(cp):
        cp.start()
        sends.append(cp)

    def gsend(g, k, ref, dev):
        start(copy(ref, g_send.at[g, k], g_recv.at[g, k], dev))

    def gwait(g, k, ref):
        copy(ref, g_send.at[g, k], g_recv.at[g, k], sib).wait_recv()

    def own(g, to):
        for k, dev in enumerate((xnb, ynb, sib)):
            if "xys"[k] in to:
                gsend(g, k, slot(g, x, c, y), dev)

    def ready(g):
        for cp in local[g]:
            cp.wait()

    def from_x(g):
        gwait(g, 0, slot(g, xo, c, y))
        if g not in LAST_X:
            gsend(g, 3, slot(g, xo, c, y), ynb)
        gsend(g, 4, slot(g, xo, c, y), sib)

    def from_y(g):
        gwait(g, 1, slot(g, x, c, yo))
        if g in LAST_X:
            gsend(g, 3, slot(g, x, c, yo), xnb)
        gsend(g, 5, slot(g, x, c, yo), sib)

    def from_diag(g):
        gwait(g, 3, slot(g, xo, c, yo))
        gsend(g, 6, slot(g, xo, c, yo), sib)

    def wait_sib(g):
        for k, ref in ((2, slot(g, x, co, y)), (4, slot(g, xo, co, y)), (5, slot(g, x, co, yo)), (6, slot(g, xo, co, yo))):
            gwait(g, k, ref)

    def c_slot(g, sx, sc):
        return cbuf.at[pl.ds(c_at(*CGRP[g][0]), len(CGRP[g])), sc, :, sx]

    def c_own(g):
        for cp in local_c[g]:
            cp.wait()
        for k, dev in enumerate((xnb, sib)):
            start(copy(c_slot(g, x, c), c_send.at[g, k], c_recv.at[g, k], dev))

    def c_relay(g):
        copy(c_slot(g, xo, c), c_send.at[g, 0], c_recv.at[g, 0], sib).wait_recv()
        start(copy(c_slot(g, xo, c), c_send.at[g, 2], c_recv.at[g, 2], sib))

    def c_wait(g):
        copy(c_slot(g, x, co), c_send.at[g, 1], c_recv.at[g, 1], sib).wait_recv()
        copy(c_slot(g, xo, co), c_send.at[g, 2], c_recv.at[g, 2], sib).wait_recv()

    def u_slot(g, sy):
        return utop.at[sy] if g == 3 else ubuf.at[g, sy]

    def u_send_to(g):
        start(copy(u_slot(g, y), u_send.at[g], u_recv.at[g], ynb))

    def u_wait(g):
        copy(u_slot(g, yo), u_send.at[g], u_recv.at[g], ynb).wait_recv()

    def base(at):
        sub3 = lax.broadcasted_iota(jnp.int32, (3, 8, 128), 1)
        lane3 = lanes((3, 8, 128))
        seg3 = lane3 >> 4
        seg24 = lanes((24, 128)) & 112
        here = [(sub3 == (lane3 & 7)) & (((lane3 >> 3) & 1) == xr) for xr in range(2)]
        segs = [seg3 == lb for lb in range(8)]
        low = [[None, None] for _ in range(4)]
        for nb in range(4):
            xr, qr = nb // 2, nb % 2
            for qc in range(2):
                acc = dg[at:at + 3, qc, qr, 0, xr]
                for lb in range(1, 8):
                    acc = jnp.where(segs[lb], dg[at:at + 3, qc, qr, lb, xr], acc)
                low[nb][qc] = acc
        rec = []
        for qc in range(2):
            dsum = jnp.where(here[0], low[qc][qc], 0.0) + jnp.where(here[1], low[2 + qc][qc], 0.0)
            rec.append(1.0 / jnp.sum(dsum, axis=1, keepdims=True))
        rhs = []
        for nb in range(4):
            for qc in range(2):
                low[nb][qc] = (low[nb][qc] * rec[qc]).reshape(24, 128)
            rhs.append([jnp.where(here[nb // 2], 1.0, 0.0) if nb % 2 == qc else jnp.zeros((3, 8, 128), F32)
                        for qc in range(2)])
        below = [sub3 > ek for ek in range(7)]
        for k in range(32):
            nk, ek = k // 8, k % 8
            xk, qk = nk // 2, nk % 2
            idx = seg24 + (8 * xk + ek)
            pivot = [rhs[nk][qc][:, ek:ek + 1, :] for qc in range(2)]
            for nb in range(nk, 4):
                if nb == nk and ek == 7:
                    continue
                col = along(low[nb][qk], idx).reshape(3, 8, 128)
                if nb == nk:
                    col = jnp.where(below[ek], col, 0.0)
                for qc in range(2):
                    rhs[nb][qc] = rhs[nb][qc] - col * pivot[qc]
        for nb in range(4):
            xr, qr = nb // 2, nb % 2
            idx = (seg3 * 16 + 8 * xr + sub3).reshape(24, 128)
            scale = along(jnp.broadcast_to(rec[qr], (3, 8, 128)).reshape(24, 128), idx).reshape(3, 8, 128)
            for qc in range(2):
                val = rhs[nb][qc] * scale
                for lb in range(8):
                    inv[at:at + 3, qc, qr, lb, xr] = jnp.where(segs[lb], val, 0.0)

    def both(ref_of):
        return jnp.concatenate([ref_of(0), ref_of(1)], axis=1)

    def inv_full(b):
        return both(lambda qc: inv[b, qc].reshape(256, 128))

    def low_block(k, j):
        return both(lambda qc: goff[OFF_AT[k, j], qc].reshape(256, 128))

    def rows_of(tiles):
        return jnp.concatenate(tiles, axis=0)

    def double(group, w):
        pairs = range(4 // w)
        n = 16 * w
        shift = {1: 4, 2: 5, 4: 6}[w]
        shape = (2, w, 2, 8, 128)
        part = lanes(shape) >> shift
        even = [part == 2 * p for p in pairs]
        pair = [(lanes((w, 2, 8, 128)) >> (shift + 1)) == p for p in pairs]
        zero = jnp.zeros(shape, F32)
        first = (lanes((n, 128)) & n) == 0
        hole = jnp.zeros((128, 128), F32)

        def rows(p, odd):
            return pl.ds((2 * p + odd) * w, w)

        def twin(one, two):
            return rows_of([both(lambda h: (one, hole)[h]), both(lambda h: (hole, two)[h])])

        def low_left(b):
            acc = [zero, zero]
            for qc in range(2):
                for p in pairs:
                    acc[qc] = jnp.where(even[p], dg[b, qc, :, rows(p, 1)], acc[qc])
            return acc[0].reshape(2 * n, 128) + turn(acc[1].reshape(2 * n, 128), n)

        def up_inv(b):
            parts = []
            for p in pairs:
                for q in range(2):
                    one, two = (inv[b, qc, q, rows(p, 0)].reshape(n, 128) for qc in range(2))
                    parts.append(jnp.where(first, one, turn(two, n)))
            return rows_of(parts)

        def low_inv(b):
            acc = [inv[b, qc, :, rows(0, 1)] for qc in range(2)]
            for qc in range(2):
                for p in pairs[1:]:
                    acc[qc] = acc[qc] + inv[b, qc, :, rows(p, 1)]
            return turn(acc[0].reshape(2 * n, 128), -n) + acc[1].reshape(2 * n, 128)

        def temp_rows(temp):
            temp = temp.reshape(shape)
            return rows_of([jnp.where(pair[p], temp[q], 0.0).reshape(n, 128) for p in pairs for q in range(2)])

        def product(lefts, rights):
            if len(lefts) == 1:
                return hdot(lefts[0], rights[0])
            return hdot(jnp.concatenate(lefts, axis=1), twin(*rights))

        here = [(lanes((w, 2, 8, 128)) >> shift) == 2 * p for p in pairs]

        def wide_rows(temp):
            temp = [temp[:, 128 * qc:128 * qc + 128].reshape(shape) for qc in range(2)]
            return rows_of([both(lambda qc: jnp.where(here[p], temp[qc][q], 0.0).reshape(n, 128))
                            for p in pairs for q in range(2)])

        if w < 4:
            temps = [hdot(low_left(b), rows_of([both(lambda qc: inv[b, qc, q, rows(p, 0)].reshape(n, 128))
                                                for p in pairs for q in range(2)])) for b in group]
            for b, temp in zip(group, temps):
                prod = -hdot(low_inv(b), wide_rows(temp))
                for qc in range(2):
                    val = prod[:, 128 * qc:128 * qc + 128].reshape(shape)
                    for p in pairs:
                        inv[b, qc, :, rows(p, 1)] = jnp.where(even[p], val, inv[b, qc, :, rows(p, 1)])
            return
        two_blocks = (group[:2], group[2:])
        temps = [product([low_left(b) for b in bs], [up_inv(b) for b in bs]) for bs in two_blocks]
        for bs, temp in zip(two_blocks, temps):
            prod = -product([low_inv(b) for b in bs],
                            [temp_rows(temp[:, 128 * h:128 * h + 128]) for h in range(len(bs))])
            for h, b in enumerate(bs):
                piece = prod[:, 128 * h:128 * h + 128]
                for qc, val in enumerate((piece, turn(piece, -n))):
                    val = val.reshape(shape)
                    for p in pairs:
                        inv[b, qc, :, rows(p, 1)] = jnp.where(even[p], val, inv[b, qc, :, rows(p, 1)])

    zst = [None] * 6

    def z_diag(j):
        return both(lambda qc: inv[j, qc, c, :, x].reshape(64, 128))

    def emit(i, j, blk):
        out[64 * i:64 * i + 64, 128 * j:128 * j + 128] = blk

    def add_terms(j, ks, acc):
        for k in ks:
            prod = hdot(zst[k], low_block(k, j))
            for i in range(k, 6):
                part = prod[64 * (i - k):64 * (i - k) + 64]
                acc[i] = part if acc[i] is None else acc[i] + part

    def finish(j, acc):
        emit(j, j, inv[j, y, c, :, x].reshape(64, 128))
        if j == 5:
            zst[5] = z_diag(5)
            return
        res = -hdot(rows_of(acc[j + 1:]), inv_full(j))
        zst[j] = rows_of([z_diag(j), res])
        mine = jnp.where(y == 0, res[:, 0:128], res[:, 128:256])
        for i in range(j + 1, 6):
            emit(i, j, mine[64 * (i - j - 1):64 * (i - j)])

    def empty():
        return [None] * 6

    def finish_first(acc):
        res = -hdot(rows_of(acc[1:]), inv[0, y].reshape(256, 128))
        for i in range(1, 6):
            emit(i, 0, res[64 * (i - 1):64 * i])

    def c_block(k, j):
        return cbuf[c_at(k, j)].reshape(256, 128)

    def u_compute_top():
        prod = hdot(z_diag(3), jnp.concatenate([c_block(3, j) for j in range(3)], axis=1))
        for j in range(3):
            utop[y, j] = prod[:, 128 * j:128 * j + 128]

    def u_compute(j):
        both_rows = hdot(zst[3][64:192], c_block(3, j)) + hdot(zst[4], c_block(4, j))
        ubuf[j, y, 0:64] = both_rows[0:64]
        ubuf[j, y, 64:128] = both_rows[64:128] + hdot(zst[5], c_block(5, j))

    def u_add(j, acc):
        parts = {3: both(lambda q: utop[q, j]), 4: both(lambda q: ubuf[j, q, 0:64]), 5: both(lambda q: ubuf[j, q, 64:128])}
        for i, part in parts.items():
            acc[i] = part if acc[i] is None else acc[i] + part

    pack(DB)
    pl.semaphore_wait(barrier, 3)
    own(DB, "yx")
    ready(BO)
    own(BO, "yx")
    from_x(DB)
    pack(DA)
    own(DA, "x")
    c_own(3)
    own(BO, "s")
    own(DA, "s")
    ready(A2)
    own(A2, "s")
    c_own(2)
    c_own(1)
    from_y(DB)
    own(DA, "y")
    ready(A1)
    own(A1, "s")
    c_own(0)
    own(A2, "x")
    from_x(BO)
    for i in range(5):
        out[64 * i:64 * i + 64, 128 * (i + 1):768] = jnp.zeros((64, 128 * (5 - i)), F32)
    own(DB, "s")
    from_y(BO)
    from_diag(DB)
    from_x(DA)
    own(A1, "y")
    from_y(DA)
    own(A2, "y")
    wait_sib(DB)
    unpack(DB)
    base(3)
    double(DIAG[DB], 1)
    c_relay(3)
    double(DIAG[DB], 2)
    own(A1, "x")
    from_diag(BO)
    double(DIAG[DB], 4)
    c_wait(3)
    u_compute_top()
    c_relay(2)
    from_diag(DA)
    u_send_to(3)
    c_relay(1)
    wait_sib(BO)
    finish(5, None)
    acc = empty()
    add_terms(4, (5,), acc)
    finish(4, acc)
    acc = empty()
    add_terms(3, (5, 4), acc)
    finish(3, acc)
    wait_sib(DA)
    c_wait(2)
    from_y(A1)
    unpack(DA)
    u_compute(2)
    base(0)
    u_send_to(2)
    c_relay(0)
    from_y(A2)
    from_x(A2)
    c_wait(1)
    u_compute(1)
    double(DIAG[DA], 1)
    u_send_to(1)
    from_x(A1)
    c_wait(0)
    u_compute(0)
    double(DIAG[DA], 2)
    u_send_to(0)
    from_diag(A1)
    double(DIAG[DA], 4)
    emit(0, 0, inv[0, y, c, :, x].reshape(64, 128))
    from_diag(A2)
    u_wait(3)
    u_wait(2)
    acc = empty()
    u_add(2, acc)
    finish(2, acc)
    wait_sib(A1)
    acc = empty()
    add_terms(1, (2,), acc)
    first = empty()
    add_terms(0, (2,), first)
    u_wait(1)
    wait_sib(A2)
    u_add(1, acc)
    finish(1, acc)
    add_terms(0, (1,), first)
    u_wait(0)
    u_add(0, first)
    finish_first(first)

    for cp in sends:
        cp.wait_send()


def solution(mesh):
    spec = P(("batch", "row"), "col")

    def body(local_l):
        rows, cols = local_l.shape
        return pl.pallas_call(
            kernel,
            out_shape=jax.ShapeDtypeStruct((rows, cols), F32),
            in_specs=[pl.BlockSpec(memory_space=pltpu.HBM)],
            out_specs=pl.BlockSpec(memory_space=pltpu.VMEM),
            scratch_shapes=[
                pltpu.VMEM((6, 8, 8, 128), F32),
                pltpu.VMEM((2, 2, 2, 2, 15, 8, 128), F32),
                pltpu.VMEM((6, 2, 2, 8, 2, 8, 128), F32),
                pltpu.VMEM((6, 2, 2, 8, 2, 8, 128), F32),
                pltpu.VMEM((9, 2, 8, 2, 8, 128), F32),
                pltpu.VMEM((2, 3, 64, 128), F32),
                pltpu.VMEM((3, 2, 128, 128), F32),
                pltpu.VMEM((6, 2, 2, 8, 2, 8, 128), F32),
                pltpu.SemaphoreType.DMA((21,)),
                pltpu.SemaphoreType.DMA((5, 7)),
                pltpu.SemaphoreType.DMA((5, 7)),
                pltpu.SemaphoreType.DMA((4, 3)),
                pltpu.SemaphoreType.DMA((4, 3)),
                pltpu.SemaphoreType.DMA((4,)),
                pltpu.SemaphoreType.DMA((4,)),
            ],
            compiler_params=pltpu.CompilerParams(
                collective_id=0, has_side_effects=True, vmem_limit_bytes=40 * 1024 * 1024),
        )(pltpu.with_memory_space_constraint(local_l.reshape(rows // 8, 8, cols), pltpu.HBM))

    return jax.shard_map(body, mesh=mesh, in_specs=(spec,), out_specs=spec, check_vma=False)
```

```python
import jax
import jax.numpy as jnp
from jax import lax
from jax.experimental import pallas as pl
from jax.experimental.pallas import tpu as pltpu
from jax.sharding import PartitionSpec as P

MESH = pl.DeviceIdType.MESH
F32 = jnp.float32
DB, DA, BO, AO = range(4)
DIAG = {DB: (5, 4, 3), DA: (2, 1, 0)}
OFF = {BO: ((5, 4), (4, 3), (5, 3)), AO: ((2, 1), (1, 0), (2, 0))}
OFF_AT = {blk: 3 * (g - 2) + i for g, grp in OFF.items() for i, blk in enumerate(grp)}


CGRP = [[(4, j), (5, j)] for j in range(3)] + [[(3, j) for j in range(3)]]


def c_at(k, j):
    return 6 + j if k == 3 else 2 * j + k - 4


def hdot(left, right):
    return jnp.dot(left, right, precision=lax.Precision.HIGHEST, preferred_element_type=F32)


def kernel(inp, out, raw, dpk, dg, goff, cbuf, utop, ubuf, inv, loc_sem, g_send, g_recv, c_send, c_recv, u_send, u_recv):
    row = lax.axis_index("row")
    y = lax.axis_index("col")
    x = row // 2
    c = row % 2
    xo, yo, co = 1 - x, 1 - y, 1 - c
    sib = {"row": 2 * x + co}
    xnb = {"row": 2 * xo + c}
    ynb = {"col": yo}

    def take(bi, bj, dst, sem):
        return pltpu.make_async_copy(inp.at[pl.ds(8 * bi, 8), :, pl.ds(128 * bj, 128)], dst, sem)

    local = {g: [take(b, b, raw.at[b], loc_sem.at[b]) for b in DIAG[g]] for g in DIAG}
    for g in OFF:
        local[g] = [take(bi, bj, goff.at[OFF_AT[bi, bj], y, c, :, x], loc_sem.at[6 + OFF_AT[bi, bj]]) for bi, bj in OFF[g]]
    local_c = [[take(bi, bj, cbuf.at[c_at(bi, bj), c, :, x], loc_sem.at[12 + c_at(bi, bj)]) for bi, bj in grp] for grp in CGRP]
    for grp in (local[BO], local[DB], local[DA], local_c[3], local_c[1], local_c[2], local[AO], local_c[0]):
        for cp in grp:
            cp.start()

    barrier = pltpu.get_barrier_semaphore()
    for nbr in (sib, xnb, ynb):
        pl.semaphore_signal(barrier, inc=1, device_id=nbr, device_id_type=MESH)

    sub = lax.broadcasted_iota(jnp.int32, (8, 128), 0)
    lane = lax.broadcasted_iota(jnp.int32, (8, 128), 1)

    def lanes(shape):
        return lax.broadcasted_iota(jnp.int32, shape, len(shape) - 1)

    def along(tile, idx):
        return jnp.take_along_axis(tile, idx, axis=1, mode="promise_in_bounds")

    def turn(tile, n):
        return along(tile, (lanes(tile.shape) + (128 - n)) & 127)

    def pack(g):
        for cp in local[g]:
            cp.wait()
        for i, b in enumerate(DIAG[g]):
            dpk[g, y, c, x, 5 * i] = raw[b, 7]
            for p in range(3):
                n = 112 - 16 * p
                dpk[g, y, c, x, 5 * i + 1 + p] = jnp.where(lane < n, raw[b, 6 - p], turn(raw[b, p], n))
            dpk[g, y, c, x, 5 * i + 4] = raw[b, 3]

    def unpack(g):
        for i, b in enumerate(DIAG[g]):
            for qc in range(2):
                for lb in range(8):
                    if lb >= 3:
                        tiles = dpk[g, qc, :, :, 5 * i + 7 - lb]
                    else:
                        tiles = dpk[g, qc, :, :, 5 * i + 1 + lb].reshape(32, 128)
                        tiles = turn(tiles, 16 * (lb + 1)).reshape(2, 2, 8, 128)
                    dg[b, qc, :, lb] = tiles

    def slot(g, sx, sc, sy):
        if g in DIAG:
            return dpk.at[g, sy, sc, sx]
        return goff.at[pl.ds(3 * (g - 2), 3), sy, sc, :, sx]

    sends = []

    def copy(ref, send, recv, dev):
        return pltpu.make_async_remote_copy(ref, ref, send, recv, device_id=dev, device_id_type=MESH)

    def start(cp):
        cp.start()
        sends.append(cp)

    def gsend(g, k, ref, dev):
        start(copy(ref, g_send.at[g, k], g_recv.at[g, k], dev))

    def gwait(g, k, ref):
        copy(ref, g_send.at[g, k], g_recv.at[g, k], sib).wait_recv()

    def own(g, to):
        for k, dev in enumerate((xnb, ynb, sib)):
            if "xys"[k] in to:
                gsend(g, k, slot(g, x, c, y), dev)

    def ready(g):
        for cp in local[g]:
            cp.wait()

    def from_x(g):
        gwait(g, 0, slot(g, xo, c, y))
        if g != AO:
            gsend(g, 3, slot(g, xo, c, y), ynb)
        gsend(g, 4, slot(g, xo, c, y), sib)

    def from_y(g):
        gwait(g, 1, slot(g, x, c, yo))
        if g == AO:
            gsend(g, 3, slot(g, x, c, yo), xnb)
        gsend(g, 5, slot(g, x, c, yo), sib)

    def from_diag(g):
        gwait(g, 3, slot(g, xo, c, yo))
        gsend(g, 6, slot(g, xo, c, yo), sib)

    def wait_sib(g):
        gwait(g, 2, slot(g, x, co, y))
        gwait(g, 4, slot(g, xo, co, y))
        gwait(g, 5, slot(g, x, co, yo))
        gwait(g, 6, slot(g, xo, co, yo))

    def c_slot(g, sx, sc):
        return cbuf.at[pl.ds(c_at(*CGRP[g][0]), len(CGRP[g])), sc, :, sx]

    def c_own(g):
        for cp in local_c[g]:
            cp.wait()
        for k, dev in enumerate((xnb, sib)):
            start(copy(c_slot(g, x, c), c_send.at[g, k], c_recv.at[g, k], dev))

    def c_relay(g):
        copy(c_slot(g, xo, c), c_send.at[g, 0], c_recv.at[g, 0], sib).wait_recv()
        start(copy(c_slot(g, xo, c), c_send.at[g, 2], c_recv.at[g, 2], sib))

    def c_wait(g):
        copy(c_slot(g, x, co), c_send.at[g, 1], c_recv.at[g, 1], sib).wait_recv()
        copy(c_slot(g, xo, co), c_send.at[g, 2], c_recv.at[g, 2], sib).wait_recv()

    def u_slot(g, sy):
        return utop.at[sy] if g == 3 else ubuf.at[g, sy]

    def u_send_to(g):
        start(copy(u_slot(g, y), u_send.at[g], u_recv.at[g], ynb))

    def u_wait(g):
        copy(u_slot(g, yo), u_send.at[g], u_recv.at[g], ynb).wait_recv()

    def base(at):
        sub3 = lax.broadcasted_iota(jnp.int32, (3, 8, 128), 1)
        lane3 = lanes((3, 8, 128))
        seg3 = lane3 >> 4
        seg24 = lanes((24, 128)) & 112
        here = [(sub3 == (lane3 & 7)) & (((lane3 >> 3) & 1) == xr) for xr in range(2)]
        segs = [seg3 == lb for lb in range(8)]
        low = [[None, None] for _ in range(4)]
        for nb in range(4):
            xr, qr = nb // 2, nb % 2
            for qc in range(2):
                acc = dg[at:at + 3, qc, qr, 0, xr]
                for lb in range(1, 8):
                    acc = jnp.where(segs[lb], dg[at:at + 3, qc, qr, lb, xr], acc)
                low[nb][qc] = acc
        rec = []
        for qc in range(2):
            dsum = jnp.where(here[0], low[qc][qc], 0.0) + jnp.where(here[1], low[2 + qc][qc], 0.0)
            rec.append(1.0 / jnp.sum(dsum, axis=1, keepdims=True))
        rhs = []
        for nb in range(4):
            for qc in range(2):
                low[nb][qc] = (low[nb][qc] * rec[qc]).reshape(24, 128)
            rhs.append([jnp.where(here[nb // 2], 1.0, 0.0) if nb % 2 == qc else jnp.zeros((3, 8, 128), F32)
                        for qc in range(2)])
        below = [sub3 > ek for ek in range(7)]
        for k in range(32):
            nk, ek = k // 8, k % 8
            xk, qk = nk // 2, nk % 2
            idx = seg24 + (8 * xk + ek)
            pivot = [rhs[nk][qc][:, ek:ek + 1, :] for qc in range(2)]
            for nb in range(nk, 4):
                if nb == nk and ek == 7:
                    continue
                col = along(low[nb][qk], idx).reshape(3, 8, 128)
                if nb == nk:
                    col = jnp.where(below[ek], col, 0.0)
                for qc in range(2):
                    rhs[nb][qc] = rhs[nb][qc] - col * pivot[qc]
        for nb in range(4):
            xr, qr = nb // 2, nb % 2
            idx = (seg3 * 16 + 8 * xr + sub3).reshape(24, 128)
            scale = along(jnp.broadcast_to(rec[qr], (3, 8, 128)).reshape(24, 128), idx).reshape(3, 8, 128)
            for qc in range(2):
                val = rhs[nb][qc] * scale
                for lb in range(8):
                    inv[at:at + 3, qc, qr, lb, xr] = jnp.where(segs[lb], val, 0.0)

    def both(ref_of):
        return jnp.concatenate([ref_of(0), ref_of(1)], axis=1)

    def inv_full(b):
        return both(lambda qc: inv[b, qc].reshape(256, 128))

    def low_block(k, j):
        return both(lambda qc: goff[OFF_AT[k, j], qc].reshape(256, 128))

    def rows_of(tiles):
        return jnp.concatenate(tiles, axis=0)

    def double(group, w):
        pairs = range(4 // w)
        n = 16 * w
        shift = {1: 4, 2: 5, 4: 6}[w]
        shape = (2, w, 2, 8, 128)
        part = lanes(shape) >> shift
        even = [part == 2 * p for p in pairs]
        pair = [(lanes((w, 2, 8, 128)) >> (shift + 1)) == p for p in pairs]
        zero = jnp.zeros(shape, F32)
        first = (lanes((n, 128)) & n) == 0
        hole = jnp.zeros((128, 128), F32)

        def rows(p, odd):
            return pl.ds((2 * p + odd) * w, w)

        def twin(one, two):
            return rows_of([both(lambda h: (one, hole)[h]), both(lambda h: (hole, two)[h])])

        def low_left(b):
            acc = [zero, zero]
            for qc in range(2):
                for p in pairs:
                    acc[qc] = jnp.where(even[p], dg[b, qc, :, rows(p, 1)], acc[qc])
            return acc[0].reshape(2 * n, 128) + turn(acc[1].reshape(2 * n, 128), n)

        def up_inv(b):
            parts = []
            for p in pairs:
                for q in range(2):
                    one, two = (inv[b, qc, q, rows(p, 0)].reshape(n, 128) for qc in range(2))
                    parts.append(jnp.where(first, one, turn(two, n)))
            return rows_of(parts)

        def low_inv(b):
            acc = [inv[b, qc, :, rows(0, 1)] for qc in range(2)]
            for qc in range(2):
                for p in pairs[1:]:
                    acc[qc] = acc[qc] + inv[b, qc, :, rows(p, 1)]
            return turn(acc[0].reshape(2 * n, 128), -n) + acc[1].reshape(2 * n, 128)

        def temp_rows(temp):
            temp = temp.reshape(shape)
            return rows_of([jnp.where(pair[p], temp[q], 0.0).reshape(n, 128) for p in pairs for q in range(2)])

        def product(lefts, rights):
            if len(lefts) == 1:
                return hdot(lefts[0], rights[0])
            return hdot(jnp.concatenate(lefts, axis=1), twin(*rights))

        here = [(lanes((w, 2, 8, 128)) >> shift) == 2 * p for p in pairs]

        def wide_rows(temp):
            temp = [temp[:, 128 * qc:128 * qc + 128].reshape(shape) for qc in range(2)]
            return rows_of([both(lambda qc: jnp.where(here[p], temp[qc][q], 0.0).reshape(n, 128))
                            for p in pairs for q in range(2)])

        if w < 4:
            temps = [hdot(low_left(b), rows_of([both(lambda qc: inv[b, qc, q, rows(p, 0)].reshape(n, 128))
                                                for p in pairs for q in range(2)])) for b in group]
            for b, temp in zip(group, temps):
                prod = -hdot(low_inv(b), wide_rows(temp))
                for qc in range(2):
                    val = prod[:, 128 * qc:128 * qc + 128].reshape(shape)
                    for p in pairs:
                        inv[b, qc, :, rows(p, 1)] = jnp.where(even[p], val, inv[b, qc, :, rows(p, 1)])
            return
        two_blocks = (group[:2], group[2:])
        temps = [product([low_left(b) for b in bs], [up_inv(b) for b in bs]) for bs in two_blocks]
        for bs, temp in zip(two_blocks, temps):
            prod = -product([low_inv(b) for b in bs],
                            [temp_rows(temp[:, 128 * h:128 * h + 128]) for h in range(len(bs))])
            for h, b in enumerate(bs):
                piece = prod[:, 128 * h:128 * h + 128]
                for qc, val in enumerate((piece, turn(piece, -n))):
                    val = val.reshape(shape)
                    for p in pairs:
                        inv[b, qc, :, rows(p, 1)] = jnp.where(even[p], val, inv[b, qc, :, rows(p, 1)])

    zst = [None] * 6

    def z_diag(j):
        return both(lambda qc: inv[j, qc, c, :, x].reshape(64, 128))

    def emit(i, j, blk):
        out[64 * i:64 * i + 64, 128 * j:128 * j + 128] = blk

    def add_terms(j, ks, acc):
        for k in ks:
            prod = hdot(zst[k], low_block(k, j))
            for i in range(k, 6):
                part = prod[64 * (i - k):64 * (i - k) + 64]
                acc[i] = part if acc[i] is None else acc[i] + part

    def finish(j, acc):
        emit(j, j, inv[j, y, c, :, x].reshape(64, 128))
        if j == 5:
            zst[5] = z_diag(5)
            return
        res = -hdot(rows_of(acc[j + 1:]), inv_full(j))
        zst[j] = rows_of([z_diag(j), res])
        mine = jnp.where(y == 0, res[:, 0:128], res[:, 128:256])
        for i in range(j + 1, 6):
            emit(i, j, mine[64 * (i - j - 1):64 * (i - j)])

    def finish_first(acc, lo, hi):
        res = -hdot(rows_of(acc[lo:hi]), inv[0, y].reshape(256, 128))
        for i in range(lo, hi):
            emit(i, 0, res[64 * (i - lo):64 * (i - lo) + 64])

    def c_block(k, j):
        return cbuf[c_at(k, j)].reshape(256, 128)

    def u_compute_top():
        prod = hdot(z_diag(3), jnp.concatenate([c_block(3, j) for j in range(3)], axis=1))
        for j in range(3):
            utop[y, j] = prod[:, 128 * j:128 * j + 128]

    def u_compute(j):
        both_rows = hdot(zst[3][64:192], c_block(3, j)) + hdot(zst[4], c_block(4, j))
        ubuf[j, y, 0:64] = both_rows[0:64]
        ubuf[j, y, 64:128] = both_rows[64:128] + hdot(zst[5], c_block(5, j))

    def u_add(j, acc):
        parts = {3: both(lambda q: utop[q, j]), 4: both(lambda q: ubuf[j, q, 0:64]), 5: both(lambda q: ubuf[j, q, 64:128])}
        for i, part in parts.items():
            acc[i] = part if acc[i] is None else acc[i] + part

    ready(BO)
    pl.semaphore_wait(barrier, 3)
    own(BO, "y")
    pack(DB)
    own(DB, "xy")
    own(BO, "x")
    pack(DA)
    for i in range(5):
        out[64 * i:64 * i + 64, 128 * (i + 1):768] = jnp.zeros((64, 128 * (5 - i)), F32)
    own(DB, "s")
    from_x(DB)
    own(DA, "xs")
    own(BO, "s")
    c_own(3)
    own(DA, "y")
    from_y(BO)
    from_x(BO)
    from_y(DB)
    from_diag(DB)
    c_own(1)
    from_x(DA)
    c_own(2)
    ready(AO)
    own(AO, "ys")
    wait_sib(DB)
    unpack(DB)
    base(3)
    c_own(0)
    double(DIAG[DB], 1)
    c_relay(3)
    double(DIAG[DB], 2)
    from_diag(BO)
    double(DIAG[DB], 4)
    c_wait(3)
    from_y(DA)
    own(AO, "x")
    u_compute_top()
    u_send_to(3)
    from_diag(DA)
    c_relay(2)
    wait_sib(BO)
    c_relay(1)
    finish(5, None)
    acc = [None] * 6
    add_terms(4, (5,), acc)
    finish(4, acc)
    acc = [None] * 6
    add_terms(3, (5, 4), acc)
    finish(3, acc)
    wait_sib(DA)
    c_wait(2)
    c_relay(0)
    from_y(AO)
    unpack(DA)
    u_compute(2)
    base(0)
    u_send_to(2)
    c_wait(1)
    u_compute(1)
    double(DIAG[DA], 1)
    u_send_to(1)
    c_wait(0)
    from_x(AO)
    u_compute(0)
    double(DIAG[DA], 2)
    u_send_to(0)
    double(DIAG[DA], 4)
    from_diag(AO)
    emit(0, 0, inv[0, y, c, :, x].reshape(64, 128))
    u_wait(3)
    u_wait(2)
    acc = [None] * 6
    u_add(2, acc)
    finish(2, acc)
    wait_sib(AO)
    acc = [None] * 6
    add_terms(1, (2,), acc)
    first = [None] * 6
    add_terms(0, (2,), first)
    u_wait(1)
    u_add(1, acc)
    finish(1, acc)
    add_terms(0, (1,), first)
    u_wait(0)
    u_add(0, first)
    finish_first(first, 1, 6)

    for cp in sends:
        cp.wait_send()


def solution(mesh):
    spec = P(("batch", "row"), "col")

    def body(local_l):
        rows, cols = local_l.shape
        return pl.pallas_call(
            kernel,
            out_shape=jax.ShapeDtypeStruct((rows, cols), F32),
            in_specs=[pl.BlockSpec(memory_space=pltpu.HBM)],
            out_specs=pl.BlockSpec(memory_space=pltpu.VMEM),
            scratch_shapes=[
                pltpu.VMEM((6, 8, 8, 128), F32),
                pltpu.VMEM((2, 2, 2, 2, 15, 8, 128), F32),
                pltpu.VMEM((6, 2, 2, 8, 2, 8, 128), F32),
                pltpu.VMEM((6, 2, 2, 8, 2, 8, 128), F32),
                pltpu.VMEM((9, 2, 8, 2, 8, 128), F32),
                pltpu.VMEM((2, 3, 64, 128), F32),
                pltpu.VMEM((3, 2, 128, 128), F32),
                pltpu.VMEM((6, 2, 2, 8, 2, 8, 128), F32),
                pltpu.SemaphoreType.DMA((21,)),
                pltpu.SemaphoreType.DMA((4, 7)),
                pltpu.SemaphoreType.DMA((4, 7)),
                pltpu.SemaphoreType.DMA((4, 3)),
                pltpu.SemaphoreType.DMA((4, 3)),
                pltpu.SemaphoreType.DMA((4,)),
                pltpu.SemaphoreType.DMA((4,)),
            ],
            compiler_params=pltpu.CompilerParams(
                collective_id=0, has_side_effects=True, vmem_limit_bytes=40 * 1024 * 1024),
        )(pltpu.with_memory_space_constraint(local_l.reshape(rows // 8, 8, cols), pltpu.HBM))

    return jax.shard_map(body, mesh=mesh, in_specs=(spec,), out_specs=spec, check_vma=False)
```

```python
import jax
import jax.numpy as jnp
from jax import lax
from jax.experimental import pallas as pl
from jax.experimental.pallas import tpu as pltpu
from jax.sharding import PartitionSpec as P

MESH = pl.DeviceIdType.MESH
F32 = jnp.float32
DB, DA, BO, A1, A2 = range(5)
DIAG = {DB: (5, 4, 3), DA: (2, 1, 0)}
OFF = {BO: ((5, 4), (4, 3), (5, 3)), A1: ((2, 1), (2, 0)), A2: ((1, 0),)}
OFF_AT = {blk: n for n, blk in enumerate(blk for grp in OFF.values() for blk in grp)}
LAST_X = (A1, A2,)


CGRP = [[(4, j), (5, j)] for j in range(3)] + [[(3, j) for j in range(3)]]


def c_at(k, j):
    return 6 + j if k == 3 else 2 * j + k - 4


def hdot(left, right):
    return jnp.dot(left, right, precision=lax.Precision.HIGHEST, preferred_element_type=F32)


def hdot2(left, right):
    half = left.shape[0] // 16 * 8
    return jnp.concatenate([hdot(left[:half], right), hdot(left[half:], right)], axis=0)


def kernel(inp, out, raw, dpk, dg, goff, cbuf, utop, ubuf, inv, loc_sem, g_send, g_recv, c_send, c_recv, u_send, u_recv):
    row = lax.axis_index("row")
    y = lax.axis_index("col")
    x = row // 2
    c = row % 2
    xo, yo, co = 1 - x, 1 - y, 1 - c
    sib = {"row": 2 * x + co}
    xnb = {"row": 2 * xo + c}
    ynb = {"col": yo}

    def take(bi, bj, dst, sem):
        return pltpu.make_async_copy(inp.at[pl.ds(8 * bi, 8), :, pl.ds(128 * bj, 128)], dst, sem)

    local = {g: [take(b, b, raw.at[b], loc_sem.at[b]) for b in DIAG[g]] for g in DIAG}
    for g in OFF:
        local[g] = [take(bi, bj, goff.at[OFF_AT[bi, bj], y, c, :, x], loc_sem.at[6 + OFF_AT[bi, bj]]) for bi, bj in OFF[g]]
    local_c = [[take(bi, bj, cbuf.at[c_at(bi, bj), c, :, x], loc_sem.at[12 + c_at(bi, bj)]) for bi, bj in grp] for grp in CGRP]
    for grp in (local[DB], local[BO], local[DA], local_c[3], local_c[2], local[A1], local_c[1], local_c[0], local[A2]):
        for cp in grp:
            cp.start()

    barrier = pltpu.get_barrier_semaphore()
    for nbr in (sib, xnb, ynb):
        pl.semaphore_signal(barrier, inc=1, device_id=nbr, device_id_type=MESH)

    sub = lax.broadcasted_iota(jnp.int32, (8, 128), 0)
    lane = lax.broadcasted_iota(jnp.int32, (8, 128), 1)

    def lanes(shape):
        return lax.broadcasted_iota(jnp.int32, shape, len(shape) - 1)

    def along(tile, idx):
        return jnp.take_along_axis(tile, idx, axis=1, mode="promise_in_bounds")

    def turn(tile, n):
        return along(tile, (lanes(tile.shape) + (128 - n)) & 127)

    def pack(g):
        for cp in local[g]:
            cp.wait()
        for i, b in enumerate(DIAG[g]):
            dpk[g, y, c, x, 5 * i] = raw[b, 7]
            for p in range(3):
                n = 112 - 16 * p
                dpk[g, y, c, x, 5 * i + 1 + p] = jnp.where(lane < n, raw[b, 6 - p], turn(raw[b, p], n))
            dpk[g, y, c, x, 5 * i + 4] = raw[b, 3]

    def unpack(g):
        for i, b in enumerate(DIAG[g]):
            for qc in range(2):
                for lb in range(8):
                    if lb >= 3:
                        tiles = dpk[g, qc, :, :, 5 * i + 7 - lb]
                    else:
                        tiles = dpk[g, qc, :, :, 5 * i + 1 + lb].reshape(32, 128)
                        tiles = turn(tiles, 16 * (lb + 1)).reshape(2, 2, 8, 128)
                    dg[b, qc, :, lb] = tiles

    def slot(g, sx, sc, sy):
        if g in DIAG:
            return dpk.at[g, sy, sc, sx]
        return goff.at[pl.ds(OFF_AT[OFF[g][0]], len(OFF[g])), sy, sc, :, sx]

    sends = []

    def copy(ref, send, recv, dev):
        return pltpu.make_async_remote_copy(ref, ref, send, recv, device_id=dev, device_id_type=MESH)

    def start(cp):
        cp.start()
        sends.append(cp)

    def gsend(g, k, ref, dev):
        start(copy(ref, g_send.at[g, k], g_recv.at[g, k], dev))

    def gwait(g, k, ref):
        copy(ref, g_send.at[g, k], g_recv.at[g, k], sib).wait_recv()

    def own(g, to):
        for k, dev in enumerate((xnb, ynb, sib)):
            if "xys"[k] in to:
                gsend(g, k, slot(g, x, c, y), dev)

    def ready(g):
        for cp in local[g]:
            cp.wait()

    def from_x(g):
        gwait(g, 0, slot(g, xo, c, y))
        if g not in LAST_X:
            gsend(g, 3, slot(g, xo, c, y), ynb)
        gsend(g, 4, slot(g, xo, c, y), sib)

    def from_y(g):
        gwait(g, 1, slot(g, x, c, yo))
        if g in LAST_X:
            gsend(g, 3, slot(g, x, c, yo), xnb)
        gsend(g, 5, slot(g, x, c, yo), sib)

    def from_diag(g):
        gwait(g, 3, slot(g, xo, c, yo))
        gsend(g, 6, slot(g, xo, c, yo), sib)

    def wait_sib(g):
        for k, ref in ((2, slot(g, x, co, y)), (4, slot(g, xo, co, y)), (5, slot(g, x, co, yo)), (6, slot(g, xo, co, yo))):
            gwait(g, k, ref)

    def c_slot(g, sx, sc):
        return cbuf.at[pl.ds(c_at(*CGRP[g][0]), len(CGRP[g])), sc, :, sx]

    def c_own(g):
        for cp in local_c[g]:
            cp.wait()
        for k, dev in enumerate((xnb, sib)):
            start(copy(c_slot(g, x, c), c_send.at[g, k], c_recv.at[g, k], dev))

    def c_relay(g):
        copy(c_slot(g, xo, c), c_send.at[g, 0], c_recv.at[g, 0], sib).wait_recv()
        start(copy(c_slot(g, xo, c), c_send.at[g, 2], c_recv.at[g, 2], sib))

    def c_wait(g):
        copy(c_slot(g, x, co), c_send.at[g, 1], c_recv.at[g, 1], sib).wait_recv()
        copy(c_slot(g, xo, co), c_send.at[g, 2], c_recv.at[g, 2], sib).wait_recv()

    def u_slot(g, sy):
        return utop.at[sy] if g == 3 else ubuf.at[g, sy]

    def u_send_to(g):
        start(copy(u_slot(g, y), u_send.at[g], u_recv.at[g], ynb))

    def u_wait(g):
        copy(u_slot(g, yo), u_send.at[g], u_recv.at[g], ynb).wait_recv()

    def base(at):
        sub3 = lax.broadcasted_iota(jnp.int32, (3, 8, 128), 1)
        lane3 = lanes((3, 8, 128))
        seg3 = lane3 >> 4
        seg24 = lanes((24, 128)) & 112
        here = [(sub3 == (lane3 & 7)) & (((lane3 >> 3) & 1) == xr) for xr in range(2)]
        segs = [seg3 == lb for lb in range(8)]
        low = [[None, None] for _ in range(4)]
        for nb in range(4):
            xr, qr = nb // 2, nb % 2
            for qc in range(2):
                acc = dg[at:at + 3, qc, qr, 0, xr]
                for lb in range(1, 8):
                    acc = jnp.where(segs[lb], dg[at:at + 3, qc, qr, lb, xr], acc)
                low[nb][qc] = acc
        rec = []
        for qc in range(2):
            dsum = jnp.where(here[0], low[qc][qc], 0.0) + jnp.where(here[1], low[2 + qc][qc], 0.0)
            rec.append(1.0 / jnp.sum(dsum, axis=1, keepdims=True))
        rhs = []
        for nb in range(4):
            for qc in range(2):
                low[nb][qc] = (low[nb][qc] * rec[qc]).reshape(24, 128)
            rhs.append([jnp.where(here[nb // 2], 1.0, 0.0) if nb % 2 == qc else jnp.zeros((3, 8, 128), F32)
                        for qc in range(2)])
        below = [sub3 > ek for ek in range(7)]
        for k in range(32):
            nk, ek = k // 8, k % 8
            xk, qk = nk // 2, nk % 2
            idx = seg24 + (8 * xk + ek)
            pivot = [rhs[nk][qc][:, ek:ek + 1, :] for qc in range(2)]
            for nb in range(nk, 4):
                if nb == nk and ek == 7:
                    continue
                col = along(low[nb][qk], idx).reshape(3, 8, 128)
                if nb == nk:
                    col = jnp.where(below[ek], col, 0.0)
                for qc in range(2):
                    rhs[nb][qc] = rhs[nb][qc] - col * pivot[qc]
        for nb in range(4):
            xr, qr = nb // 2, nb % 2
            idx = (seg3 * 16 + 8 * xr + sub3).reshape(24, 128)
            scale = along(jnp.broadcast_to(rec[qr], (3, 8, 128)).reshape(24, 128), idx).reshape(3, 8, 128)
            for qc in range(2):
                val = rhs[nb][qc] * scale
                for lb in range(8):
                    inv[at:at + 3, qc, qr, lb, xr] = jnp.where(segs[lb], val, 0.0)

    def both(ref_of):
        return jnp.concatenate([ref_of(0), ref_of(1)], axis=1)

    def inv_full(b):
        return both(lambda qc: inv[b, qc].reshape(256, 128))

    def low_block(k, j):
        return both(lambda qc: goff[OFF_AT[k, j], qc].reshape(256, 128))

    def rows_of(tiles):
        return jnp.concatenate(tiles, axis=0)

    def double(group, w):
        pairs = range(4 // w)
        n = 16 * w
        shift = {1: 4, 2: 5, 4: 6}[w]
        shape = (2, w, 2, 8, 128)
        part = lanes(shape) >> shift
        even = [part == 2 * p for p in pairs]
        pair = [(lanes((w, 2, 8, 128)) >> (shift + 1)) == p for p in pairs]
        zero = jnp.zeros(shape, F32)
        first = (lanes((n, 128)) & n) == 0
        hole = jnp.zeros((128, 128), F32)

        def rows(p, odd):
            return pl.ds((2 * p + odd) * w, w)

        def twin(one, two):
            return rows_of([both(lambda h: (one, hole)[h]), both(lambda h: (hole, two)[h])])

        def low_left(b):
            acc = [zero, zero]
            for qc in range(2):
                for p in pairs:
                    acc[qc] = jnp.where(even[p], dg[b, qc, :, rows(p, 1)], acc[qc])
            return acc[0].reshape(2 * n, 128) + turn(acc[1].reshape(2 * n, 128), n)

        def up_inv(b):
            parts = []
            for p in pairs:
                for q in range(2):
                    one, two = (inv[b, qc, q, rows(p, 0)].reshape(n, 128) for qc in range(2))
                    parts.append(jnp.where(first, one, turn(two, n)))
            return rows_of(parts)

        def low_inv(b):
            acc = [inv[b, qc, :, rows(0, 1)] for qc in range(2)]
            for qc in range(2):
                for p in pairs[1:]:
                    acc[qc] = acc[qc] + inv[b, qc, :, rows(p, 1)]
            return turn(acc[0].reshape(2 * n, 128), -n) + acc[1].reshape(2 * n, 128)

        def temp_rows(temp):
            temp = temp.reshape(shape)
            return rows_of([jnp.where(pair[p], temp[q], 0.0).reshape(n, 128) for p in pairs for q in range(2)])

        def product(lefts, rights):
            if len(lefts) == 1:
                return hdot(lefts[0], rights[0])
            return hdot(jnp.concatenate(lefts, axis=1), twin(*rights))

        here = [(lanes((w, 2, 8, 128)) >> shift) == 2 * p for p in pairs]

        def wide_rows(temp):
            temp = [temp[:, 128 * qc:128 * qc + 128].reshape(shape) for qc in range(2)]
            return rows_of([both(lambda qc: jnp.where(here[p], temp[qc][q], 0.0).reshape(n, 128))
                            for p in pairs for q in range(2)])

        if w < 4:
            temps = [hdot(low_left(b), rows_of([both(lambda qc: inv[b, qc, q, rows(p, 0)].reshape(n, 128))
                                                for p in pairs for q in range(2)])) for b in group]
            for b, temp in zip(group, temps):
                prod = -hdot(low_inv(b), wide_rows(temp))
                for qc in range(2):
                    val = prod[:, 128 * qc:128 * qc + 128].reshape(shape)
                    for p in pairs:
                        inv[b, qc, :, rows(p, 1)] = jnp.where(even[p], val, inv[b, qc, :, rows(p, 1)])
            return
        two_blocks = (group[:2], group[2:])
        temps = [product([low_left(b) for b in bs], [up_inv(b) for b in bs]) for bs in two_blocks]
        for bs, temp in zip(two_blocks, temps):
            prod = -product([low_inv(b) for b in bs],
                            [temp_rows(temp[:, 128 * h:128 * h + 128]) for h in range(len(bs))])
            for h, b in enumerate(bs):
                piece = prod[:, 128 * h:128 * h + 128]
                for qc, val in enumerate((piece, turn(piece, -n))):
                    val = val.reshape(shape)
                    for p in pairs:
                        inv[b, qc, :, rows(p, 1)] = jnp.where(even[p], val, inv[b, qc, :, rows(p, 1)])

    zst = [None] * 6

    def z_diag(j):
        return both(lambda qc: inv[j, qc, c, :, x].reshape(64, 128))

    def emit(i, j, blk):
        out[64 * i:64 * i + 64, 128 * j:128 * j + 128] = blk

    def add_terms(j, ks, acc):
        for k in ks:
            prod = (hdot2 if k == j + 1 else hdot)(zst[k], low_block(k, j))
            for i in range(k, 6):
                part = prod[64 * (i - k):64 * (i - k) + 64]
                acc[i] = part if acc[i] is None else acc[i] + part

    def finish(j, acc):
        emit(j, j, inv[j, y, c, :, x].reshape(64, 128))
        if j == 5:
            zst[5] = z_diag(5)
            return
        res = -hdot2(rows_of(acc[j + 1:]), inv_full(j))
        zst[j] = rows_of([z_diag(j), res])
        mine = jnp.where(y == 0, res[:, 0:128], res[:, 128:256])
        for i in range(j + 1, 6):
            emit(i, j, mine[64 * (i - j - 1):64 * (i - j)])

    def empty():
        return [None] * 6

    def finish_first(acc):
        res = -hdot2(rows_of(acc[1:]), inv[0, y].reshape(256, 128))
        for i in range(1, 6):
            emit(i, 0, res[64 * (i - 1):64 * i])

    def c_block(k, j):
        return cbuf[c_at(k, j)].reshape(256, 128)

    def u_compute_top():
        prod = hdot(z_diag(3), jnp.concatenate([c_block(3, j) for j in range(3)], axis=1))
        for j in range(3):
            utop[y, j] = prod[:, 128 * j:128 * j + 128]

    def u_compute(j):
        both_rows = hdot(zst[3][64:192], c_block(3, j)) + hdot(zst[4], c_block(4, j))
        ubuf[j, y, 0:64] = both_rows[0:64]
        ubuf[j, y, 64:128] = both_rows[64:128] + hdot(zst[5], c_block(5, j))

    def u_add(j, acc):
        parts = {3: both(lambda q: utop[q, j]), 4: both(lambda q: ubuf[j, q, 0:64]), 5: both(lambda q: ubuf[j, q, 64:128])}
        for i, part in parts.items():
            acc[i] = part if acc[i] is None else acc[i] + part

    pack(DB)
    pl.semaphore_wait(barrier, 3)
    own(DB, "yx")
    ready(BO)
    own(BO, "sx")
    own(DB, "s")
    own(BO, "y")
    from_x(DB)
    pack(DA)
    own(DA, "yx")
    from_y(DB)
    c_own(3)
    from_x(BO)
    c_own(2)
    own(DA, "s")
    c_own(0)
    for i in range(5):
        out[64 * i:64 * i + 64, 128 * (i + 1):768] = jnp.zeros((64, 128 * (5 - i)), F32)
    from_diag(DB)
    wait_sib(DB)
    from_y(DA)
    from_x(DA)
    unpack(DB)
    base(3)
    c_own(1)
    double(DIAG[DB], 1)
    ready(A1)
    own(A1, "y")
    from_y(BO)
    c_relay(3)
    double(DIAG[DB], 2)
    own(A1, "x")
    from_diag(BO)
    ready(A2)
    own(A2, "xy")
    double(DIAG[DB], 4)
    c_wait(3)
    u_compute_top()
    u_send_to(3)
    from_diag(DA)
    wait_sib(BO)
    c_relay(2)
    finish(5, None)
    acc = empty()
    add_terms(4, (5,), acc)
    finish(4, acc)
    acc = empty()
    add_terms(3, (5, 4), acc)
    finish(3, acc)
    c_relay(1)
    from_y(A1)
    c_relay(0)
    wait_sib(DA)
    c_wait(2)
    unpack(DA)
    u_compute(2)
    base(0)
    u_send_to(2)
    own(A1, "s")
    own(A2, "s")
    from_y(A2)
    c_wait(1)
    u_compute(1)
    double(DIAG[DA], 1)
    u_send_to(1)
    c_wait(0)
    from_x(A2)
    from_x(A1)
    u_compute(0)
    double(DIAG[DA], 2)
    u_send_to(0)
    from_diag(A1)
    double(DIAG[DA], 4)
    emit(0, 0, inv[0, y, c, :, x].reshape(64, 128))
    from_diag(A2)
    u_wait(3)
    u_wait(2)
    acc = empty()
    u_add(2, acc)
    finish(2, acc)
    wait_sib(A1)
    acc = empty()
    add_terms(1, (2,), acc)
    first = empty()
    add_terms(0, (2,), first)
    u_wait(1)
    wait_sib(A2)
    u_add(1, acc)
    finish(1, acc)
    add_terms(0, (1,), first)
    u_wait(0)
    u_add(0, first)
    finish_first(first)

    for cp in sends:
        cp.wait_send()


def solution(mesh):
    spec = P(("batch", "row"), "col")

    def body(local_l):
        rows, cols = local_l.shape
        return pl.pallas_call(
            kernel,
            out_shape=jax.ShapeDtypeStruct((rows, cols), F32),
            in_specs=[pl.BlockSpec(memory_space=pltpu.HBM)],
            out_specs=pl.BlockSpec(memory_space=pltpu.VMEM),
            scratch_shapes=[
                pltpu.VMEM((6, 8, 8, 128), F32),
                pltpu.VMEM((2, 2, 2, 2, 15, 8, 128), F32),
                pltpu.VMEM((6, 2, 2, 8, 2, 8, 128), F32),
                pltpu.VMEM((6, 2, 2, 8, 2, 8, 128), F32),
                pltpu.VMEM((9, 2, 8, 2, 8, 128), F32),
                pltpu.VMEM((2, 3, 64, 128), F32),
                pltpu.VMEM((3, 2, 128, 128), F32),
                pltpu.VMEM((6, 2, 2, 8, 2, 8, 128), F32),
                pltpu.SemaphoreType.DMA((21,)),
                pltpu.SemaphoreType.DMA((5, 7)),
                pltpu.SemaphoreType.DMA((5, 7)),
                pltpu.SemaphoreType.DMA((4, 3)),
                pltpu.SemaphoreType.DMA((4, 3)),
                pltpu.SemaphoreType.DMA((4,)),
                pltpu.SemaphoreType.DMA((4,)),
            ],
            compiler_params=pltpu.CompilerParams(
                collective_id=0, has_side_effects=True, vmem_limit_bytes=40 * 1024 * 1024),
        )(pltpu.with_memory_space_constraint(local_l.reshape(rows // 8, 8, cols), pltpu.HBM))

    return jax.shard_map(body, mesh=mesh, in_specs=(spec,), out_specs=spec, check_vma=False)
```

```python
import jax
import jax.numpy as jnp
from jax import lax
from jax.experimental import pallas as pl
from jax.experimental.pallas import tpu as pltpu
from jax.sharding import PartitionSpec as P

MESH = pl.DeviceIdType.MESH
F32 = jnp.float32
DB, DA, BO, A1, A2 = range(5)
DIAG = {DB: (5, 4, 3), DA: (2, 1, 0)}
OFF = {BO: ((5, 4), (4, 3), (5, 3)), A1: ((2, 1), (2, 0)), A2: ((1, 0),)}
OFF_AT = {blk: n for n, blk in enumerate(blk for grp in OFF.values() for blk in grp)}
LAST_X = (A1, A2,)


CGRP = [[(4, j), (5, j)] for j in range(3)] + [[(3, j) for j in range(3)]]


def c_at(k, j):
    return 6 + j if k == 3 else 2 * j + k - 4


def hdot(left, right):
    return jnp.dot(left, right, precision=lax.Precision.HIGHEST, preferred_element_type=F32)


def hdot2(left, right):
    half = left.shape[0] // 16 * 8
    return jnp.concatenate([hdot(left[:half], right), hdot(left[half:], right)], axis=0)


def kernel(inp, out, raw, dpk, dg, goff, cbuf, utop, ubuf, inv, loc_sem, g_send, g_recv, c_send, c_recv, u_send, u_recv):
    row = lax.axis_index("row")
    y = lax.axis_index("col")
    x = row // 2
    c = row % 2
    xo, yo, co = 1 - x, 1 - y, 1 - c
    sib = {"row": 2 * x + co}
    xnb = {"row": 2 * xo + c}
    ynb = {"col": yo}

    def take(bi, bj, dst, sem):
        return pltpu.make_async_copy(inp.at[pl.ds(8 * bi, 8), :, pl.ds(128 * bj, 128)], dst, sem)

    local = {g: [take(b, b, raw.at[b], loc_sem.at[b]) for b in DIAG[g]] for g in DIAG}
    for g in OFF:
        local[g] = [take(bi, bj, goff.at[OFF_AT[bi, bj], y, c, :, x], loc_sem.at[6 + OFF_AT[bi, bj]]) for bi, bj in OFF[g]]
    local_c = [[take(bi, bj, cbuf.at[c_at(bi, bj), c, :, x], loc_sem.at[12 + c_at(bi, bj)]) for bi, bj in grp] for grp in CGRP]
    for grp in (local[DB], local[BO], local[DA], local_c[3], local_c[2], local[A1], local_c[1], local_c[0], local[A2]):
        for cp in grp:
            cp.start()

    barrier = pltpu.get_barrier_semaphore()
    for nbr in (sib, xnb, ynb):
        pl.semaphore_signal(barrier, inc=1, device_id=nbr, device_id_type=MESH)

    sub = lax.broadcasted_iota(jnp.int32, (8, 128), 0)
    lane = lax.broadcasted_iota(jnp.int32, (8, 128), 1)

    def lanes(shape):
        return lax.broadcasted_iota(jnp.int32, shape, len(shape) - 1)

    def along(tile, idx):
        return jnp.take_along_axis(tile, idx, axis=1, mode="promise_in_bounds")

    def turn(tile, n):
        return along(tile, (lanes(tile.shape) + (128 - n)) & 127)

    def pack(g):
        for cp in local[g]:
            cp.wait()
        for i, b in enumerate(DIAG[g]):
            dpk[g, y, c, x, 5 * i] = raw[b, 7]
            for p in range(3):
                n = 112 - 16 * p
                dpk[g, y, c, x, 5 * i + 1 + p] = jnp.where(lane < n, raw[b, 6 - p], turn(raw[b, p], n))
            dpk[g, y, c, x, 5 * i + 4] = raw[b, 3]

    def unpack(g):
        for i, b in enumerate(DIAG[g]):
            for qc in range(2):
                for lb in range(8):
                    if lb >= 3:
                        tiles = dpk[g, qc, :, :, 5 * i + 7 - lb]
                    else:
                        tiles = dpk[g, qc, :, :, 5 * i + 1 + lb].reshape(32, 128)
                        tiles = turn(tiles, 16 * (lb + 1)).reshape(2, 2, 8, 128)
                    dg[b, qc, :, lb] = tiles

    def slot(g, sx, sc, sy):
        if g in DIAG:
            return dpk.at[g, sy, sc, sx]
        return goff.at[pl.ds(OFF_AT[OFF[g][0]], len(OFF[g])), sy, sc, :, sx]

    sends = []

    def copy(ref, send, recv, dev):
        return pltpu.make_async_remote_copy(ref, ref, send, recv, device_id=dev, device_id_type=MESH)

    def start(cp):
        cp.start()
        sends.append(cp)

    def gsend(g, k, ref, dev):
        start(copy(ref, g_send.at[g, k], g_recv.at[g, k], dev))

    def gwait(g, k, ref):
        copy(ref, g_send.at[g, k], g_recv.at[g, k], sib).wait_recv()

    def own(g, to):
        for k, dev in enumerate((xnb, ynb, sib)):
            if "xys"[k] in to:
                gsend(g, k, slot(g, x, c, y), dev)

    def ready(g):
        for cp in local[g]:
            cp.wait()

    def from_x(g):
        gwait(g, 0, slot(g, xo, c, y))
        if g not in LAST_X:
            gsend(g, 3, slot(g, xo, c, y), ynb)
        gsend(g, 4, slot(g, xo, c, y), sib)

    def from_y(g):
        gwait(g, 1, slot(g, x, c, yo))
        if g in LAST_X:
            gsend(g, 3, slot(g, x, c, yo), xnb)
        gsend(g, 5, slot(g, x, c, yo), sib)

    def from_diag(g):
        gwait(g, 3, slot(g, xo, c, yo))
        gsend(g, 6, slot(g, xo, c, yo), sib)

    def wait_sib(g):
        for k, ref in ((2, slot(g, x, co, y)), (4, slot(g, xo, co, y)), (5, slot(g, x, co, yo)), (6, slot(g, xo, co, yo))):
            gwait(g, k, ref)

    def c_slot(g, sx, sc):
        return cbuf.at[pl.ds(c_at(*CGRP[g][0]), len(CGRP[g])), sc, :, sx]

    def c_own(g):
        for cp in local_c[g]:
            cp.wait()
        for k, dev in enumerate((xnb, sib)):
            start(copy(c_slot(g, x, c), c_send.at[g, k], c_recv.at[g, k], dev))

    def c_relay(g):
        copy(c_slot(g, xo, c), c_send.at[g, 0], c_recv.at[g, 0], sib).wait_recv()
        start(copy(c_slot(g, xo, c), c_send.at[g, 2], c_recv.at[g, 2], sib))

    def c_wait(g):
        copy(c_slot(g, x, co), c_send.at[g, 1], c_recv.at[g, 1], sib).wait_recv()
        copy(c_slot(g, xo, co), c_send.at[g, 2], c_recv.at[g, 2], sib).wait_recv()

    def u_slot(g, sy):
        return utop.at[sy] if g == 3 else ubuf.at[g, sy]

    def u_send_to(g):
        start(copy(u_slot(g, y), u_send.at[g], u_recv.at[g], ynb))

    def u_wait(g):
        copy(u_slot(g, yo), u_send.at[g], u_recv.at[g], ynb).wait_recv()

    def base(at):
        sub3 = lax.broadcasted_iota(jnp.int32, (3, 8, 128), 1)
        lane3 = lanes((3, 8, 128))
        seg3 = lane3 >> 4
        seg24 = lanes((24, 128)) & 112
        here = [(sub3 == (lane3 & 7)) & (((lane3 >> 3) & 1) == xr) for xr in range(2)]
        segs = [seg3 == lb for lb in range(8)]
        low = [[None, None] for _ in range(4)]
        for nb in range(4):
            xr, qr = nb // 2, nb % 2
            for qc in range(2):
                acc = dg[at:at + 3, qc, qr, 0, xr]
                for lb in range(1, 8):
                    acc = jnp.where(segs[lb], dg[at:at + 3, qc, qr, lb, xr], acc)
                low[nb][qc] = acc
        rec = []
        for qc in range(2):
            dsum = jnp.where(here[0], low[qc][qc], 0.0) + jnp.where(here[1], low[2 + qc][qc], 0.0)
            rec.append(1.0 / jnp.sum(dsum, axis=1, keepdims=True))
        rhs = []
        for nb in range(4):
            for qc in range(2):
                low[nb][qc] = (low[nb][qc] * rec[qc]).reshape(24, 128)
            rhs.append([jnp.where(here[nb // 2], 1.0, 0.0) if nb % 2 == qc else jnp.zeros((3, 8, 128), F32)
                        for qc in range(2)])
        below = [sub3 > ek for ek in range(7)]
        for k in range(32):
            nk, ek = k // 8, k % 8
            xk, qk = nk // 2, nk % 2
            idx = seg24 + (8 * xk + ek)
            pivot = [rhs[nk][qc][:, ek:ek + 1, :] for qc in range(2)]
            for nb in range(nk, 4):
                if nb == nk and ek == 7:
                    continue
                col = along(low[nb][qk], idx).reshape(3, 8, 128)
                if nb == nk:
                    col = jnp.where(below[ek], col, 0.0)
                for qc in range(2):
                    rhs[nb][qc] = rhs[nb][qc] - col * pivot[qc]
        for nb in range(4):
            xr, qr = nb // 2, nb % 2
            idx = (seg3 * 16 + 8 * xr + sub3).reshape(24, 128)
            scale = along(jnp.broadcast_to(rec[qr], (3, 8, 128)).reshape(24, 128), idx).reshape(3, 8, 128)
            for qc in range(2):
                val = rhs[nb][qc] * scale
                for lb in range(8):
                    inv[at:at + 3, qc, qr, lb, xr] = jnp.where(segs[lb], val, 0.0)

    def both(ref_of):
        return jnp.concatenate([ref_of(0), ref_of(1)], axis=1)

    def inv_full(b):
        return both(lambda qc: inv[b, qc].reshape(256, 128))

    def low_block(k, j):
        return both(lambda qc: goff[OFF_AT[k, j], qc].reshape(256, 128))

    def rows_of(tiles):
        return jnp.concatenate(tiles, axis=0)

    def double(group, w):
        pairs = range(4 // w)
        n = 16 * w
        shift = {1: 4, 2: 5, 4: 6}[w]
        shape = (2, w, 2, 8, 128)
        part = lanes(shape) >> shift
        even = [part == 2 * p for p in pairs]
        pair = [(lanes((w, 2, 8, 128)) >> (shift + 1)) == p for p in pairs]
        zero = jnp.zeros(shape, F32)
        first = (lanes((n, 128)) & n) == 0
        hole = jnp.zeros((128, 128), F32)

        def rows(p, odd):
            return pl.ds((2 * p + odd) * w, w)

        def twin(one, two):
            return rows_of([both(lambda h: (one, hole)[h]), both(lambda h: (hole, two)[h])])

        def low_left(b):
            acc = [zero, zero]
            for qc in range(2):
                for p in pairs:
                    acc[qc] = jnp.where(even[p], dg[b, qc, :, rows(p, 1)], acc[qc])
            return acc[0].reshape(2 * n, 128) + turn(acc[1].reshape(2 * n, 128), n)

        def up_inv(b):
            parts = []
            for p in pairs:
                for q in range(2):
                    one, two = (inv[b, qc, q, rows(p, 0)].reshape(n, 128) for qc in range(2))
                    parts.append(jnp.where(first, one, turn(two, n)))
            return rows_of(parts)

        def low_inv(b):
            acc = [inv[b, qc, :, rows(0, 1)] for qc in range(2)]
            for qc in range(2):
                for p in pairs[1:]:
                    acc[qc] = acc[qc] + inv[b, qc, :, rows(p, 1)]
            return turn(acc[0].reshape(2 * n, 128), -n) + acc[1].reshape(2 * n, 128)

        def temp_rows(temp):
            temp = temp.reshape(shape)
            return rows_of([jnp.where(pair[p], temp[q], 0.0).reshape(n, 128) for p in pairs for q in range(2)])

        def product(lefts, rights):
            if len(lefts) == 1:
                return hdot(lefts[0], rights[0])
            return hdot(jnp.concatenate(lefts, axis=1), twin(*rights))

        here = [(lanes((w, 2, 8, 128)) >> shift) == 2 * p for p in pairs]

        def wide_rows(temp):
            temp = [temp[:, 128 * qc:128 * qc + 128].reshape(shape) for qc in range(2)]
            return rows_of([both(lambda qc: jnp.where(here[p], temp[qc][q], 0.0).reshape(n, 128))
                            for p in pairs for q in range(2)])

        if w < 4:
            temps = [hdot(low_left(b), rows_of([both(lambda qc: inv[b, qc, q, rows(p, 0)].reshape(n, 128))
                                                for p in pairs for q in range(2)])) for b in group]
            for b, temp in zip(group, temps):
                prod = -hdot(low_inv(b), wide_rows(temp))
                for qc in range(2):
                    val = prod[:, 128 * qc:128 * qc + 128].reshape(shape)
                    for p in pairs:
                        inv[b, qc, :, rows(p, 1)] = jnp.where(even[p], val, inv[b, qc, :, rows(p, 1)])
            return
        two_blocks = (group[:2], group[2:])
        temps = [product([low_left(b) for b in bs], [up_inv(b) for b in bs]) for bs in two_blocks]
        for bs, temp in zip(two_blocks, temps):
            prod = -product([low_inv(b) for b in bs],
                            [temp_rows(temp[:, 128 * h:128 * h + 128]) for h in range(len(bs))])
            for h, b in enumerate(bs):
                piece = prod[:, 128 * h:128 * h + 128]
                for qc, val in enumerate((piece, turn(piece, -n))):
                    val = val.reshape(shape)
                    for p in pairs:
                        inv[b, qc, :, rows(p, 1)] = jnp.where(even[p], val, inv[b, qc, :, rows(p, 1)])

    zst = [None] * 6

    def z_diag(j):
        return both(lambda qc: inv[j, qc, c, :, x].reshape(64, 128))

    def emit(i, j, blk):
        out[64 * i:64 * i + 64, 128 * j:128 * j + 128] = blk

    def add_terms(j, ks, acc):
        for k in ks:
            prod = (hdot2 if k == j + 1 else hdot)(zst[k], low_block(k, j))
            for i in range(k, 6):
                part = prod[64 * (i - k):64 * (i - k) + 64]
                acc[i] = part if acc[i] is None else acc[i] + part

    def finish(j, acc):
        emit(j, j, inv[j, y, c, :, x].reshape(64, 128))
        if j == 5:
            zst[5] = z_diag(5)
            return
        res = -hdot2(rows_of(acc[j + 1:]), inv_full(j))
        zst[j] = rows_of([z_diag(j), res])
        mine = jnp.where(y == 0, res[:, 0:128], res[:, 128:256])
        for i in range(j + 1, 6):
            emit(i, j, mine[64 * (i - j - 1):64 * (i - j)])

    def empty():
        return [None] * 6

    def finish_first(acc, rows):
        res = -hdot(rows_of([acc[i] for i in rows]), inv[0, y].reshape(256, 128))
        for n, i in enumerate(rows):
            emit(i, 0, res[64 * n:64 * n + 64])

    def c_block(k, j):
        return cbuf[c_at(k, j)].reshape(256, 128)

    def u_compute_top():
        prod = hdot(z_diag(3), jnp.concatenate([c_block(3, j) for j in range(3)], axis=1))
        for j in range(3):
            utop[y, j] = prod[:, 128 * j:128 * j + 128]

    def u_compute(j):
        both_rows = hdot(zst[3][64:192], c_block(3, j)) + hdot(zst[4], c_block(4, j))
        ubuf[j, y, 0:64] = both_rows[0:64]
        ubuf[j, y, 64:128] = both_rows[64:128] + hdot(zst[5], c_block(5, j))

    def u_rows(i, j, q):
        if i == 3:
            return utop[q, j]
        return ubuf[j, q, 64 * (i - 4):64 * (i - 3)]

    def u_add(j, acc, rows=(3, 4, 5)):
        for i in rows:
            part = both(lambda q: u_rows(i, j, q))
            acc[i] = part if acc[i] is None else acc[i] + part

    pack(DB)
    pl.semaphore_wait(barrier, 3)
    own(DB, "yx")
    ready(BO)
    own(BO, "sx")
    own(DB, "s")
    own(BO, "y")
    from_x(DB)
    pack(DA)
    own(DA, "yx")
    from_y(DB)
    c_own(3)
    from_x(BO)
    c_own(2)
    own(DA, "s")
    c_own(0)
    for i in range(5):
        out[64 * i:64 * i + 64, 128 * (i + 1):768] = jnp.zeros((64, 128 * (5 - i)), F32)
    from_diag(DB)
    wait_sib(DB)
    from_y(DA)
    from_x(DA)
    unpack(DB)
    base(3)
    c_own(1)
    double(DIAG[DB], 1)
    ready(A1)
    own(A1, "y")
    from_y(BO)
    c_relay(3)
    double(DIAG[DB], 2)
    own(A1, "x")
    from_diag(BO)
    ready(A2)
    own(A2, "xy")
    double(DIAG[DB], 4)
    c_wait(3)
    u_compute_top()
    u_send_to(3)
    from_diag(DA)
    wait_sib(BO)
    c_relay(2)
    finish(5, None)
    acc = empty()
    add_terms(4, (5,), acc)
    finish(4, acc)
    acc = empty()
    add_terms(3, (5, 4), acc)
    finish(3, acc)
    c_relay(1)
    from_y(A1)
    c_relay(0)
    wait_sib(DA)
    c_wait(2)
    unpack(DA)
    u_compute(2)
    base(0)
    u_send_to(2)
    own(A1, "s")
    own(A2, "s")
    from_y(A2)
    c_wait(1)
    u_compute(1)
    double(DIAG[DA], 1)
    u_send_to(1)
    c_wait(0)
    from_x(A2)
    from_x(A1)
    u_compute(0)
    double(DIAG[DA], 2)
    u_send_to(0)
    from_diag(A1)
    double(DIAG[DA], 4)
    emit(0, 0, inv[0, y, c, :, x].reshape(64, 128))
    from_diag(A2)
    u_wait(3)
    u_wait(2)
    acc = empty()
    u_add(2, acc)
    finish(2, acc)
    wait_sib(A1)
    acc = empty()
    add_terms(1, (2,), acc)
    first = empty()
    add_terms(0, (2,), first)
    u_wait(1)
    wait_sib(A2)
    u_add(1, acc)
    finish(1, acc)
    add_terms(0, (1,), first)
    u_add(0, first, (3,))
    finish_first(first, (1, 2, 3))
    u_wait(0)
    u_add(0, first, (4, 5))
    finish_first(first, (4, 5))

    for cp in sends:
        cp.wait_send()


def solution(mesh):
    spec = P(("batch", "row"), "col")

    def body(local_l):
        rows, cols = local_l.shape
        return pl.pallas_call(
            kernel,
            out_shape=jax.ShapeDtypeStruct((rows, cols), F32),
            in_specs=[pl.BlockSpec(memory_space=pltpu.HBM)],
            out_specs=pl.BlockSpec(memory_space=pltpu.VMEM),
            scratch_shapes=[
                pltpu.VMEM((6, 8, 8, 128), F32),
                pltpu.VMEM((2, 2, 2, 2, 15, 8, 128), F32),
                pltpu.VMEM((6, 2, 2, 8, 2, 8, 128), F32),
                pltpu.VMEM((6, 2, 2, 8, 2, 8, 128), F32),
                pltpu.VMEM((9, 2, 8, 2, 8, 128), F32),
                pltpu.VMEM((2, 3, 64, 128), F32),
                pltpu.VMEM((3, 2, 128, 128), F32),
                pltpu.VMEM((6, 2, 2, 8, 2, 8, 128), F32),
                pltpu.SemaphoreType.DMA((21,)),
                pltpu.SemaphoreType.DMA((5, 7)),
                pltpu.SemaphoreType.DMA((5, 7)),
                pltpu.SemaphoreType.DMA((4, 3)),
                pltpu.SemaphoreType.DMA((4, 3)),
                pltpu.SemaphoreType.DMA((4,)),
                pltpu.SemaphoreType.DMA((4,)),
            ],
            compiler_params=pltpu.CompilerParams(
                collective_id=0, has_side_effects=True, vmem_limit_bytes=40 * 1024 * 1024),
        )(pltpu.with_memory_space_constraint(local_l.reshape(rows // 8, 8, cols), pltpu.HBM))

    return jax.shard_map(body, mesh=mesh, in_specs=(spec,), out_specs=spec, check_vma=False)
```

```python
import jax
import jax.numpy as jnp
from jax import lax
from jax.experimental import pallas as pl
from jax.experimental.pallas import tpu as pltpu
from jax.sharding import PartitionSpec as P

MESH = pl.DeviceIdType.MESH
F32 = jnp.float32
DB, DA, BO, A1, A2 = range(5)
DIAG = {DB: (5, 4, 3), DA: (2, 1, 0)}
OFF = {BO: ((5, 4), (4, 3), (5, 3)), A1: ((2, 1), (2, 0)), A2: ((1, 0),)}
OFF_AT = {blk: n for n, blk in enumerate(blk for grp in OFF.values() for blk in grp)}
LAST_X = (A1, A2,)


CGRP = [[(4, j), (5, j)] for j in range(3)] + [[(3, j) for j in range(3)]]


def c_at(k, j):
    return 6 + j if k == 3 else 2 * j + k - 4


def hdot(left, right):
    return jnp.dot(left, right, precision=lax.Precision.HIGHEST, preferred_element_type=F32)


def hdot2(left, right):
    half = left.shape[0] // 16 * 8
    return jnp.concatenate([hdot(left[:half], right), hdot(left[half:], right)], axis=0)


def kernel(inp, out, raw, dpk, dg, goff, cbuf, utop, ubuf, inv, loc_sem, g_send, g_recv, c_send, c_recv, u_send, u_recv):
    row = lax.axis_index("row")
    y = lax.axis_index("col")
    x = row // 2
    c = row % 2
    xo, yo, co = 1 - x, 1 - y, 1 - c
    sib = {"row": 2 * x + co}
    xnb = {"row": 2 * xo + c}
    ynb = {"col": yo}

    def take(bi, bj, dst, sem):
        return pltpu.make_async_copy(inp.at[pl.ds(8 * bi, 8), :, pl.ds(128 * bj, 128)], dst, sem)

    local = {g: [take(b, b, raw.at[b], loc_sem.at[b]) for b in DIAG[g]] for g in DIAG}
    for g in OFF:
        local[g] = [take(bi, bj, goff.at[OFF_AT[bi, bj], y, c, :, x], loc_sem.at[6 + OFF_AT[bi, bj]]) for bi, bj in OFF[g]]
    local_c = [[take(bi, bj, cbuf.at[c_at(bi, bj), c, :, x], loc_sem.at[12 + c_at(bi, bj)]) for bi, bj in grp] for grp in CGRP]
    for grp in (local[DB], local[BO], local[DA], local_c[3], local_c[2], local[A1], local_c[1], local_c[0], local[A2]):
        for cp in grp:
            cp.start()

    barrier = pltpu.get_barrier_semaphore()
    for nbr in (sib, xnb, ynb):
        pl.semaphore_signal(barrier, inc=1, device_id=nbr, device_id_type=MESH)

    sub = lax.broadcasted_iota(jnp.int32, (8, 128), 0)
    lane = lax.broadcasted_iota(jnp.int32, (8, 128), 1)

    def lanes(shape):
        return lax.broadcasted_iota(jnp.int32, shape, len(shape) - 1)

    def along(tile, idx):
        return jnp.take_along_axis(tile, idx, axis=1, mode="promise_in_bounds")

    def turn(tile, n):
        return along(tile, (lanes(tile.shape) + (128 - n)) & 127)

    def pack(g):
        for cp in local[g]:
            cp.wait()
        for i, b in enumerate(DIAG[g]):
            dpk[g, y, c, x, 4 * i] = raw[b, 7]
            for p in range(3):
                n = 112 - 16 * p
                dpk[g, y, c, x, 4 * i + 1 + p] = jnp.where(lane < n, raw[b, 6 - p], turn(raw[b, p], n))
        one, two, three = DIAG[g]
        dpk[g, y, c, x, 12] = jnp.where(lane < 64, raw[one, 3], turn(raw[two, 3], 64))
        dpk[g, y, c, x, 13] = raw[three, 3]

    def unpack(g):
        for i, b in enumerate(DIAG[g]):
            for qc in range(2):
                for lb in range(8):
                    at = 4 * i + (7 - lb if lb > 3 else 1 + lb)
                    n = 16 * (lb + 1)
                    if lb == 3:
                        at, n = 12 + i // 2, 64 * (i % 2)
                    tiles = dpk[g, qc, :, :, at]
                    if lb < 4 and n:
                        tiles = turn(tiles.reshape(32, 128), n).reshape(2, 2, 8, 128)
                    dg[b, qc, :, lb] = tiles

    def slot(g, sx, sc, sy):
        if g in DIAG:
            return dpk.at[g, sy, sc, sx]
        return goff.at[pl.ds(OFF_AT[OFF[g][0]], len(OFF[g])), sy, sc, :, sx]

    sends = []

    def copy(ref, send, recv, dev):
        return pltpu.make_async_remote_copy(ref, ref, send, recv, device_id=dev, device_id_type=MESH)

    def start(cp):
        cp.start()
        sends.append(cp)

    def gsend(g, k, ref, dev):
        start(copy(ref, g_send.at[g, k], g_recv.at[g, k], dev))

    def gwait(g, k, ref):
        copy(ref, g_send.at[g, k], g_recv.at[g, k], sib).wait_recv()

    def own(g, to):
        for k, dev in enumerate((xnb, ynb, sib)):
            if "xys"[k] in to:
                gsend(g, k, slot(g, x, c, y), dev)

    def ready(g):
        for cp in local[g]:
            cp.wait()

    def from_x(g):
        gwait(g, 0, slot(g, xo, c, y))
        if g not in LAST_X:
            gsend(g, 3, slot(g, xo, c, y), ynb)
        gsend(g, 4, slot(g, xo, c, y), sib)

    def from_y(g):
        gwait(g, 1, slot(g, x, c, yo))
        if g in LAST_X:
            gsend(g, 3, slot(g, x, c, yo), xnb)
        gsend(g, 5, slot(g, x, c, yo), sib)

    def from_diag(g):
        gwait(g, 3, slot(g, xo, c, yo))
        gsend(g, 6, slot(g, xo, c, yo), sib)

    def wait_sib(g):
        for k, ref in ((2, slot(g, x, co, y)), (4, slot(g, xo, co, y)), (5, slot(g, x, co, yo)), (6, slot(g, xo, co, yo))):
            gwait(g, k, ref)

    def c_slot(g, sx, sc):
        return cbuf.at[pl.ds(c_at(*CGRP[g][0]), len(CGRP[g])), sc, :, sx]

    def c_own(g):
        for cp in local_c[g]:
            cp.wait()
        for k, dev in enumerate((xnb, sib)):
            start(copy(c_slot(g, x, c), c_send.at[g, k], c_recv.at[g, k], dev))

    def c_relay(g):
        copy(c_slot(g, xo, c), c_send.at[g, 0], c_recv.at[g, 0], sib).wait_recv()
        start(copy(c_slot(g, xo, c), c_send.at[g, 2], c_recv.at[g, 2], sib))

    def c_wait(g):
        copy(c_slot(g, x, co), c_send.at[g, 1], c_recv.at[g, 1], sib).wait_recv()
        copy(c_slot(g, xo, co), c_send.at[g, 2], c_recv.at[g, 2], sib).wait_recv()

    def u_slot(g, sy):
        return utop.at[sy] if g == 3 else ubuf.at[g, sy]

    def u_send_to(g):
        start(copy(u_slot(g, y), u_send.at[g], u_recv.at[g], ynb))

    def u_wait(g):
        copy(u_slot(g, yo), u_send.at[g], u_recv.at[g], ynb).wait_recv()

    def base(at):
        sub3 = lax.broadcasted_iota(jnp.int32, (3, 8, 128), 1)
        lane3 = lanes((3, 8, 128))
        seg3 = lane3 >> 4
        seg24 = lanes((24, 128)) & 112
        here = [(sub3 == (lane3 & 7)) & (((lane3 >> 3) & 1) == xr) for xr in range(2)]
        segs = [seg3 == lb for lb in range(8)]
        low = [[None, None] for _ in range(4)]
        for nb in range(4):
            xr, qr = nb // 2, nb % 2
            for qc in range(2):
                acc = dg[at:at + 3, qc, qr, 0, xr]
                for lb in range(1, 8):
                    acc = jnp.where(segs[lb], dg[at:at + 3, qc, qr, lb, xr], acc)
                low[nb][qc] = acc
        rec = []
        for qc in range(2):
            dsum = jnp.where(here[0], low[qc][qc], 0.0) + jnp.where(here[1], low[2 + qc][qc], 0.0)
            rec.append(1.0 / jnp.sum(dsum, axis=1, keepdims=True))
        rhs = []
        for nb in range(4):
            for qc in range(2):
                low[nb][qc] = (low[nb][qc] * rec[qc]).reshape(24, 128)
            rhs.append([jnp.where(here[nb // 2], 1.0, 0.0) if nb % 2 == qc else jnp.zeros((3, 8, 128), F32)
                        for qc in range(2)])
        below = [sub3 > ek for ek in range(7)]
        for k in range(32):
            nk, ek = k // 8, k % 8
            xk, qk = nk // 2, nk % 2
            idx = seg24 + (8 * xk + ek)
            pivot = [rhs[nk][qc][:, ek:ek + 1, :] for qc in range(2)]
            for nb in range(nk, 4):
                if nb == nk and ek == 7:
                    continue
                col = along(low[nb][qk], idx).reshape(3, 8, 128)
                if nb == nk:
                    col = jnp.where(below[ek], col, 0.0)
                for qc in range(2):
                    rhs[nb][qc] = rhs[nb][qc] - col * pivot[qc]
        for nb in range(4):
            xr, qr = nb // 2, nb % 2
            idx = (seg3 * 16 + 8 * xr + sub3).reshape(24, 128)
            scale = along(jnp.broadcast_to(rec[qr], (3, 8, 128)).reshape(24, 128), idx).reshape(3, 8, 128)
            for qc in range(2):
                val = rhs[nb][qc] * scale
                for lb in range(8):
                    inv[at:at + 3, qc, qr, lb, xr] = jnp.where(segs[lb], val, 0.0)

    def both(ref_of):
        return jnp.concatenate([ref_of(0), ref_of(1)], axis=1)

    def inv_full(b):
        return both(lambda qc: inv[b, qc].reshape(256, 128))

    def low_block(k, j):
        return both(lambda qc: goff[OFF_AT[k, j], qc].reshape(256, 128))

    def rows_of(tiles):
        return jnp.concatenate(tiles, axis=0)

    def double(group, w):
        pairs = range(4 // w)
        n = 16 * w
        shift = {1: 4, 2: 5, 4: 6}[w]
        shape = (2, w, 2, 8, 128)
        part = lanes(shape) >> shift
        even = [part == 2 * p for p in pairs]
        pair = [(lanes((w, 2, 8, 128)) >> (shift + 1)) == p for p in pairs]
        zero = jnp.zeros(shape, F32)
        first = (lanes((n, 128)) & n) == 0
        hole = jnp.zeros((128, 128), F32)

        def rows(p, odd):
            return pl.ds((2 * p + odd) * w, w)

        def twin(one, two):
            return rows_of([both(lambda h: (one, hole)[h]), both(lambda h: (hole, two)[h])])

        def low_left(b):
            acc = [zero, zero]
            for qc in range(2):
                for p in pairs:
                    acc[qc] = jnp.where(even[p], dg[b, qc, :, rows(p, 1)], acc[qc])
            return acc[0].reshape(2 * n, 128) + turn(acc[1].reshape(2 * n, 128), n)

        def up_inv(b):
            parts = []
            for p in pairs:
                for q in range(2):
                    one, two = (inv[b, qc, q, rows(p, 0)].reshape(n, 128) for qc in range(2))
                    parts.append(jnp.where(first, one, turn(two, n)))
            return rows_of(parts)

        def low_inv(b):
            acc = [inv[b, qc, :, rows(0, 1)] for qc in range(2)]
            for qc in range(2):
                for p in pairs[1:]:
                    acc[qc] = acc[qc] + inv[b, qc, :, rows(p, 1)]
            return turn(acc[0].reshape(2 * n, 128), -n) + acc[1].reshape(2 * n, 128)

        def temp_rows(temp):
            temp = temp.reshape(shape)
            return rows_of([jnp.where(pair[p], temp[q], 0.0).reshape(n, 128) for p in pairs for q in range(2)])

        def product(lefts, rights):
            if len(lefts) == 1:
                return hdot(lefts[0], rights[0])
            return hdot(jnp.concatenate(lefts, axis=1), twin(*rights))

        here = [(lanes((w, 2, 8, 128)) >> shift) == 2 * p for p in pairs]

        def wide_rows(temp):
            temp = [temp[:, 128 * qc:128 * qc + 128].reshape(shape) for qc in range(2)]
            return rows_of([both(lambda qc: jnp.where(here[p], temp[qc][q], 0.0).reshape(n, 128))
                            for p in pairs for q in range(2)])

        if w < 4:
            temps = [hdot(low_left(b), rows_of([both(lambda qc: inv[b, qc, q, rows(p, 0)].reshape(n, 128))
                                                for p in pairs for q in range(2)])) for b in group]
            for b, temp in zip(group, temps):
                prod = -hdot(low_inv(b), wide_rows(temp))
                for qc in range(2):
                    val = prod[:, 128 * qc:128 * qc + 128].reshape(shape)
                    for p in pairs:
                        inv[b, qc, :, rows(p, 1)] = jnp.where(even[p], val, inv[b, qc, :, rows(p, 1)])
            return
        two_blocks = (group[:2], group[2:])
        temps = [product([low_left(b) for b in bs], [up_inv(b) for b in bs]) for bs in two_blocks]
        for bs, temp in zip(two_blocks, temps):
            prod = -product([low_inv(b) for b in bs],
                            [temp_rows(temp[:, 128 * h:128 * h + 128]) for h in range(len(bs))])
            for h, b in enumerate(bs):
                piece = prod[:, 128 * h:128 * h + 128]
                for qc, val in enumerate((piece, turn(piece, -n))):
                    val = val.reshape(shape)
                    for p in pairs:
                        inv[b, qc, :, rows(p, 1)] = jnp.where(even[p], val, inv[b, qc, :, rows(p, 1)])

    zst = [None] * 6

    def z_diag(j):
        return both(lambda qc: inv[j, qc, c, :, x].reshape(64, 128))

    def emit(i, j, blk):
        out[64 * i:64 * i + 64, 128 * j:128 * j + 128] = blk

    def add_terms(j, ks, acc):
        for k in ks:
            prod = (hdot2 if k == j + 1 else hdot)(zst[k], low_block(k, j))
            for i in range(k, 6):
                part = prod[64 * (i - k):64 * (i - k) + 64]
                acc[i] = part if acc[i] is None else acc[i] + part

    def finish(j, acc):
        emit(j, j, inv[j, y, c, :, x].reshape(64, 128))
        if j == 5:
            zst[5] = z_diag(5)
            return
        res = -hdot2(rows_of(acc[j + 1:]), inv_full(j))
        zst[j] = rows_of([z_diag(j), res])
        mine = jnp.where(y == 0, res[:, 0:128], res[:, 128:256])
        for i in range(j + 1, 6):
            emit(i, j, mine[64 * (i - j - 1):64 * (i - j)])

    def empty():
        return [None] * 6

    def finish_first(acc, rows):
        res = -hdot(rows_of([acc[i] for i in rows]), inv[0, y].reshape(256, 128))
        for n, i in enumerate(rows):
            emit(i, 0, res[64 * n:64 * n + 64])

    def c_block(k, j):
        return cbuf[c_at(k, j)].reshape(256, 128)

    def u_compute_top():
        prod = hdot(z_diag(3), jnp.concatenate([c_block(3, j) for j in range(3)], axis=1))
        for j in range(3):
            utop[y, j] = prod[:, 128 * j:128 * j + 128]

    def u_compute(j):
        both_rows = hdot(zst[3][64:192], c_block(3, j)) + hdot(zst[4], c_block(4, j))
        ubuf[j, y, 0:64] = both_rows[0:64]
        ubuf[j, y, 64:128] = both_rows[64:128] + hdot(zst[5], c_block(5, j))

    def u_rows(i, j, q):
        if i == 3:
            return utop[q, j]
        return ubuf[j, q, 64 * (i - 4):64 * (i - 3)]

    def u_add(j, acc, rows=(3, 4, 5)):
        for i in rows:
            part = both(lambda q: u_rows(i, j, q))
            acc[i] = part if acc[i] is None else acc[i] + part

    pack(DB)
    pl.semaphore_wait(barrier, 3)
    own(DB, "yx")
    ready(BO)
    own(BO, "sx")
    own(DB, "s")
    own(BO, "y")
    from_x(DB)
    pack(DA)
    own(DA, "yx")
    from_y(DB)
    c_own(3)
    from_x(BO)
    c_own(2)
    own(DA, "s")
    c_own(0)
    for i in range(5):
        out[64 * i:64 * i + 64, 128 * (i + 1):768] = jnp.zeros((64, 128 * (5 - i)), F32)
    from_diag(DB)
    wait_sib(DB)
    from_y(DA)
    from_x(DA)
    unpack(DB)
    base(3)
    c_own(1)
    double(DIAG[DB], 1)
    ready(A1)
    own(A1, "y")
    from_y(BO)
    c_relay(3)
    double(DIAG[DB], 2)
    own(A1, "x")
    from_diag(BO)
    ready(A2)
    own(A2, "xy")
    double(DIAG[DB], 4)
    c_wait(3)
    u_compute_top()
    u_send_to(3)
    from_diag(DA)
    wait_sib(BO)
    c_relay(2)
    finish(5, None)
    acc = empty()
    add_terms(4, (5,), acc)
    finish(4, acc)
    acc = empty()
    add_terms(3, (5, 4), acc)
    finish(3, acc)
    c_relay(1)
    from_y(A1)
    c_relay(0)
    wait_sib(DA)
    c_wait(2)
    unpack(DA)
    u_compute(2)
    base(0)
    u_send_to(2)
    own(A1, "s")
    own(A2, "s")
    from_y(A2)
    c_wait(1)
    u_compute(1)
    double(DIAG[DA], 1)
    u_send_to(1)
    c_wait(0)
    from_x(A2)
    from_x(A1)
    u_compute(0)
    double(DIAG[DA], 2)
    u_send_to(0)
    from_diag(A1)
    double(DIAG[DA], 4)
    emit(0, 0, inv[0, y, c, :, x].reshape(64, 128))
    from_diag(A2)
    u_wait(3)
    u_wait(2)
    acc = empty()
    u_add(2, acc)
    finish(2, acc)
    wait_sib(A1)
    acc = empty()
    add_terms(1, (2,), acc)
    first = empty()
    add_terms(0, (2,), first)
    u_wait(1)
    wait_sib(A2)
    u_add(1, acc)
    finish(1, acc)
    add_terms(0, (1,), first)
    u_add(0, first, (3,))
    finish_first(first, (1, 2, 3))
    u_wait(0)
    u_add(0, first, (4, 5))
    finish_first(first, (4, 5))

    for cp in sends:
        cp.wait_send()


def solution(mesh):
    spec = P(("batch", "row"), "col")

    def body(local_l):
        rows, cols = local_l.shape
        return pl.pallas_call(
            kernel,
            out_shape=jax.ShapeDtypeStruct((rows, cols), F32),
            in_specs=[pl.BlockSpec(memory_space=pltpu.HBM)],
            out_specs=pl.BlockSpec(memory_space=pltpu.VMEM),
            scratch_shapes=[
                pltpu.VMEM((6, 8, 8, 128), F32),
                pltpu.VMEM((2, 2, 2, 2, 14, 8, 128), F32),
                pltpu.VMEM((6, 2, 2, 8, 2, 8, 128), F32),
                pltpu.VMEM((6, 2, 2, 8, 2, 8, 128), F32),
                pltpu.VMEM((9, 2, 8, 2, 8, 128), F32),
                pltpu.VMEM((2, 3, 64, 128), F32),
                pltpu.VMEM((3, 2, 128, 128), F32),
                pltpu.VMEM((6, 2, 2, 8, 2, 8, 128), F32),
                pltpu.SemaphoreType.DMA((21,)),
                pltpu.SemaphoreType.DMA((5, 7)),
                pltpu.SemaphoreType.DMA((5, 7)),
                pltpu.SemaphoreType.DMA((4, 3)),
                pltpu.SemaphoreType.DMA((4, 3)),
                pltpu.SemaphoreType.DMA((4,)),
                pltpu.SemaphoreType.DMA((4,)),
            ],
            compiler_params=pltpu.CompilerParams(
                collective_id=0, has_side_effects=True, vmem_limit_bytes=40 * 1024 * 1024),
        )(pltpu.with_memory_space_constraint(local_l.reshape(rows // 8, 8, cols), pltpu.HBM))

    return jax.shard_map(body, mesh=mesh, in_specs=(spec,), out_specs=spec, check_vma=False)
```

```python
import jax
import jax.numpy as jnp
from jax import lax
from jax.experimental import pallas as pl
from jax.experimental.pallas import tpu as pltpu
from jax.sharding import PartitionSpec as P

MESH = pl.DeviceIdType.MESH
F32 = jnp.float32
DB, DA, BO, A1, A2 = range(5)
DIAG = {DB: (5, 4, 3), DA: (2, 1, 0)}
OFF = {BO: ((5, 4), (4, 3), (5, 3)), A1: ((2, 1), (2, 0)), A2: ((1, 0),)}
OFF_AT = {blk: n for n, blk in enumerate(blk for grp in OFF.values() for blk in grp)}
LAST_X = (A1, A2,)


CGRP = [[(4, j), (5, j)] for j in range(3)] + [[(3, j) for j in range(3)]]


def c_at(k, j):
    return 6 + j if k == 3 else 2 * j + k - 4


def hdot(left, right):
    return jnp.dot(left, right, precision=lax.Precision.HIGHEST, preferred_element_type=F32)


def hdot2(left, right):
    half = left.shape[0] // 16 * 8
    return jnp.concatenate([hdot(left[:half], right), hdot(left[half:], right)], axis=0)


def kernel(inp, out, raw, dpk, dg, goff, cbuf, utop, ubuf, inv, loc_sem, g_send, g_recv, c_send, c_recv, u_send, u_recv):
    row = lax.axis_index("row")
    y = lax.axis_index("col")
    x = row // 2
    c = row % 2
    xo, yo, co = 1 - x, 1 - y, 1 - c
    sib = {"row": 2 * x + co}
    xnb = {"row": 2 * xo + c}
    ynb = {"col": yo}

    barrier = pltpu.get_barrier_semaphore()
    for nbr in (sib, xnb, ynb):
        pl.semaphore_signal(barrier, inc=1, device_id=nbr, device_id_type=MESH)

    def take(bi, bj, dst, sem):
        return pltpu.make_async_copy(inp.at[pl.ds(8 * bi, 8), :, pl.ds(128 * bj, 128)], dst, sem)

    local = {g: [take(b, b, raw.at[b], loc_sem.at[b]) for b in DIAG[g]] for g in DIAG}
    for g in OFF:
        local[g] = [take(bi, bj, goff.at[OFF_AT[bi, bj], y, c, :, x], loc_sem.at[6 + OFF_AT[bi, bj]]) for bi, bj in OFF[g]]
    local_c = [[take(bi, bj, cbuf.at[c_at(bi, bj), c, :, x], loc_sem.at[12 + c_at(bi, bj)]) for bi, bj in grp] for grp in CGRP]
    for grp in (local[DB], local[BO], local[DA], local_c[3], local_c[2], local[A1], local_c[1], local_c[0], local[A2]):
        for cp in grp:
            cp.start()

    sub = lax.broadcasted_iota(jnp.int32, (8, 128), 0)
    lane = lax.broadcasted_iota(jnp.int32, (8, 128), 1)

    def lanes(shape):
        return lax.broadcasted_iota(jnp.int32, shape, len(shape) - 1)

    def along(tile, idx):
        return jnp.take_along_axis(tile, idx, axis=1, mode="promise_in_bounds")

    def turn(tile, n):
        return along(tile, (lanes(tile.shape) + (128 - n)) & 127)

    def pack(g):
        for cp in local[g]:
            cp.wait()
        for i, b in enumerate(DIAG[g]):
            dpk[g, y, c, x, 4 * i] = raw[b, 7]
            for p in range(3):
                n = 112 - 16 * p
                dpk[g, y, c, x, 4 * i + 1 + p] = jnp.where(lane < n, raw[b, 6 - p], turn(raw[b, p], n))
        one, two, three = DIAG[g]
        dpk[g, y, c, x, 12] = jnp.where(lane < 64, raw[one, 3], turn(raw[two, 3], 64))
        dpk[g, y, c, x, 13] = raw[three, 3]

    def unpack(g):
        for i, b in enumerate(DIAG[g]):
            for qc in range(2):
                for lb in range(8):
                    at = 4 * i + (7 - lb if lb > 3 else 1 + lb)
                    n = 16 * (lb + 1)
                    if lb == 3:
                        at, n = 12 + i // 2, 64 * (i % 2)
                    tiles = dpk[g, qc, :, :, at]
                    if lb < 4 and n:
                        tiles = turn(tiles.reshape(32, 128), n).reshape(2, 2, 8, 128)
                    dg[b, qc, :, lb] = tiles

    def slot(g, sx, sc, sy):
        if g in DIAG:
            return dpk.at[g, sy, sc, sx]
        return goff.at[pl.ds(OFF_AT[OFF[g][0]], len(OFF[g])), sy, sc, :, sx]

    sends = []

    def copy(ref, send, recv, dev):
        return pltpu.make_async_remote_copy(ref, ref, send, recv, device_id=dev, device_id_type=MESH)

    def start(cp):
        cp.start()
        sends.append(cp)

    def gsend(g, k, ref, dev):
        start(copy(ref, g_send.at[g, k], g_recv.at[g, k], dev))

    def gwait(g, k, ref):
        copy(ref, g_send.at[g, k], g_recv.at[g, k], sib).wait_recv()

    def own(g, to):
        for k, dev in enumerate((xnb, ynb, sib)):
            if "xys"[k] in to:
                gsend(g, k, slot(g, x, c, y), dev)

    def ready(g):
        for cp in local[g]:
            cp.wait()

    def from_x(g):
        gwait(g, 0, slot(g, xo, c, y))
        if g not in LAST_X:
            gsend(g, 3, slot(g, xo, c, y), ynb)
        gsend(g, 4, slot(g, xo, c, y), sib)

    def from_y(g):
        gwait(g, 1, slot(g, x, c, yo))
        if g in LAST_X:
            gsend(g, 3, slot(g, x, c, yo), xnb)
        gsend(g, 5, slot(g, x, c, yo), sib)

    def from_diag(g):
        gwait(g, 3, slot(g, xo, c, yo))
        gsend(g, 6, slot(g, xo, c, yo), sib)

    def wait_sib(g):
        for k, ref in ((2, slot(g, x, co, y)), (4, slot(g, xo, co, y)), (5, slot(g, x, co, yo)), (6, slot(g, xo, co, yo))):
            gwait(g, k, ref)

    def c_slot(g, sx, sc):
        return cbuf.at[pl.ds(c_at(*CGRP[g][0]), len(CGRP[g])), sc, :, sx]

    def c_own(g):
        for cp in local_c[g]:
            cp.wait()
        for k, dev in enumerate((xnb, sib)):
            start(copy(c_slot(g, x, c), c_send.at[g, k], c_recv.at[g, k], dev))

    def c_relay(g):
        copy(c_slot(g, xo, c), c_send.at[g, 0], c_recv.at[g, 0], sib).wait_recv()
        start(copy(c_slot(g, xo, c), c_send.at[g, 2], c_recv.at[g, 2], sib))

    def c_wait(g):
        copy(c_slot(g, x, co), c_send.at[g, 1], c_recv.at[g, 1], sib).wait_recv()
        copy(c_slot(g, xo, co), c_send.at[g, 2], c_recv.at[g, 2], sib).wait_recv()

    def u_slot(g, sy):
        return utop.at[sy] if g == 3 else ubuf.at[g, sy]

    def u_send_to(g):
        start(copy(u_slot(g, y), u_send.at[g], u_recv.at[g], ynb))

    def u_wait(g):
        copy(u_slot(g, yo), u_send.at[g], u_recv.at[g], ynb).wait_recv()

    def base(at):
        sub3 = lax.broadcasted_iota(jnp.int32, (3, 8, 128), 1)
        lane3 = lanes((3, 8, 128))
        seg3 = lane3 >> 4
        seg24 = lanes((24, 128)) & 112
        here = [(sub3 == (lane3 & 7)) & (((lane3 >> 3) & 1) == xr) for xr in range(2)]
        segs = [seg3 == lb for lb in range(8)]
        low = [[None, None] for _ in range(4)]
        for nb in range(4):
            xr, qr = nb // 2, nb % 2
            for qc in range(2):
                acc = dg[at:at + 3, qc, qr, 0, xr]
                for lb in range(1, 8):
                    acc = jnp.where(segs[lb], dg[at:at + 3, qc, qr, lb, xr], acc)
                low[nb][qc] = acc
        rec = []
        for qc in range(2):
            dsum = jnp.where(here[0], low[qc][qc], 0.0) + jnp.where(here[1], low[2 + qc][qc], 0.0)
            rec.append(1.0 / jnp.sum(dsum, axis=1, keepdims=True))
        rhs = []
        for nb in range(4):
            for qc in range(2):
                low[nb][qc] = (low[nb][qc] * rec[qc]).reshape(24, 128)
            rhs.append([jnp.where(here[nb // 2], 1.0, 0.0) if nb % 2 == qc else jnp.zeros((3, 8, 128), F32)
                        for qc in range(2)])
        below = [sub3 > ek for ek in range(7)]
        for k in range(32):
            nk, ek = k // 8, k % 8
            xk, qk = nk // 2, nk % 2
            idx = seg24 + (8 * xk + ek)
            pivot = [rhs[nk][qc][:, ek:ek + 1, :] for qc in range(2)]
            for nb in range(nk, 4):
                if nb == nk and ek == 7:
                    continue
                col = along(low[nb][qk], idx).reshape(3, 8, 128)
                if nb == nk:
                    col = jnp.where(below[ek], col, 0.0)
                for qc in range(2):
                    rhs[nb][qc] = rhs[nb][qc] - col * pivot[qc]
        for nb in range(4):
            xr, qr = nb // 2, nb % 2
            idx = (seg3 * 16 + 8 * xr + sub3).reshape(24, 128)
            scale = along(jnp.broadcast_to(rec[qr], (3, 8, 128)).reshape(24, 128), idx).reshape(3, 8, 128)
            for qc in range(2):
                val = rhs[nb][qc] * scale
                for lb in range(8):
                    inv[at:at + 3, qc, qr, lb, xr] = jnp.where(segs[lb], val, 0.0)

    def both(ref_of):
        return jnp.concatenate([ref_of(0), ref_of(1)], axis=1)

    def inv_full(b):
        return both(lambda qc: inv[b, qc].reshape(256, 128))

    def low_block(k, j):
        return both(lambda qc: goff[OFF_AT[k, j], qc].reshape(256, 128))

    def rows_of(tiles):
        return jnp.concatenate(tiles, axis=0)

    def double(group, w):
        pairs = range(4 // w)
        n = 16 * w
        shift = {1: 4, 2: 5, 4: 6}[w]
        shape = (2, w, 2, 8, 128)
        part = lanes(shape) >> shift
        even = [part == 2 * p for p in pairs]
        pair = [(lanes((w, 2, 8, 128)) >> (shift + 1)) == p for p in pairs]
        zero = jnp.zeros(shape, F32)
        first = (lanes((n, 128)) & n) == 0
        hole = jnp.zeros((128, 128), F32)

        def rows(p, odd):
            return pl.ds((2 * p + odd) * w, w)

        def twin(one, two):
            return rows_of([both(lambda h: (one, hole)[h]), both(lambda h: (hole, two)[h])])

        def low_left(b):
            acc = [zero, zero]
            for qc in range(2):
                for p in pairs:
                    acc[qc] = jnp.where(even[p], dg[b, qc, :, rows(p, 1)], acc[qc])
            return acc[0].reshape(2 * n, 128) + turn(acc[1].reshape(2 * n, 128), n)

        def up_inv(b):
            parts = []
            for p in pairs:
                for q in range(2):
                    one, two = (inv[b, qc, q, rows(p, 0)].reshape(n, 128) for qc in range(2))
                    parts.append(jnp.where(first, one, turn(two, n)))
            return rows_of(parts)

        def low_inv(b):
            acc = [inv[b, qc, :, rows(0, 1)] for qc in range(2)]
            for qc in range(2):
                for p in pairs[1:]:
                    acc[qc] = acc[qc] + inv[b, qc, :, rows(p, 1)]
            return turn(acc[0].reshape(2 * n, 128), -n) + acc[1].reshape(2 * n, 128)

        def temp_rows(temp):
            temp = temp.reshape(shape)
            return rows_of([jnp.where(pair[p], temp[q], 0.0).reshape(n, 128) for p in pairs for q in range(2)])

        def product(lefts, rights):
            if len(lefts) == 1:
                return hdot(lefts[0], rights[0])
            return hdot(jnp.concatenate(lefts, axis=1), twin(*rights))

        here = [(lanes((w, 2, 8, 128)) >> shift) == 2 * p for p in pairs]

        def wide_rows(temp):
            temp = [temp[:, 128 * qc:128 * qc + 128].reshape(shape) for qc in range(2)]
            return rows_of([both(lambda qc: jnp.where(here[p], temp[qc][q], 0.0).reshape(n, 128))
                            for p in pairs for q in range(2)])

        if w < 4:
            temps = [hdot(low_left(b), rows_of([both(lambda qc: inv[b, qc, q, rows(p, 0)].reshape(n, 128))
                                                for p in pairs for q in range(2)])) for b in group]
            for b, temp in zip(group, temps):
                prod = -hdot(low_inv(b), wide_rows(temp))
                for qc in range(2):
                    val = prod[:, 128 * qc:128 * qc + 128].reshape(shape)
                    for p in pairs:
                        inv[b, qc, :, rows(p, 1)] = jnp.where(even[p], val, inv[b, qc, :, rows(p, 1)])
            return
        two_blocks = (group[:2], group[2:])
        temps = [product([low_left(b) for b in bs], [up_inv(b) for b in bs]) for bs in two_blocks]
        for bs, temp in zip(two_blocks, temps):
            prod = -product([low_inv(b) for b in bs],
                            [temp_rows(temp[:, 128 * h:128 * h + 128]) for h in range(len(bs))])
            for h, b in enumerate(bs):
                piece = prod[:, 128 * h:128 * h + 128]
                for qc, val in enumerate((piece, turn(piece, -n))):
                    val = val.reshape(shape)
                    for p in pairs:
                        inv[b, qc, :, rows(p, 1)] = jnp.where(even[p], val, inv[b, qc, :, rows(p, 1)])

    zst = [None] * 6

    def z_diag(j):
        return both(lambda qc: inv[j, qc, c, :, x].reshape(64, 128))

    def emit(i, j, blk):
        out[64 * i:64 * i + 64, 128 * j:128 * j + 128] = blk

    def add_terms(j, ks, acc):
        for k in ks:
            prod = (hdot2 if k == j + 1 else hdot)(zst[k], low_block(k, j))
            for i in range(k, 6):
                part = prod[64 * (i - k):64 * (i - k) + 64]
                acc[i] = part if acc[i] is None else acc[i] + part

    def finish(j, acc):
        emit(j, j, inv[j, y, c, :, x].reshape(64, 128))
        if j == 5:
            zst[5] = z_diag(5)
            return
        res = -hdot2(rows_of(acc[j + 1:]), inv_full(j))
        zst[j] = rows_of([z_diag(j), res])
        mine = jnp.where(y == 0, res[:, 0:128], res[:, 128:256])
        for i in range(j + 1, 6):
            emit(i, j, mine[64 * (i - j - 1):64 * (i - j)])

    def empty():
        return [None] * 6

    def finish_first(acc, rows):
        res = -hdot(rows_of([acc[i] for i in rows]), inv[0, y].reshape(256, 128))
        for n, i in enumerate(rows):
            emit(i, 0, res[64 * n:64 * n + 64])

    def c_block(k, j):
        return cbuf[c_at(k, j)].reshape(256, 128)

    def u_compute_top():
        prod = hdot(z_diag(3), jnp.concatenate([c_block(3, j) for j in range(3)], axis=1))
        for j in range(3):
            utop[y, j] = prod[:, 128 * j:128 * j + 128]

    def u_compute(j):
        both_rows = hdot(zst[3][64:192], c_block(3, j)) + hdot(zst[4], c_block(4, j))
        ubuf[j, y, 0:64] = both_rows[0:64]
        ubuf[j, y, 64:128] = both_rows[64:128] + hdot(zst[5], c_block(5, j))

    def u_rows(i, j, q):
        if i == 3:
            return utop[q, j]
        return ubuf[j, q, 64 * (i - 4):64 * (i - 3)]

    def u_add(j, acc, rows=(3, 4, 5)):
        for i in rows:
            part = both(lambda q: u_rows(i, j, q))
            acc[i] = part if acc[i] is None else acc[i] + part

    pack(DB)
    pl.semaphore_wait(barrier, 3)
    own(DB, "yx")
    ready(BO)
    own(BO, "sx")
    own(DB, "s")
    own(BO, "y")
    from_x(DB)
    pack(DA)
    own(DA, "yx")
    from_y(DB)
    c_own(3)
    from_x(BO)
    c_own(2)
    own(DA, "s")
    c_own(0)
    for i in range(5):
        out[64 * i:64 * i + 64, 128 * (i + 1):768] = jnp.zeros((64, 128 * (5 - i)), F32)
    from_diag(DB)
    wait_sib(DB)
    from_y(DA)
    from_x(DA)
    unpack(DB)
    base(3)
    c_own(1)
    double(DIAG[DB], 1)
    ready(A1)
    own(A1, "y")
    from_y(BO)
    c_relay(3)
    double(DIAG[DB], 2)
    own(A1, "x")
    from_diag(BO)
    ready(A2)
    own(A2, "xy")
    double(DIAG[DB], 4)
    c_wait(3)
    u_compute_top()
    u_send_to(3)
    from_diag(DA)
    wait_sib(BO)
    c_relay(2)
    finish(5, None)
    acc = empty()
    add_terms(4, (5,), acc)
    finish(4, acc)
    acc = empty()
    add_terms(3, (5, 4), acc)
    finish(3, acc)
    c_relay(1)
    from_y(A1)
    c_relay(0)
    wait_sib(DA)
    c_wait(2)
    unpack(DA)
    u_compute(2)
    base(0)
    u_send_to(2)
    own(A1, "s")
    own(A2, "s")
    from_y(A2)
    c_wait(1)
    u_compute(1)
    double(DIAG[DA], 1)
    u_send_to(1)
    c_wait(0)
    from_x(A2)
    from_x(A1)
    u_compute(0)
    double(DIAG[DA], 2)
    u_send_to(0)
    from_diag(A1)
    double(DIAG[DA], 4)
    emit(0, 0, inv[0, y, c, :, x].reshape(64, 128))
    from_diag(A2)
    u_wait(3)
    u_wait(2)
    acc = empty()
    u_add(2, acc)
    finish(2, acc)
    wait_sib(A1)
    acc = empty()
    add_terms(1, (2,), acc)
    first = empty()
    add_terms(0, (2,), first)
    u_wait(1)
    wait_sib(A2)
    u_add(1, acc)
    finish(1, acc)
    add_terms(0, (1,), first)
    u_add(0, first, (3,))
    finish_first(first, (1, 2, 3))
    u_wait(0)
    u_add(0, first, (4, 5))
    finish_first(first, (4, 5))

    for cp in sends:
        cp.wait_send()


def solution(mesh):
    spec = P(("batch", "row"), "col")

    def body(local_l):
        rows, cols = local_l.shape
        return pl.pallas_call(
            kernel,
            out_shape=jax.ShapeDtypeStruct((rows, cols), F32),
            in_specs=[pl.BlockSpec(memory_space=pltpu.HBM)],
            out_specs=pl.BlockSpec(memory_space=pltpu.VMEM),
            scratch_shapes=[
                pltpu.VMEM((6, 8, 8, 128), F32),
                pltpu.VMEM((2, 2, 2, 2, 14, 8, 128), F32),
                pltpu.VMEM((6, 2, 2, 8, 2, 8, 128), F32),
                pltpu.VMEM((6, 2, 2, 8, 2, 8, 128), F32),
                pltpu.VMEM((9, 2, 8, 2, 8, 128), F32),
                pltpu.VMEM((2, 3, 64, 128), F32),
                pltpu.VMEM((3, 2, 128, 128), F32),
                pltpu.VMEM((6, 2, 2, 8, 2, 8, 128), F32),
                pltpu.SemaphoreType.DMA((21,)),
                pltpu.SemaphoreType.DMA((5, 7)),
                pltpu.SemaphoreType.DMA((5, 7)),
                pltpu.SemaphoreType.DMA((4, 3)),
                pltpu.SemaphoreType.DMA((4, 3)),
                pltpu.SemaphoreType.DMA((4,)),
                pltpu.SemaphoreType.DMA((4,)),
            ],
            compiler_params=pltpu.CompilerParams(
                collective_id=0, has_side_effects=True, vmem_limit_bytes=40 * 1024 * 1024),
        )(pltpu.with_memory_space_constraint(local_l.reshape(rows // 8, 8, cols), pltpu.HBM))

    return jax.shard_map(body, mesh=mesh, in_specs=(spec,), out_specs=spec, check_vma=False)
```

```python
import jax
import jax.numpy as jnp
from jax import lax
from jax.experimental import pallas as pl
from jax.experimental.pallas import tpu as pltpu
from jax.sharding import PartitionSpec as P

MESH = pl.DeviceIdType.MESH
F32 = jnp.float32
DB, DA, BO, A1, A2 = range(5)
DIAG = {DB: (5, 4, 3), DA: (2, 1, 0)}
OFF = {BO: ((5, 4), (4, 3), (5, 3)), A1: ((2, 1), (2, 0)), A2: ((1, 0),)}
OFF_AT = {blk: n for n, blk in enumerate(blk for grp in OFF.values() for blk in grp)}
LAST_X = (A1, A2,)


CGRP = [[(4, j), (5, j)] for j in range(3)] + [[(3, j) for j in range(3)]]


def c_at(k, j):
    return 6 + j if k == 3 else 2 * j + k - 4


def hdot(left, right):
    return jnp.dot(left, right, precision=lax.Precision.HIGHEST, preferred_element_type=F32)


def hdot2(left, right):
    half = left.shape[0] // 16 * 8
    return jnp.concatenate([hdot(left[:half], right), hdot(left[half:], right)], axis=0)


def kernel(inp, out, raw, dpk, dg, goff, cbuf, utop, ubuf, inv, loc_sem, g_send, g_recv, c_send, c_recv, u_send, u_recv):
    row = lax.axis_index("row")
    y = lax.axis_index("col")
    x = row // 2
    c = row % 2
    xo, yo, co = 1 - x, 1 - y, 1 - c
    sib = {"row": 2 * x + co}
    xnb = {"row": 2 * xo + c}
    ynb = {"col": yo}

    barrier = pltpu.get_barrier_semaphore()
    for nbr in (sib, xnb, ynb):
        pl.semaphore_signal(barrier, inc=1, device_id=nbr, device_id_type=MESH)

    def take(bi, bj, dst, sem):
        return pltpu.make_async_copy(inp.at[pl.ds(8 * bi, 8), :, pl.ds(128 * bj, 128)], dst, sem)

    local = {g: [take(b, b, raw.at[b], loc_sem.at[b]) for b in DIAG[g]] for g in DIAG}
    for g in OFF:
        local[g] = [take(bi, bj, goff.at[OFF_AT[bi, bj], y, c, :, x], loc_sem.at[6 + OFF_AT[bi, bj]]) for bi, bj in OFF[g]]
    local_c = [[take(bi, bj, cbuf.at[c_at(bi, bj), c, :, x], loc_sem.at[12 + c_at(bi, bj)]) for bi, bj in grp] for grp in CGRP]
    for grp in (local[DB], local[BO], local[DA], local_c[3], local_c[2], local[A1], local_c[1], local_c[0], local[A2]):
        for cp in grp:
            cp.start()

    sub = lax.broadcasted_iota(jnp.int32, (8, 128), 0)
    lane = lax.broadcasted_iota(jnp.int32, (8, 128), 1)

    def lanes(shape):
        return lax.broadcasted_iota(jnp.int32, shape, len(shape) - 1)

    def along(tile, idx):
        return jnp.take_along_axis(tile, idx, axis=1, mode="promise_in_bounds")

    def turn(tile, n):
        return along(tile, (lanes(tile.shape) + (128 - n)) & 127)

    def pack(g):
        for cp in local[g]:
            cp.wait()
        for i, b in enumerate(DIAG[g]):
            dpk[g, y, c, x, 4 * i] = raw[b, 7]
            for p in range(3):
                n = 112 - 16 * p
                dpk[g, y, c, x, 4 * i + 1 + p] = jnp.where(lane < n, raw[b, 6 - p], turn(raw[b, p], n))
        one, two, three = DIAG[g]
        dpk[g, y, c, x, 12] = jnp.where(lane < 64, raw[one, 3], turn(raw[two, 3], 64))
        dpk[g, y, c, x, 13] = raw[three, 3]

    def unpack(g):
        for i, b in enumerate(DIAG[g]):
            for qc in range(2):
                for lb in range(8):
                    at = 4 * i + (7 - lb if lb > 3 else 1 + lb)
                    n = 16 * (lb + 1)
                    if lb == 3:
                        at, n = 12 + i // 2, 64 * (i % 2)
                    tiles = dpk[g, qc, :, :, at]
                    if lb < 4 and n:
                        tiles = turn(tiles.reshape(32, 128), n).reshape(2, 2, 8, 128)
                    dg[b, qc, :, lb] = tiles

    def slot(g, sx, sc, sy):
        if g in DIAG:
            return dpk.at[g, sy, sc, sx]
        return goff.at[pl.ds(OFF_AT[OFF[g][0]], len(OFF[g])), sy, sc, :, sx]

    sends = []

    def copy(ref, send, recv, dev):
        return pltpu.make_async_remote_copy(ref, ref, send, recv, device_id=dev, device_id_type=MESH)

    def start(cp):
        cp.start()
        sends.append(cp)

    def gsend(g, k, ref, dev):
        start(copy(ref, g_send.at[g, k], g_recv.at[g, k], dev))

    def gwait(g, k, ref):
        copy(ref, g_send.at[g, k], g_recv.at[g, k], sib).wait_recv()

    def own(g, to):
        for k, dev in enumerate((xnb, ynb, sib)):
            if "xys"[k] in to:
                gsend(g, k, slot(g, x, c, y), dev)

    def ready(g):
        for cp in local[g]:
            cp.wait()

    def from_x(g):
        gwait(g, 0, slot(g, xo, c, y))
        if g not in LAST_X:
            gsend(g, 3, slot(g, xo, c, y), ynb)
        gsend(g, 4, slot(g, xo, c, y), sib)

    def from_y(g):
        gwait(g, 1, slot(g, x, c, yo))
        if g in LAST_X:
            gsend(g, 3, slot(g, x, c, yo), xnb)
        gsend(g, 5, slot(g, x, c, yo), sib)

    def from_diag(g):
        gwait(g, 3, slot(g, xo, c, yo))
        gsend(g, 6, slot(g, xo, c, yo), sib)

    def wait_sib(g):
        for k, ref in ((2, slot(g, x, co, y)), (4, slot(g, xo, co, y)), (5, slot(g, x, co, yo)), (6, slot(g, xo, co, yo))):
            gwait(g, k, ref)

    def c_slot(g, sx, sc):
        return cbuf.at[pl.ds(c_at(*CGRP[g][0]), len(CGRP[g])), sc, :, sx]

    def c_own(g):
        for cp in local_c[g]:
            cp.wait()
        for k, dev in enumerate((xnb, sib)):
            start(copy(c_slot(g, x, c), c_send.at[g, k], c_recv.at[g, k], dev))

    def c_relay(g):
        copy(c_slot(g, xo, c), c_send.at[g, 0], c_recv.at[g, 0], sib).wait_recv()
        start(copy(c_slot(g, xo, c), c_send.at[g, 2], c_recv.at[g, 2], sib))

    def c_wait(g):
        copy(c_slot(g, x, co), c_send.at[g, 1], c_recv.at[g, 1], sib).wait_recv()
        copy(c_slot(g, xo, co), c_send.at[g, 2], c_recv.at[g, 2], sib).wait_recv()

    def u_slot(g, sy):
        return utop.at[sy] if g == 3 else ubuf.at[g, sy]

    def u_send_to(g):
        start(copy(u_slot(g, y), u_send.at[g], u_recv.at[g], ynb))

    def u_wait(g):
        copy(u_slot(g, yo), u_send.at[g], u_recv.at[g], ynb).wait_recv()

    def base(at):
        sub3 = lax.broadcasted_iota(jnp.int32, (3, 8, 128), 1)
        lane3 = lanes((3, 8, 128))
        seg3 = lane3 >> 4
        seg24 = lanes((24, 128)) & 112
        here = [(sub3 == (lane3 & 7)) & (((lane3 >> 3) & 1) == xr) for xr in range(2)]
        segs = [seg3 == lb for lb in range(8)]
        low = [[None, None] for _ in range(4)]
        for nb in range(4):
            xr, qr = nb // 2, nb % 2
            for qc in range(2):
                acc = dg[at:at + 3, qc, qr, 0, xr]
                for lb in range(1, 8):
                    acc = jnp.where(segs[lb], dg[at:at + 3, qc, qr, lb, xr], acc)
                low[nb][qc] = acc
        rec = []
        for qc in range(2):
            dsum = jnp.where(here[0], low[qc][qc], 0.0) + jnp.where(here[1], low[2 + qc][qc], 0.0)
            rec.append(1.0 / jnp.sum(dsum, axis=1, keepdims=True))
        rhs = []
        for nb in range(4):
            for qc in range(2):
                low[nb][qc] = (low[nb][qc] * rec[qc]).reshape(24, 128)
            rhs.append([jnp.where(here[nb // 2], 1.0, 0.0) if nb % 2 == qc else jnp.zeros((3, 8, 128), F32)
                        for qc in range(2)])
        below = [sub3 > ek for ek in range(7)]
        for k in range(32):
            nk, ek = k // 8, k % 8
            xk, qk = nk // 2, nk % 2
            idx = seg24 + (8 * xk + ek)
            pivot = [rhs[nk][qc][:, ek:ek + 1, :] for qc in range(2)]
            for nb in range(nk, 4):
                if nb == nk and ek == 7:
                    continue
                col = along(low[nb][qk], idx).reshape(3, 8, 128)
                if nb == nk:
                    col = jnp.where(below[ek], col, 0.0)
                for qc in range(2):
                    rhs[nb][qc] = rhs[nb][qc] - col * pivot[qc]
        for nb in range(4):
            xr, qr = nb // 2, nb % 2
            idx = (seg3 * 16 + 8 * xr + sub3).reshape(24, 128)
            scale = along(jnp.broadcast_to(rec[qr], (3, 8, 128)).reshape(24, 128), idx).reshape(3, 8, 128)
            for qc in range(2):
                val = rhs[nb][qc] * scale
                for lb in range(8):
                    inv[at:at + 3, qc, qr, lb, xr] = jnp.where(segs[lb], val, 0.0)

    def both(ref_of):
        return jnp.concatenate([ref_of(0), ref_of(1)], axis=1)

    def inv_full(b):
        return both(lambda qc: inv[b, qc].reshape(256, 128))

    def low_block(k, j):
        return both(lambda qc: goff[OFF_AT[k, j], qc].reshape(256, 128))

    def rows_of(tiles):
        return jnp.concatenate(tiles, axis=0)

    def double(group, w):
        pairs = range(4 // w)
        n = 16 * w
        shift = {1: 4, 2: 5, 4: 6}[w]
        shape = (2, w, 2, 8, 128)
        part = lanes(shape) >> shift
        even = [part == 2 * p for p in pairs]
        pair = [(lanes((w, 2, 8, 128)) >> (shift + 1)) == p for p in pairs]
        zero = jnp.zeros(shape, F32)
        first = (lanes((n, 128)) & n) == 0
        hole = jnp.zeros((128, 128), F32)

        def rows(p, odd):
            return pl.ds((2 * p + odd) * w, w)

        def twin(one, two):
            return rows_of([both(lambda h: (one, hole)[h]), both(lambda h: (hole, two)[h])])

        def low_left(b):
            acc = [zero, zero]
            for qc in range(2):
                for p in pairs:
                    acc[qc] = jnp.where(even[p], dg[b, qc, :, rows(p, 1)], acc[qc])
            return acc[0].reshape(2 * n, 128) + turn(acc[1].reshape(2 * n, 128), n)

        def up_inv(b):
            parts = []
            for p in pairs:
                for q in range(2):
                    one, two = (inv[b, qc, q, rows(p, 0)].reshape(n, 128) for qc in range(2))
                    parts.append(jnp.where(first, one, turn(two, n)))
            return rows_of(parts)

        def low_inv(b):
            acc = [inv[b, qc, :, rows(0, 1)] for qc in range(2)]
            for qc in range(2):
                for p in pairs[1:]:
                    acc[qc] = acc[qc] + inv[b, qc, :, rows(p, 1)]
            return turn(acc[0].reshape(2 * n, 128), -n) + acc[1].reshape(2 * n, 128)

        def temp_rows(temp):
            temp = temp.reshape(shape)
            return rows_of([jnp.where(pair[p], temp[q], 0.0).reshape(n, 128) for p in pairs for q in range(2)])

        def product(lefts, rights):
            if len(lefts) == 1:
                return hdot(lefts[0], rights[0])
            return hdot(jnp.concatenate(lefts, axis=1), twin(*rights))

        here = [(lanes((w, 2, 8, 128)) >> shift) == 2 * p for p in pairs]

        def wide_rows(temp):
            temp = [temp[:, 128 * qc:128 * qc + 128].reshape(shape) for qc in range(2)]
            return rows_of([both(lambda qc: jnp.where(here[p], temp[qc][q], 0.0).reshape(n, 128))
                            for p in pairs for q in range(2)])

        if w < 4:
            temps = [hdot(low_left(b), rows_of([both(lambda qc: inv[b, qc, q, rows(p, 0)].reshape(n, 128))
                                                for p in pairs for q in range(2)])) for b in group]
            for b, temp in zip(group, temps):
                prod = -hdot(low_inv(b), wide_rows(temp))
                for qc in range(2):
                    val = prod[:, 128 * qc:128 * qc + 128].reshape(shape)
                    for p in pairs:
                        inv[b, qc, :, rows(p, 1)] = jnp.where(even[p], val, inv[b, qc, :, rows(p, 1)])
            return
        two_blocks = (group[:2], group[2:])
        temps = [product([low_left(b) for b in bs], [up_inv(b) for b in bs]) for bs in two_blocks]
        for bs, temp in zip(two_blocks, temps):
            prod = -product([low_inv(b) for b in bs],
                            [temp_rows(temp[:, 128 * h:128 * h + 128]) for h in range(len(bs))])
            for h, b in enumerate(bs):
                piece = prod[:, 128 * h:128 * h + 128]
                for qc, val in enumerate((piece, turn(piece, -n))):
                    val = val.reshape(shape)
                    for p in pairs:
                        inv[b, qc, :, rows(p, 1)] = jnp.where(even[p], val, inv[b, qc, :, rows(p, 1)])

    zst = [None] * 6

    def z_diag(j):
        return both(lambda qc: inv[j, qc, c, :, x].reshape(64, 128))

    def emit(i, j, blk):
        out[64 * i:64 * i + 64, 128 * j:128 * j + 128] = blk

    def add_terms(j, ks, acc):
        for k in ks:
            prod = (hdot2 if k == 1 else hdot)(zst[k], low_block(k, j))
            for i in range(k, 6):
                part = prod[64 * (i - k):64 * (i - k) + 64]
                acc[i] = part if acc[i] is None else acc[i] + part

    def finish(j, acc):
        emit(j, j, inv[j, y, c, :, x].reshape(64, 128))
        if j == 5:
            zst[5] = z_diag(5)
            return
        res = -(hdot2 if j < 3 else hdot)(rows_of(acc[j + 1:]), inv_full(j))
        zst[j] = rows_of([z_diag(j), res])
        mine = jnp.where(y == 0, res[:, 0:128], res[:, 128:256])
        for i in range(j + 1, 6):
            emit(i, j, mine[64 * (i - j - 1):64 * (i - j)])

    def empty():
        return [None] * 6

    def finish_first(acc, rows):
        res = -hdot(rows_of([acc[i] for i in rows]), inv[0, y].reshape(256, 128))
        for n, i in enumerate(rows):
            emit(i, 0, res[64 * n:64 * n + 64])

    def c_block(k, j):
        return cbuf[c_at(k, j)].reshape(256, 128)

    def u_compute_top():
        prod = hdot(z_diag(3), jnp.concatenate([c_block(3, j) for j in range(3)], axis=1))
        for j in range(3):
            utop[y, j] = prod[:, 128 * j:128 * j + 128]

    def u_compute(j):
        both_rows = hdot(zst[3][64:192], c_block(3, j)) + hdot(zst[4], c_block(4, j))
        ubuf[j, y, 0:64] = both_rows[0:64]
        ubuf[j, y, 64:128] = both_rows[64:128] + hdot(zst[5], c_block(5, j))

    def u_rows(i, j, q):
        if i == 3:
            return utop[q, j]
        return ubuf[j, q, 64 * (i - 4):64 * (i - 3)]

    def u_add(j, acc, rows=(3, 4, 5)):
        for i in rows:
            part = both(lambda q: u_rows(i, j, q))
            acc[i] = part if acc[i] is None else acc[i] + part

    pack(DB)
    pl.semaphore_wait(barrier, 3)
    own(DB, "yx")
    ready(BO)
    own(BO, "sx")
    own(DB, "s")
    own(BO, "y")
    from_x(DB)
    pack(DA)
    own(DA, "yx")
    from_y(DB)
    c_own(3)
    from_x(BO)
    c_own(2)
    own(DA, "s")
    c_own(0)
    for i in range(5):
        out[64 * i:64 * i + 64, 128 * (i + 1):768] = jnp.zeros((64, 128 * (5 - i)), F32)
    from_diag(DB)
    wait_sib(DB)
    from_y(DA)
    from_x(DA)
    unpack(DB)
    base(3)
    c_own(1)
    double(DIAG[DB], 1)
    ready(A1)
    own(A1, "y")
    from_y(BO)
    c_relay(3)
    double(DIAG[DB], 2)
    own(A1, "x")
    from_diag(BO)
    ready(A2)
    own(A2, "xy")
    double(DIAG[DB], 4)
    c_wait(3)
    u_compute_top()
    u_send_to(3)
    from_diag(DA)
    wait_sib(BO)
    c_relay(2)
    finish(5, None)
    acc = empty()
    add_terms(4, (5,), acc)
    finish(4, acc)
    acc = empty()
    add_terms(3, (5, 4), acc)
    finish(3, acc)
    c_relay(1)
    from_y(A1)
    c_relay(0)
    wait_sib(DA)
    c_wait(2)
    unpack(DA)
    u_compute(2)
    base(0)
    u_send_to(2)
    own(A1, "s")
    own(A2, "s")
    from_y(A2)
    c_wait(1)
    u_compute(1)
    double(DIAG[DA], 1)
    u_send_to(1)
    c_wait(0)
    from_x(A2)
    from_x(A1)
    u_compute(0)
    double(DIAG[DA], 2)
    last_u = copy(ubuf.at[0, y], u_send.at[0], u_recv.at[0], ynb)
    sends.append(last_u)
    pl.when(c == 0)(last_u.start)
    from_diag(A1)
    double(DIAG[DA], 4)
    pl.when(c == 1)(last_u.start)
    emit(0, 0, inv[0, y, c, :, x].reshape(64, 128))
    from_diag(A2)
    u_wait(3)
    u_wait(2)
    acc = empty()
    u_add(2, acc)
    finish(2, acc)
    wait_sib(A1)
    acc = empty()
    add_terms(1, (2,), acc)
    first = empty()
    add_terms(0, (2,), first)
    u_wait(1)
    wait_sib(A2)
    u_add(1, acc)
    finish(1, acc)
    add_terms(0, (1,), first)
    u_add(0, first, (3,))
    finish_first(first, (1, 2, 3))
    u_wait(0)
    u_add(0, first, (4, 5))
    finish_first(first, (4, 5))

    for cp in sends:
        cp.wait_send()


def solution(mesh):
    spec = P(("batch", "row"), "col")

    def body(local_l):
        rows, cols = local_l.shape
        return pl.pallas_call(
            kernel,
            out_shape=jax.ShapeDtypeStruct((rows, cols), F32),
            in_specs=[pl.BlockSpec(memory_space=pltpu.HBM)],
            out_specs=pl.BlockSpec(memory_space=pltpu.VMEM),
            scratch_shapes=[
                pltpu.VMEM((6, 8, 8, 128), F32),
                pltpu.VMEM((2, 2, 2, 2, 14, 8, 128), F32),
                pltpu.VMEM((6, 2, 2, 8, 2, 8, 128), F32),
                pltpu.VMEM((6, 2, 2, 8, 2, 8, 128), F32),
                pltpu.VMEM((9, 2, 8, 2, 8, 128), F32),
                pltpu.VMEM((2, 3, 64, 128), F32),
                pltpu.VMEM((3, 2, 128, 128), F32),
                pltpu.VMEM((6, 2, 2, 8, 2, 8, 128), F32),
                pltpu.SemaphoreType.DMA((21,)),
                pltpu.SemaphoreType.DMA((5, 7)),
                pltpu.SemaphoreType.DMA((5, 7)),
                pltpu.SemaphoreType.DMA((4, 3)),
                pltpu.SemaphoreType.DMA((4, 3)),
                pltpu.SemaphoreType.DMA((4,)),
                pltpu.SemaphoreType.DMA((4,)),
            ],
            compiler_params=pltpu.CompilerParams(
                collective_id=0, has_side_effects=True, vmem_limit_bytes=40 * 1024 * 1024),
        )(pltpu.with_memory_space_constraint(local_l.reshape(rows // 8, 8, cols), pltpu.HBM))

    return jax.shard_map(body, mesh=mesh, in_specs=(spec,), out_specs=spec, check_vma=False)
```

```python
import jax
import jax.numpy as jnp
from jax import lax
from jax.experimental import pallas as pl
from jax.experimental.pallas import tpu as pltpu
from jax.sharding import PartitionSpec as P

MESH = pl.DeviceIdType.MESH
F32 = jnp.float32
DB, DA, BO, A1, A2 = range(5)
DIAG = {DB: (5, 4, 3), DA: (2, 1, 0)}
OFF = {BO: ((5, 4), (4, 3), (5, 3)), A1: ((2, 1), (2, 0)), A2: ((1, 0),)}
OFF_AT = {blk: n for n, blk in enumerate(blk for grp in OFF.values() for blk in grp)}
LAST_X = (A1, A2,)


CGRP = [[(4, j), (5, j)] for j in range(3)] + [[(3, j) for j in range(3)]]


def c_at(k, j):
    return 6 + j if k == 3 else 2 * j + k - 4


def hdot(left, right):
    return jnp.dot(left, right, precision=lax.Precision.HIGHEST, preferred_element_type=F32)


def hdot2(left, right):
    half = left.shape[0] // 16 * 8
    return jnp.concatenate([hdot(left[:half], right), hdot(left[half:], right)], axis=0)


def kernel(inp, out, raw, dpk, dg, goff, cbuf, utop, ubuf, inv, loc_sem, g_send, g_recv, c_send, c_recv, u_send, u_recv):
    row = lax.axis_index("row")
    y = lax.axis_index("col")
    x = row // 2
    c = row % 2
    xo, yo, co = 1 - x, 1 - y, 1 - c
    sib = {"row": 2 * x + co}
    xnb = {"row": 2 * xo + c}
    ynb = {"col": yo}

    barrier = pltpu.get_barrier_semaphore()
    for nbr in (sib, xnb, ynb):
        pl.semaphore_signal(barrier, inc=1, device_id=nbr, device_id_type=MESH)

    def take(bi, bj, dst, sem):
        return pltpu.make_async_copy(inp.at[pl.ds(8 * bi, 8), :, pl.ds(128 * bj, 128)], dst, sem)

    local = {g: [take(b, b, raw.at[b], loc_sem.at[b]) for b in DIAG[g]] for g in DIAG}
    for g in OFF:
        local[g] = [take(bi, bj, goff.at[OFF_AT[bi, bj], y, c, :, x], loc_sem.at[6 + OFF_AT[bi, bj]]) for bi, bj in OFF[g]]
    local_c = [[take(bi, bj, cbuf.at[c_at(bi, bj), c, :, x], loc_sem.at[12 + c_at(bi, bj)]) for bi, bj in grp] for grp in CGRP]
    for grp in (local[DB], local[BO], local[DA], local_c[3], local_c[2], local[A1], local_c[1], local_c[0], local[A2]):
        for cp in grp:
            cp.start()

    sub = lax.broadcasted_iota(jnp.int32, (8, 128), 0)
    lane = lax.broadcasted_iota(jnp.int32, (8, 128), 1)

    def lanes(shape):
        return lax.broadcasted_iota(jnp.int32, shape, len(shape) - 1)

    def along(tile, idx):
        return jnp.take_along_axis(tile, idx, axis=1, mode="promise_in_bounds")

    def turn(tile, n):
        return along(tile, (lanes(tile.shape) + (128 - n)) & 127)

    def pack(g):
        for cp in local[g]:
            cp.wait()
        for i, b in enumerate(DIAG[g]):
            dpk[g, y, c, x, 4 * i] = raw[b, 7]
            for p in range(3):
                n = 112 - 16 * p
                dpk[g, y, c, x, 4 * i + 1 + p] = jnp.where(lane < n, raw[b, 6 - p], turn(raw[b, p], n))
        one, two, three = DIAG[g]
        dpk[g, y, c, x, 12] = jnp.where(lane < 64, raw[one, 3], turn(raw[two, 3], 64))
        dpk[g, y, c, x, 13] = raw[three, 3]

    def unpack(g):
        for i, b in enumerate(DIAG[g]):
            for qc in range(2):
                for lb in range(8):
                    at = 4 * i + (7 - lb if lb > 3 else 1 + lb)
                    n = 16 * (lb + 1)
                    if lb == 3:
                        at, n = 12 + i // 2, 64 * (i % 2)
                    tiles = dpk[g, qc, :, :, at]
                    if lb < 4 and n:
                        tiles = turn(tiles.reshape(32, 128), n).reshape(2, 2, 8, 128)
                    dg[b, qc, :, lb] = tiles

    def slot(g, sx, sc, sy):
        if g in DIAG:
            return dpk.at[g, sy, sc, sx]
        return goff.at[pl.ds(OFF_AT[OFF[g][0]], len(OFF[g])), sy, sc, :, sx]

    sends = []

    def copy(ref, send, recv, dev):
        return pltpu.make_async_remote_copy(ref, ref, send, recv, device_id=dev, device_id_type=MESH)

    def start(cp):
        cp.start()
        sends.append(cp)

    def gsend(g, k, ref, dev):
        start(copy(ref, g_send.at[g, k], g_recv.at[g, k], dev))

    def gwait(g, k, ref):
        copy(ref, g_send.at[g, k], g_recv.at[g, k], sib).wait_recv()

    def own(g, to):
        for k, dev in enumerate((xnb, ynb, sib)):
            if "xys"[k] in to:
                gsend(g, k, slot(g, x, c, y), dev)

    def ready(g):
        for cp in local[g]:
            cp.wait()

    def from_x(g):
        gwait(g, 0, slot(g, xo, c, y))
        if g not in LAST_X:
            gsend(g, 3, slot(g, xo, c, y), ynb)
        gsend(g, 4, slot(g, xo, c, y), sib)

    def from_y(g):
        gwait(g, 1, slot(g, x, c, yo))
        if g in LAST_X:
            gsend(g, 3, slot(g, x, c, yo), xnb)
        gsend(g, 5, slot(g, x, c, yo), sib)

    def from_diag(g):
        gwait(g, 3, slot(g, xo, c, yo))
        gsend(g, 6, slot(g, xo, c, yo), sib)

    def wait_sib(g):
        for k, ref in ((2, slot(g, x, co, y)), (4, slot(g, xo, co, y)), (5, slot(g, x, co, yo)), (6, slot(g, xo, co, yo))):
            gwait(g, k, ref)

    def c_slot(g, sx, sc):
        return cbuf.at[pl.ds(c_at(*CGRP[g][0]), len(CGRP[g])), sc, :, sx]

    def c_own(g):
        for cp in local_c[g]:
            cp.wait()
        for k, dev in enumerate((xnb, sib)):
            start(copy(c_slot(g, x, c), c_send.at[g, k], c_recv.at[g, k], dev))

    def c_relay(g):
        copy(c_slot(g, xo, c), c_send.at[g, 0], c_recv.at[g, 0], sib).wait_recv()
        start(copy(c_slot(g, xo, c), c_send.at[g, 2], c_recv.at[g, 2], sib))

    def c_wait(g):
        copy(c_slot(g, x, co), c_send.at[g, 1], c_recv.at[g, 1], sib).wait_recv()
        copy(c_slot(g, xo, co), c_send.at[g, 2], c_recv.at[g, 2], sib).wait_recv()

    def u_slot(g, sy):
        return utop.at[sy] if g == 3 else ubuf.at[g, sy]

    def u_copy(g):
        return copy(u_slot(g, y), u_send.at[g], u_recv.at[g], ynb)

    def u_send_to(g):
        start(u_copy(g))

    def u_wait(g):
        copy(u_slot(g, yo), u_send.at[g], u_recv.at[g], ynb).wait_recv()

    def base(at):
        sub3 = lax.broadcasted_iota(jnp.int32, (3, 8, 128), 1)
        lane3 = lanes((3, 8, 128))
        seg3 = lane3 >> 4
        seg24 = lanes((24, 128)) & 112
        here = [(sub3 == (lane3 & 7)) & (((lane3 >> 3) & 1) == xr) for xr in range(2)]
        segs = [seg3 == lb for lb in range(8)]
        low = [[None, None] for _ in range(4)]
        for nb in range(4):
            xr, qr = nb // 2, nb % 2
            for qc in range(2):
                acc = dg[at:at + 3, qc, qr, 0, xr]
                for lb in range(1, 8):
                    acc = jnp.where(segs[lb], dg[at:at + 3, qc, qr, lb, xr], acc)
                low[nb][qc] = acc
        rec = []
        for qc in range(2):
            dsum = jnp.where(here[0], low[qc][qc], 0.0) + jnp.where(here[1], low[2 + qc][qc], 0.0)
            rec.append(1.0 / jnp.sum(dsum, axis=1, keepdims=True))
        rhs = []
        for nb in range(4):
            for qc in range(2):
                low[nb][qc] = (low[nb][qc] * rec[qc]).reshape(24, 128)
            rhs.append([jnp.where(here[nb // 2], 1.0, 0.0) if nb % 2 == qc else jnp.zeros((3, 8, 128), F32)
                        for qc in range(2)])
        below = [sub3 > ek for ek in range(7)]
        for k in range(32):
            nk, ek = k // 8, k % 8
            xk, qk = nk // 2, nk % 2
            idx = seg24 + (8 * xk + ek)
            pivot = [rhs[nk][qc][:, ek:ek + 1, :] for qc in range(2)]
            for nb in range(nk, 4):
                if nb == nk and ek == 7:
                    continue
                col = along(low[nb][qk], idx).reshape(3, 8, 128)
                if nb == nk:
                    col = jnp.where(below[ek], col, 0.0)
                for qc in range(2):
                    rhs[nb][qc] = rhs[nb][qc] - col * pivot[qc]
        for nb in range(4):
            xr, qr = nb // 2, nb % 2
            idx = (seg3 * 16 + 8 * xr + sub3).reshape(24, 128)
            scale = along(jnp.broadcast_to(rec[qr], (3, 8, 128)).reshape(24, 128), idx).reshape(3, 8, 128)
            for qc in range(2):
                val = rhs[nb][qc] * scale
                for lb in range(8):
                    inv[at:at + 3, qc, qr, lb, xr] = jnp.where(segs[lb], val, 0.0)

    def both(ref_of):
        return jnp.concatenate([ref_of(0), ref_of(1)], axis=1)

    def inv_full(b):
        return both(lambda qc: inv[b, qc].reshape(256, 128))

    def low_block(k, j):
        return both(lambda qc: goff[OFF_AT[k, j], qc].reshape(256, 128))

    def rows_of(tiles):
        return jnp.concatenate(tiles, axis=0)

    def double(group, w):
        pairs = range(4 // w)
        n = 16 * w
        shift = {1: 4, 2: 5, 4: 6}[w]
        shape = (2, w, 2, 8, 128)
        part = lanes(shape) >> shift
        even = [part == 2 * p for p in pairs]
        pair = [(lanes((w, 2, 8, 128)) >> (shift + 1)) == p for p in pairs]
        zero = jnp.zeros(shape, F32)
        first = (lanes((n, 128)) & n) == 0
        hole = jnp.zeros((128, 128), F32)

        def rows(p, odd):
            return pl.ds((2 * p + odd) * w, w)

        def twin(one, two):
            return rows_of([both(lambda h: (one, hole)[h]), both(lambda h: (hole, two)[h])])

        def low_left(b):
            acc = [zero, zero]
            for qc in range(2):
                for p in pairs:
                    acc[qc] = jnp.where(even[p], dg[b, qc, :, rows(p, 1)], acc[qc])
            return acc[0].reshape(2 * n, 128) + turn(acc[1].reshape(2 * n, 128), n)

        def up_inv(b):
            parts = []
            for p in pairs:
                for q in range(2):
                    one, two = (inv[b, qc, q, rows(p, 0)].reshape(n, 128) for qc in range(2))
                    parts.append(jnp.where(first, one, turn(two, n)))
            return rows_of(parts)

        def low_inv(b):
            acc = [inv[b, qc, :, rows(0, 1)] for qc in range(2)]
            for qc in range(2):
                for p in pairs[1:]:
                    acc[qc] = acc[qc] + inv[b, qc, :, rows(p, 1)]
            return turn(acc[0].reshape(2 * n, 128), -n) + acc[1].reshape(2 * n, 128)

        def temp_rows(temp):
            temp = temp.reshape(shape)
            return rows_of([jnp.where(pair[p], temp[q], 0.0).reshape(n, 128) for p in pairs for q in range(2)])

        def product(lefts, rights):
            if len(lefts) == 1:
                return hdot(lefts[0], rights[0])
            return hdot(jnp.concatenate(lefts, axis=1), twin(*rights))

        here = [(lanes((w, 2, 8, 128)) >> shift) == 2 * p for p in pairs]

        def wide_rows(temp):
            temp = [temp[:, 128 * qc:128 * qc + 128].reshape(shape) for qc in range(2)]
            return rows_of([both(lambda qc: jnp.where(here[p], temp[qc][q], 0.0).reshape(n, 128))
                            for p in pairs for q in range(2)])

        if w < 4:
            temps = [hdot(low_left(b), rows_of([both(lambda qc: inv[b, qc, q, rows(p, 0)].reshape(n, 128))
                                                for p in pairs for q in range(2)])) for b in group]
            for b, temp in zip(group, temps):
                prod = -hdot(low_inv(b), wide_rows(temp))
                for qc in range(2):
                    val = prod[:, 128 * qc:128 * qc + 128].reshape(shape)
                    for p in pairs:
                        inv[b, qc, :, rows(p, 1)] = jnp.where(even[p], val, inv[b, qc, :, rows(p, 1)])
            return
        two_blocks = (group[:2], group[2:])
        temps = [product([low_left(b) for b in bs], [up_inv(b) for b in bs]) for bs in two_blocks]
        for bs, temp in zip(two_blocks, temps):
            prod = -product([low_inv(b) for b in bs],
                            [temp_rows(temp[:, 128 * h:128 * h + 128]) for h in range(len(bs))])
            for h, b in enumerate(bs):
                piece = prod[:, 128 * h:128 * h + 128]
                for qc, val in enumerate((piece, turn(piece, -n))):
                    val = val.reshape(shape)
                    for p in pairs:
                        inv[b, qc, :, rows(p, 1)] = jnp.where(even[p], val, inv[b, qc, :, rows(p, 1)])

    zst = [None] * 6

    def z_diag(j):
        return both(lambda qc: inv[j, qc, c, :, x].reshape(64, 128))

    def emit(i, j, blk):
        out[64 * i:64 * i + 64, 128 * j:128 * j + 128] = blk

    def add_terms(j, ks, acc):
        for k in ks:
            prod = (hdot2 if k == 1 else hdot)(zst[k], low_block(k, j))
            for i in range(k, 6):
                part = prod[64 * (i - k):64 * (i - k) + 64]
                acc[i] = part if acc[i] is None else acc[i] + part

    def finish(j, acc):
        emit(j, j, inv[j, y, c, :, x].reshape(64, 128))
        if j == 5:
            zst[5] = z_diag(5)
            return
        res = -(hdot2 if j < 3 else hdot)(rows_of(acc[j + 1:]), inv_full(j))
        zst[j] = rows_of([z_diag(j), res])
        mine = jnp.where(y == 0, res[:, 0:128], res[:, 128:256])
        for i in range(j + 1, 6):
            emit(i, j, mine[64 * (i - j - 1):64 * (i - j)])

    def empty():
        return [None] * 6

    def finish_first(acc, rows):
        res = -hdot(rows_of([acc[i] for i in rows]), inv[0, y].reshape(256, 128))
        for n, i in enumerate(rows):
            emit(i, 0, res[64 * n:64 * n + 64])

    def c_block(k, j):
        return cbuf[c_at(k, j)].reshape(256, 128)

    def u_compute_top():
        prod = hdot(z_diag(3), jnp.concatenate([c_block(3, j) for j in range(3)], axis=1))
        for j in range(3):
            utop[y, j] = prod[:, 128 * j:128 * j + 128]

    def u_compute(j):
        both_rows = hdot(zst[3][64:192], c_block(3, j)) + hdot(zst[4], c_block(4, j))
        ubuf[j, y, 0:64] = both_rows[0:64]
        ubuf[j, y, 64:128] = both_rows[64:128] + hdot(zst[5], c_block(5, j))

    def u_rows(i, j, q):
        if i == 3:
            return utop[q, j]
        return ubuf[j, q, 64 * (i - 4):64 * (i - 3)]

    def u_add(j, acc, rows=(3, 4, 5)):
        for i in rows:
            part = both(lambda q: u_rows(i, j, q))
            acc[i] = part if acc[i] is None else acc[i] + part

    pack(DB)
    pl.semaphore_wait(barrier, 3)
    own(DB, "yx")
    ready(BO)
    own(BO, "sx")
    own(DB, "s")
    own(BO, "y")
    from_x(DB)
    pack(DA)
    own(DA, "yx")
    from_y(DB)
    c_own(3)
    from_x(BO)
    c_own(2)
    own(DA, "s")
    c_own(0)
    for i in range(5):
        out[64 * i:64 * i + 64, 128 * (i + 1):768] = jnp.zeros((64, 128 * (5 - i)), F32)
    from_diag(DB)
    wait_sib(DB)
    from_y(DA)
    from_x(DA)
    unpack(DB)
    base(3)
    c_own(1)
    double(DIAG[DB], 1)
    ready(A1)
    own(A1, "y")
    from_y(BO)
    c_relay(3)
    double(DIAG[DB], 2)
    own(A1, "x")
    from_diag(BO)
    ready(A2)
    own(A2, "xy")
    double(DIAG[DB], 4)
    c_wait(3)
    u_compute_top()
    u_send_to(3)
    from_diag(DA)
    wait_sib(BO)
    c_relay(2)
    finish(5, None)
    acc = empty()
    add_terms(4, (5,), acc)
    finish(4, acc)
    acc = empty()
    add_terms(3, (5, 4), acc)
    finish(3, acc)
    c_relay(1)
    from_y(A1)
    c_relay(0)
    wait_sib(DA)
    c_wait(2)
    unpack(DA)
    u_compute(2)
    base(0)
    u_send_to(2)
    own(A1, "s")
    own(A2, "s")
    from_y(A2)
    c_wait(1)
    u_compute(1)
    double(DIAG[DA], 1)
    u_send_to(1)
    c_wait(0)
    from_x(A2)
    from_x(A1)
    u_compute(0)
    double(DIAG[DA], 2)
    last_u = u_copy(0)
    sends.append(last_u)
    pl.when(c == 0)(last_u.start)
    from_diag(A1)
    double(DIAG[DA], 4)
    pl.when(c == 1)(last_u.start)
    emit(0, 0, inv[0, y, c, :, x].reshape(64, 128))
    from_diag(A2)
    u_wait(3)
    u_wait(2)
    acc = empty()
    u_add(2, acc)
    finish(2, acc)
    wait_sib(A1)
    acc = empty()
    add_terms(1, (2,), acc)
    first = empty()
    add_terms(0, (2,), first)
    u_wait(1)
    wait_sib(A2)
    u_add(1, acc)
    finish(1, acc)
    add_terms(0, (1,), first)
    u_add(0, first, (3,))
    finish_first(first, (1, 2, 3))
    u_wait(0)
    u_add(0, first, (4, 5))
    finish_first(first, (4, 5))

    for cp in sends:
        cp.wait_send()


def solution(mesh):
    spec = P(("batch", "row"), "col")

    def body(local_l):
        rows, cols = local_l.shape
        tiles = (2, 8, 2, 8, 128)
        return pl.pallas_call(
            kernel,
            out_shape=jax.ShapeDtypeStruct((rows, cols), F32),
            in_specs=[pl.BlockSpec(memory_space=pltpu.HBM)],
            out_specs=pl.BlockSpec(memory_space=pltpu.VMEM),
            scratch_shapes=[
                pltpu.VMEM((6, 8, 8, 128), F32),
                pltpu.VMEM((2, 2, 2, 2, 14, 8, 128), F32),
                pltpu.VMEM((6, 2, *tiles), F32),
                pltpu.VMEM((6, 2, *tiles), F32),
                pltpu.VMEM((9, *tiles), F32),
                pltpu.VMEM((2, 3, 64, 128), F32),
                pltpu.VMEM((3, 2, 128, 128), F32),
                pltpu.VMEM((6, 2, *tiles), F32),
                pltpu.SemaphoreType.DMA((21,)),
                pltpu.SemaphoreType.DMA((5, 7)),
                pltpu.SemaphoreType.DMA((5, 7)),
                pltpu.SemaphoreType.DMA((4, 3)),
                pltpu.SemaphoreType.DMA((4, 3)),
                pltpu.SemaphoreType.DMA((4,)),
                pltpu.SemaphoreType.DMA((4,)),
            ],
            compiler_params=pltpu.CompilerParams(
                collective_id=0, has_side_effects=True, vmem_limit_bytes=40 * 1024 * 1024),
        )(pltpu.with_memory_space_constraint(local_l.reshape(rows // 8, 8, cols), pltpu.HBM))

    return jax.shard_map(body, mesh=mesh, in_specs=(spec,), out_specs=spec, check_vma=False)
```

```python
import jax
import jax.numpy as jnp
from jax import lax
from jax.experimental import pallas as pl
from jax.experimental.pallas import tpu as pltpu
from jax.sharding import PartitionSpec as P

MESH = pl.DeviceIdType.MESH
F32 = jnp.float32
DB, DA, BO, A1, A2 = range(5)
DIAG = {DB: (5, 4, 3), DA: (2, 1, 0)}
OFF = {BO: ((5, 4), (4, 3), (5, 3)), A1: ((2, 1), (2, 0)), A2: ((1, 0),)}
OFF_AT = {blk: n for n, blk in enumerate(blk for grp in OFF.values() for blk in grp)}
LAST_X = (A1, A2,)


CGRP = [[(4, j), (5, j)] for j in range(3)] + [[(3, j) for j in range(3)]]


def c_at(k, j):
    return 6 + j if k == 3 else 2 * j + k - 4


def hdot(left, right):
    return jnp.dot(left, right, precision=lax.Precision.HIGHEST, preferred_element_type=F32)


def hdot2(left, right):
    half = left.shape[0] // 16 * 8
    return jnp.concatenate([hdot(left[:half], right), hdot(left[half:], right)], axis=0)


def kernel(inp, out, raw, dpk, dg, goff, cbuf, utop, ubuf, inv, loc_sem, g_send, g_recv, c_send, c_recv, u_send, u_recv):
    row = lax.axis_index("row")
    y = lax.axis_index("col")
    x = row // 2
    c = row % 2
    xo, yo, co = 1 - x, 1 - y, 1 - c
    sib = {"row": 2 * x + co}
    xnb = {"row": 2 * xo + c}
    ynb = {"col": yo}

    barrier = pltpu.get_barrier_semaphore()
    for nbr in (sib, xnb, ynb):
        pl.semaphore_signal(barrier, inc=1, device_id=nbr, device_id_type=MESH)

    def take(bi, bj, dst, sem):
        return pltpu.make_async_copy(inp.at[pl.ds(8 * bi, 8), :, pl.ds(128 * bj, 128)], dst, sem)

    local = {g: [take(b, b, raw.at[b], loc_sem.at[b]) for b in DIAG[g]] for g in DIAG}
    for g in OFF:
        local[g] = [take(bi, bj, goff.at[OFF_AT[bi, bj], y, c, :, x], loc_sem.at[6 + OFF_AT[bi, bj]]) for bi, bj in OFF[g]]
    local_c = [[take(bi, bj, cbuf.at[c_at(bi, bj), c, :, x], loc_sem.at[12 + c_at(bi, bj)]) for bi, bj in grp] for grp in CGRP]
    for grp in (local[DB], local[BO], local[DA], local_c[3], local_c[2], local[A1], local_c[1], local_c[0], local[A2]):
        for cp in grp:
            cp.start()

    sub = lax.broadcasted_iota(jnp.int32, (8, 128), 0)
    lane = lax.broadcasted_iota(jnp.int32, (8, 128), 1)

    def lanes(shape):
        return lax.broadcasted_iota(jnp.int32, shape, len(shape) - 1)

    def along(tile, idx):
        return jnp.take_along_axis(tile, idx, axis=1, mode="promise_in_bounds")

    def turn(tile, n):
        return along(tile, (lanes(tile.shape) + (128 - n)) & 127)

    def pack(g):
        for cp in local[g]:
            cp.wait()
        for i, b in enumerate(DIAG[g]):
            dpk[g, y, c, x, 4 * i] = raw[b, 7]
            for p in range(3):
                n = 112 - 16 * p
                dpk[g, y, c, x, 4 * i + 1 + p] = jnp.where(lane < n, raw[b, 6 - p], turn(raw[b, p], n))
        one, two, three = DIAG[g]
        dpk[g, y, c, x, 12] = jnp.where(lane < 64, raw[one, 3], turn(raw[two, 3], 64))
        dpk[g, y, c, x, 13] = raw[three, 3]

    def unpack(g):
        for i, b in enumerate(DIAG[g]):
            for qc in range(2):
                for lb in range(8):
                    at = 4 * i + (7 - lb if lb > 3 else 1 + lb)
                    n = 16 * (lb + 1)
                    if lb == 3:
                        at, n = 12 + i // 2, 64 * (i % 2)
                    tiles = dpk[g, qc, :, :, at]
                    if lb < 4 and n:
                        tiles = turn(tiles.reshape(32, 128), n).reshape(2, 2, 8, 128)
                    dg[b, qc, :, lb] = tiles

    def slot(g, sx, sc, sy):
        if g in DIAG:
            return dpk.at[g, sy, sc, sx]
        return goff.at[pl.ds(OFF_AT[OFF[g][0]], len(OFF[g])), sy, sc, :, sx]

    sends = []

    def copy(ref, send, recv, dev):
        return pltpu.make_async_remote_copy(ref, ref, send, recv, device_id=dev, device_id_type=MESH)

    def start(cp):
        cp.start()
        sends.append(cp)

    def gsend(g, k, ref, dev):
        start(copy(ref, g_send.at[g, k], g_recv.at[g, k], dev))

    def gwait(g, k, ref):
        copy(ref, g_send.at[g, k], g_recv.at[g, k], sib).wait_recv()

    def own(g, to):
        for k, dev in enumerate((xnb, ynb, sib)):
            if "xys"[k] in to:
                gsend(g, k, slot(g, x, c, y), dev)

    def ready(g):
        for cp in local[g]:
            cp.wait()

    def from_x(g):
        gwait(g, 0, slot(g, xo, c, y))
        if g not in LAST_X:
            gsend(g, 3, slot(g, xo, c, y), ynb)
        gsend(g, 4, slot(g, xo, c, y), sib)

    def from_y(g):
        gwait(g, 1, slot(g, x, c, yo))
        if g in LAST_X:
            gsend(g, 3, slot(g, x, c, yo), xnb)
        gsend(g, 5, slot(g, x, c, yo), sib)

    def from_diag(g):
        gwait(g, 3, slot(g, xo, c, yo))
        gsend(g, 6, slot(g, xo, c, yo), sib)

    def wait_sib(g):
        for k, ref in ((2, slot(g, x, co, y)), (4, slot(g, xo, co, y)), (5, slot(g, x, co, yo)), (6, slot(g, xo, co, yo))):
            gwait(g, k, ref)

    def c_slot(g, sx, sc):
        return cbuf.at[pl.ds(c_at(*CGRP[g][0]), len(CGRP[g])), sc, :, sx]

    def c_own(g):
        for cp in local_c[g]:
            cp.wait()
        for k, dev in enumerate((xnb, sib)):
            start(copy(c_slot(g, x, c), c_send.at[g, k], c_recv.at[g, k], dev))

    def c_relay(g):
        copy(c_slot(g, xo, c), c_send.at[g, 0], c_recv.at[g, 0], sib).wait_recv()
        start(copy(c_slot(g, xo, c), c_send.at[g, 2], c_recv.at[g, 2], sib))

    def c_wait(g):
        copy(c_slot(g, x, co), c_send.at[g, 1], c_recv.at[g, 1], sib).wait_recv()
        copy(c_slot(g, xo, co), c_send.at[g, 2], c_recv.at[g, 2], sib).wait_recv()

    def u_slot(g, sy):
        return utop.at[sy] if g == 3 else ubuf.at[g, sy]

    def u_copy(g):
        return copy(u_slot(g, y), u_send.at[g], u_recv.at[g], ynb)

    def u_send_to(g):
        start(u_copy(g))

    def u_wait(g):
        copy(u_slot(g, yo), u_send.at[g], u_recv.at[g], ynb).wait_recv()

    def base(at):
        sub3 = lax.broadcasted_iota(jnp.int32, (3, 8, 128), 1)
        lane3 = lanes((3, 8, 128))
        seg3 = lane3 >> 4
        seg24 = lanes((24, 128)) & 112
        here = [(sub3 == (lane3 & 7)) & (((lane3 >> 3) & 1) == xr) for xr in range(2)]
        segs = [seg3 == lb for lb in range(8)]
        low = [[None, None] for _ in range(4)]
        for nb in range(4):
            xr, qr = nb // 2, nb % 2
            for qc in range(2):
                acc = dg[at:at + 3, qc, qr, 0, xr]
                for lb in range(1, 8):
                    acc = jnp.where(segs[lb], dg[at:at + 3, qc, qr, lb, xr], acc)
                low[nb][qc] = acc
        rec = []
        for qc in range(2):
            dsum = jnp.where(here[0], low[qc][qc], 0.0) + jnp.where(here[1], low[2 + qc][qc], 0.0)
            rec.append(1.0 / jnp.sum(dsum, axis=1, keepdims=True))
        rhs = []
        for nb in range(4):
            for qc in range(2):
                low[nb][qc] = (low[nb][qc] * rec[qc]).reshape(24, 128)
            rhs.append([jnp.where(here[nb // 2], 1.0, 0.0) if nb % 2 == qc else jnp.zeros((3, 8, 128), F32)
                        for qc in range(2)])
        below = [sub3 > ek for ek in range(7)]
        for k in range(32):
            nk, ek = k // 8, k % 8
            xk, qk = nk // 2, nk % 2
            idx = seg24 + (8 * xk + ek)
            pivot = [rhs[nk][qc][:, ek:ek + 1, :] for qc in range(2)]
            for nb in range(nk, 4):
                if nb == nk and ek == 7:
                    continue
                col = along(low[nb][qk], idx).reshape(3, 8, 128)
                if nb == nk:
                    col = jnp.where(below[ek], col, 0.0)
                for qc in range(2):
                    rhs[nb][qc] = rhs[nb][qc] - col * pivot[qc]
        for nb in range(4):
            xr, qr = nb // 2, nb % 2
            idx = (seg3 * 16 + 8 * xr + sub3).reshape(24, 128)
            scale = along(jnp.broadcast_to(rec[qr], (3, 8, 128)).reshape(24, 128), idx).reshape(3, 8, 128)
            for qc in range(2):
                val = rhs[nb][qc] * scale
                for lb in range(8):
                    inv[at:at + 3, qc, qr, lb, xr] = jnp.where(segs[lb], val, 0.0)

    def both(ref_of):
        return jnp.concatenate([ref_of(0), ref_of(1)], axis=1)

    def inv_full(b):
        return both(lambda qc: inv[b, qc].reshape(256, 128))

    def low_block(k, j):
        return both(lambda qc: goff[OFF_AT[k, j], qc].reshape(256, 128))

    def rows_of(tiles):
        return jnp.concatenate(tiles, axis=0)

    def double(group, w):
        pairs = range(4 // w)
        n = 16 * w
        shift = {1: 4, 2: 5, 4: 6}[w]
        shape = (2, w, 2, 8, 128)
        part = lanes(shape) >> shift
        even = [part == 2 * p for p in pairs]
        pair = [(lanes((w, 2, 8, 128)) >> (shift + 1)) == p for p in pairs]
        zero = jnp.zeros(shape, F32)
        first = (lanes((n, 128)) & n) == 0
        hole = jnp.zeros((128, 128), F32)

        def rows(p, odd):
            return pl.ds((2 * p + odd) * w, w)

        def twin(one, two):
            return rows_of([both(lambda h: (one, hole)[h]), both(lambda h: (hole, two)[h])])

        def low_left(b):
            acc = [zero, zero]
            for qc in range(2):
                for p in pairs:
                    acc[qc] = jnp.where(even[p], dg[b, qc, :, rows(p, 1)], acc[qc])
            return acc[0].reshape(2 * n, 128) + turn(acc[1].reshape(2 * n, 128), n)

        def up_inv(b):
            parts = []
            for p in pairs:
                for q in range(2):
                    one, two = (inv[b, qc, q, rows(p, 0)].reshape(n, 128) for qc in range(2))
                    parts.append(jnp.where(first, one, turn(two, n)))
            return rows_of(parts)

        def low_inv(b):
            acc = [inv[b, qc, :, rows(0, 1)] for qc in range(2)]
            for qc in range(2):
                for p in pairs[1:]:
                    acc[qc] = acc[qc] + inv[b, qc, :, rows(p, 1)]
            return turn(acc[0].reshape(2 * n, 128), -n) + acc[1].reshape(2 * n, 128)

        def temp_rows(temp):
            temp = temp.reshape(shape)
            return rows_of([jnp.where(pair[p], temp[q], 0.0).reshape(n, 128) for p in pairs for q in range(2)])

        def product(lefts, rights):
            if len(lefts) == 1:
                return hdot(lefts[0], rights[0])
            return hdot(jnp.concatenate(lefts, axis=1), twin(*rights))

        here = [(lanes((w, 2, 8, 128)) >> shift) == 2 * p for p in pairs]

        def wide_rows(temp):
            temp = [temp[:, 128 * qc:128 * qc + 128].reshape(shape) for qc in range(2)]
            return rows_of([both(lambda qc: jnp.where(here[p], temp[qc][q], 0.0).reshape(n, 128))
                            for p in pairs for q in range(2)])

        if w < 4:
            temps = [hdot(low_left(b), rows_of([both(lambda qc: inv[b, qc, q, rows(p, 0)].reshape(n, 128))
                                                for p in pairs for q in range(2)])) for b in group]
            for b, temp in zip(group, temps):
                prod = -hdot(low_inv(b), wide_rows(temp))
                for qc in range(2):
                    val = prod[:, 128 * qc:128 * qc + 128].reshape(shape)
                    for p in pairs:
                        inv[b, qc, :, rows(p, 1)] = jnp.where(even[p], val, inv[b, qc, :, rows(p, 1)])
            return
        two_blocks = (group[:2], group[2:])
        temps = [product([low_left(b) for b in bs], [up_inv(b) for b in bs]) for bs in two_blocks]
        for bs, temp in zip(two_blocks, temps):
            prod = -product([low_inv(b) for b in bs],
                            [temp_rows(temp[:, 128 * h:128 * h + 128]) for h in range(len(bs))])
            for h, b in enumerate(bs):
                piece = prod[:, 128 * h:128 * h + 128]
                for qc, val in enumerate((piece, turn(piece, -n))):
                    val = val.reshape(shape)
                    for p in pairs:
                        inv[b, qc, :, rows(p, 1)] = jnp.where(even[p], val, inv[b, qc, :, rows(p, 1)])

    zst = [None] * 6

    def z_diag(j):
        return both(lambda qc: inv[j, qc, c, :, x].reshape(64, 128))

    def emit(i, j, blk):
        out[64 * i:64 * i + 64, 128 * j:128 * j + 128] = blk

    def add_terms(j, ks, acc):
        for k in ks:
            prod = (hdot2 if k == 1 else hdot)(zst[k], low_block(k, j))
            for i in range(k, 6):
                part = prod[64 * (i - k):64 * (i - k) + 64]
                acc[i] = part if acc[i] is None else acc[i] + part

    def finish(j, acc):
        emit(j, j, inv[j, y, c, :, x].reshape(64, 128))
        if j == 5:
            zst[5] = z_diag(5)
            return
        res = -(hdot2 if j < 3 else hdot)(rows_of(acc[j + 1:]), inv_full(j))
        zst[j] = rows_of([z_diag(j), res])
        mine = jnp.where(y == 0, res[:, 0:128], res[:, 128:256])
        for i in range(j + 1, 6):
            emit(i, j, mine[64 * (i - j - 1):64 * (i - j)])

    def empty():
        return [None] * 6

    def finish_first(acc, rows):
        res = -hdot(rows_of([acc[i] for i in rows]), inv[0, y].reshape(256, 128))
        for n, i in enumerate(rows):
            emit(i, 0, res[64 * n:64 * n + 64])

    def c_block(k, j):
        return cbuf[c_at(k, j)].reshape(256, 128)

    def u_compute_top():
        prod = hdot(z_diag(3), jnp.concatenate([c_block(3, j) for j in range(3)], axis=1))
        for j in range(3):
            utop[y, j] = prod[:, 128 * j:128 * j + 128]

    def u_compute(j):
        both_rows = hdot(zst[3][64:192], c_block(3, j)) + hdot(zst[4], c_block(4, j))
        ubuf[j, y, 0:64] = both_rows[0:64]
        ubuf[j, y, 64:128] = both_rows[64:128] + hdot(zst[5], c_block(5, j))

    def u_rows(i, j, q):
        if i == 3:
            return utop[q, j]
        return ubuf[j, q, 64 * (i - 4):64 * (i - 3)]

    def u_add(j, acc, rows=(3, 4, 5)):
        for i in rows:
            part = both(lambda q: u_rows(i, j, q))
            acc[i] = part if acc[i] is None else acc[i] + part

    pack(DB)
    pl.semaphore_wait(barrier, 3)
    own(DB, "xy")
    ready(BO)
    own(BO, "xy")
    from_x(DB)
    pack(DA)
    own(DA, "x")
    from_y(DB)
    own(DA, "s")
    c_own(3)
    own(DB, "s")
    c_own(2)
    own(DA, "y")
    from_x(BO)
    c_own(1)
    from_diag(DB)
    from_x(DA)
    own(BO, "s")
    ready(A1)
    own(A1, "y")
    c_own(0)
    for i in range(5):
        out[64 * i:64 * i + 64, 128 * (i + 1):768] = jnp.zeros((64, 128 * (5 - i)), F32)
    from_y(BO)
    from_y(DA)
    ready(A2)
    own(A2, "yx")
    wait_sib(DB)
    unpack(DB)
    base(3)
    double(DIAG[DB], 1)
    c_relay(3)
    double(DIAG[DB], 2)
    from_diag(BO)
    double(DIAG[DB], 4)
    own(A1, "s")
    c_wait(3)
    u_compute_top()
    u_send_to(3)
    c_relay(2)
    from_diag(DA)
    own(A1, "x")
    c_relay(1)
    wait_sib(BO)
    finish(5, None)
    acc = empty()
    add_terms(4, (5,), acc)
    finish(4, acc)
    acc = empty()
    add_terms(3, (5, 4), acc)
    finish(3, acc)
    from_y(A1)
    wait_sib(DA)
    c_relay(0)
    c_wait(2)
    unpack(DA)
    u_compute(2)
    base(0)
    u_send_to(2)
    from_x(A2)
    c_wait(1)
    own(A2, "s")
    from_y(A2)
    u_compute(1)
    double(DIAG[DA], 1)
    u_send_to(1)
    c_wait(0)
    u_compute(0)
    double(DIAG[DA], 2)
    last_u = u_copy(0)
    sends.append(last_u)
    pl.when(c == 0)(last_u.start)
    from_x(A1)
    from_diag(A1)
    double(DIAG[DA], 4)
    pl.when(c == 1)(last_u.start)
    emit(0, 0, inv[0, y, c, :, x].reshape(64, 128))
    from_diag(A2)
    u_wait(3)
    u_wait(2)
    acc = empty()
    u_add(2, acc)
    finish(2, acc)
    wait_sib(A1)
    acc = empty()
    add_terms(1, (2,), acc)
    first = empty()
    add_terms(0, (2,), first)
    u_wait(1)
    wait_sib(A2)
    u_add(1, acc)
    finish(1, acc)
    add_terms(0, (1,), first)
    u_add(0, first, (3,))
    finish_first(first, (1, 2, 3))
    u_wait(0)
    u_add(0, first, (4, 5))
    finish_first(first, (4, 5))

    for cp in sends:
        cp.wait_send()


def solution(mesh):
    spec = P(("batch", "row"), "col")

    def body(local_l):
        rows, cols = local_l.shape
        tiles = (2, 8, 2, 8, 128)
        return pl.pallas_call(
            kernel,
            out_shape=jax.ShapeDtypeStruct((rows, cols), F32),
            in_specs=[pl.BlockSpec(memory_space=pltpu.HBM)],
            out_specs=pl.BlockSpec(memory_space=pltpu.VMEM),
            scratch_shapes=[
                pltpu.VMEM((6, 8, 8, 128), F32),
                pltpu.VMEM((2, 2, 2, 2, 14, 8, 128), F32),
                pltpu.VMEM((6, 2, *tiles), F32),
                pltpu.VMEM((6, 2, *tiles), F32),
                pltpu.VMEM((9, *tiles), F32),
                pltpu.VMEM((2, 3, 64, 128), F32),
                pltpu.VMEM((3, 2, 128, 128), F32),
                pltpu.VMEM((6, 2, *tiles), F32),
                pltpu.SemaphoreType.DMA((21,)),
                pltpu.SemaphoreType.DMA((5, 7)),
                pltpu.SemaphoreType.DMA((5, 7)),
                pltpu.SemaphoreType.DMA((4, 3)),
                pltpu.SemaphoreType.DMA((4, 3)),
                pltpu.SemaphoreType.DMA((4,)),
                pltpu.SemaphoreType.DMA((4,)),
            ],
            compiler_params=pltpu.CompilerParams(
                collective_id=0, has_side_effects=True, vmem_limit_bytes=40 * 1024 * 1024),
        )(pltpu.with_memory_space_constraint(local_l.reshape(rows // 8, 8, cols), pltpu.HBM))

    return jax.shard_map(body, mesh=mesh, in_specs=(spec,), out_specs=spec, check_vma=False)
```

```python
import jax
import jax.numpy as jnp
from jax import lax
from jax.experimental import pallas as pl
from jax.experimental.pallas import tpu as pltpu
from jax.sharding import PartitionSpec as P

MESH = pl.DeviceIdType.MESH
F32 = jnp.float32
DB, DA, BO, A1, A2 = range(5)
DIAG = {DB: (5, 4, 3), DA: (2, 1, 0)}
OFF = {BO: ((5, 4), (4, 3), (5, 3)), A1: ((2, 1), (2, 0)), A2: ((1, 0),)}
OFF_AT = {blk: n for n, blk in enumerate(blk for grp in OFF.values() for blk in grp)}
LAST_X = (A1, A2,)


CGRP = [[(4, j), (5, j)] for j in range(3)] + [[(3, j) for j in range(3)]]


def c_at(k, j):
    return 6 + j if k == 3 else 2 * j + k - 4


def hdot(left, right):
    return jnp.dot(left, right, precision=lax.Precision.HIGHEST, preferred_element_type=F32)


def hdot2(left, right):
    half = left.shape[0] // 16 * 8
    return jnp.concatenate([hdot(left[:half], right), hdot(left[half:], right)], axis=0)


def kernel(inp, out, raw, dpk, dg, goff, cbuf, utop, ubuf, inv, loc_sem, g_send, g_recv, c_send, c_recv, u_send, u_recv):
    row = lax.axis_index("row")
    y = lax.axis_index("col")
    x = row // 2
    c = row % 2
    xo, yo, co = 1 - x, 1 - y, 1 - c
    sib = {"row": 2 * x + co}
    xnb = {"row": 2 * xo + c}
    ynb = {"col": yo}

    barrier = pltpu.get_barrier_semaphore()
    for nbr in (sib, xnb, ynb):
        pl.semaphore_signal(barrier, inc=1, device_id=nbr, device_id_type=MESH)

    def take(bi, bj, dst, sem):
        return pltpu.make_async_copy(inp.at[pl.ds(8 * bi, 8), :, pl.ds(128 * bj, 128)], dst, sem)

    local = {g: [take(b, b, raw.at[b], loc_sem.at[b]) for b in DIAG[g]] for g in DIAG}
    for g in OFF:
        local[g] = [take(bi, bj, goff.at[OFF_AT[bi, bj], y, c, :, x], loc_sem.at[6 + OFF_AT[bi, bj]]) for bi, bj in OFF[g]]
    local_c = [[take(bi, bj, cbuf.at[c_at(bi, bj), c, :, x], loc_sem.at[12 + c_at(bi, bj)]) for bi, bj in grp] for grp in CGRP]
    for grp in (local[DB], local[BO], local[DA], local_c[3], local_c[2], local[A1], local_c[1], local_c[0], local[A2]):
        for cp in grp:
            cp.start()

    sub = lax.broadcasted_iota(jnp.int32, (8, 128), 0)
    lane = lax.broadcasted_iota(jnp.int32, (8, 128), 1)

    def lanes(shape):
        return lax.broadcasted_iota(jnp.int32, shape, len(shape) - 1)

    def along(tile, idx):
        return jnp.take_along_axis(tile, idx, axis=1, mode="promise_in_bounds")

    def turn(tile, n):
        return along(tile, (lanes(tile.shape) + (128 - n)) & 127)

    def pack(g):
        for cp in local[g]:
            cp.wait()
        for i, b in enumerate(DIAG[g]):
            dpk[g, y, c, x, 4 * i] = raw[b, 7]
            for p in range(3):
                n = 112 - 16 * p
                dpk[g, y, c, x, 4 * i + 1 + p] = jnp.where(lane < n, raw[b, 6 - p], turn(raw[b, p], n))
        one, two, three = DIAG[g]
        dpk[g, y, c, x, 12] = jnp.where(lane < 64, raw[one, 3], turn(raw[two, 3], 64))
        dpk[g, y, c, x, 13] = raw[three, 3]

    def unpack(g):
        for i, b in enumerate(DIAG[g]):
            for qc in range(2):
                for lb in range(8):
                    at = 4 * i + (7 - lb if lb > 3 else 1 + lb)
                    n = 16 * (lb + 1)
                    if lb == 3:
                        at, n = 12 + i // 2, 64 * (i % 2)
                    tiles = dpk[g, qc, :, :, at]
                    if lb < 4 and n:
                        tiles = turn(tiles.reshape(32, 128), n).reshape(2, 2, 8, 128)
                    dg[b, qc, :, lb] = tiles

    def slot(g, sx, sc, sy):
        if g in DIAG:
            return dpk.at[g, sy, sc, sx]
        return goff.at[pl.ds(OFF_AT[OFF[g][0]], len(OFF[g])), sy, sc, :, sx]

    sends = []

    def copy(ref, send, recv, dev):
        return pltpu.make_async_remote_copy(ref, ref, send, recv, device_id=dev, device_id_type=MESH)

    def start(cp):
        cp.start()
        sends.append(cp)

    def gsend(g, k, ref, dev):
        start(copy(ref, g_send.at[g, k], g_recv.at[g, k], dev))

    def gwait(g, k, ref):
        copy(ref, g_send.at[g, k], g_recv.at[g, k], sib).wait_recv()

    def own(g, to):
        for k, dev in enumerate((xnb, ynb, sib)):
            if "xys"[k] in to:
                gsend(g, k, slot(g, x, c, y), dev)

    def ready(g):
        for cp in local[g]:
            cp.wait()

    def from_x(g):
        gwait(g, 0, slot(g, xo, c, y))
        if g not in LAST_X:
            gsend(g, 3, slot(g, xo, c, y), ynb)
        gsend(g, 4, slot(g, xo, c, y), sib)

    def from_y(g):
        gwait(g, 1, slot(g, x, c, yo))
        if g in LAST_X:
            gsend(g, 3, slot(g, x, c, yo), xnb)
        gsend(g, 5, slot(g, x, c, yo), sib)

    def from_diag(g):
        gwait(g, 3, slot(g, xo, c, yo))
        gsend(g, 6, slot(g, xo, c, yo), sib)

    def wait_sib(g):
        for k, ref in ((2, slot(g, x, co, y)), (4, slot(g, xo, co, y)), (5, slot(g, x, co, yo)), (6, slot(g, xo, co, yo))):
            gwait(g, k, ref)

    def c_slot(g, sx, sc):
        return cbuf.at[pl.ds(c_at(*CGRP[g][0]), len(CGRP[g])), sc, :, sx]

    def c_own(g):
        for cp in local_c[g]:
            cp.wait()
        for k, dev in enumerate((xnb, sib)):
            start(copy(c_slot(g, x, c), c_send.at[g, k], c_recv.at[g, k], dev))

    def c_relay(g):
        copy(c_slot(g, xo, c), c_send.at[g, 0], c_recv.at[g, 0], sib).wait_recv()
        start(copy(c_slot(g, xo, c), c_send.at[g, 2], c_recv.at[g, 2], sib))

    def c_wait(g):
        copy(c_slot(g, x, co), c_send.at[g, 1], c_recv.at[g, 1], sib).wait_recv()
        copy(c_slot(g, xo, co), c_send.at[g, 2], c_recv.at[g, 2], sib).wait_recv()

    def u_slot(g, sy):
        return utop.at[sy] if g == 3 else ubuf.at[g, sy]

    def u_copy(g):
        return copy(u_slot(g, y), u_send.at[g], u_recv.at[g], ynb)

    def u_send_to(g):
        start(u_copy(g))

    def u_wait(g):
        copy(u_slot(g, yo), u_send.at[g], u_recv.at[g], ynb).wait_recv()

    def base(at):
        sub3 = lax.broadcasted_iota(jnp.int32, (3, 8, 128), 1)
        lane3 = lanes((3, 8, 128))
        seg3 = lane3 >> 4
        seg24 = lanes((24, 128)) & 112
        here = [(sub3 == (lane3 & 7)) & (((lane3 >> 3) & 1) == xr) for xr in range(2)]
        segs = [seg3 == lb for lb in range(8)]
        low = [[None, None] for _ in range(4)]
        for nb in range(4):
            xr, qr = nb // 2, nb % 2
            for qc in range(2):
                acc = dg[at:at + 3, qc, qr, 0, xr]
                for lb in range(1, 8):
                    acc = jnp.where(segs[lb], dg[at:at + 3, qc, qr, lb, xr], acc)
                low[nb][qc] = acc
        rec = []
        for qc in range(2):
            dsum = jnp.where(here[0], low[qc][qc], 0.0) + jnp.where(here[1], low[2 + qc][qc], 0.0)
            rec.append(1.0 / jnp.sum(dsum, axis=1, keepdims=True))
        rhs = []
        for nb in range(4):
            for qc in range(2):
                low[nb][qc] = (low[nb][qc] * rec[qc]).reshape(24, 128)
            rhs.append([jnp.where(here[nb // 2], 1.0, 0.0) if nb % 2 == qc else jnp.zeros((3, 8, 128), F32)
                        for qc in range(2)])
        below = [sub3 > ek for ek in range(7)]
        for k in range(32):
            nk, ek = k // 8, k % 8
            xk, qk = nk // 2, nk % 2
            idx = seg24 + (8 * xk + ek)
            pivot = [rhs[nk][qc][:, ek:ek + 1, :] for qc in range(2)]
            for nb in range(nk, 4):
                if nb == nk and ek == 7:
                    continue
                col = along(low[nb][qk], idx).reshape(3, 8, 128)
                if nb == nk:
                    col = jnp.where(below[ek], col, 0.0)
                for qc in range(2):
                    rhs[nb][qc] = rhs[nb][qc] - col * pivot[qc]
        for nb in range(4):
            xr, qr = nb // 2, nb % 2
            idx = (seg3 * 16 + 8 * xr + sub3).reshape(24, 128)
            scale = along(jnp.broadcast_to(rec[qr], (3, 8, 128)).reshape(24, 128), idx).reshape(3, 8, 128)
            for qc in range(2):
                val = rhs[nb][qc] * scale
                for lb in range(8):
                    inv[at:at + 3, qc, qr, lb, xr] = jnp.where(segs[lb], val, 0.0)

    def both(ref_of):
        return jnp.concatenate([ref_of(0), ref_of(1)], axis=1)

    def inv_full(b):
        return both(lambda qc: inv[b, qc].reshape(256, 128))

    def low_block(k, j):
        return both(lambda qc: goff[OFF_AT[k, j], qc].reshape(256, 128))

    def rows_of(tiles):
        return jnp.concatenate(tiles, axis=0)

    def double(group, w):
        pairs = range(4 // w)
        n = 16 * w
        shift = {1: 4, 2: 5, 4: 6}[w]
        shape = (2, w, 2, 8, 128)
        part = lanes(shape) >> shift
        even = [part == 2 * p for p in pairs]
        pair = [(lanes((w, 2, 8, 128)) >> (shift + 1)) == p for p in pairs]
        zero = jnp.zeros(shape, F32)
        first = (lanes((n, 128)) & n) == 0
        hole = jnp.zeros((128, 128), F32)

        def rows(p, odd):
            return pl.ds((2 * p + odd) * w, w)

        def twin(one, two):
            return rows_of([both(lambda h: (one, hole)[h]), both(lambda h: (hole, two)[h])])

        def low_left(b):
            acc = [zero, zero]
            for qc in range(2):
                for p in pairs:
                    acc[qc] = jnp.where(even[p], dg[b, qc, :, rows(p, 1)], acc[qc])
            return acc[0].reshape(2 * n, 128) + turn(acc[1].reshape(2 * n, 128), n)

        def up_inv(b):
            parts = []
            for p in pairs:
                for q in range(2):
                    one, two = (inv[b, qc, q, rows(p, 0)].reshape(n, 128) for qc in range(2))
                    parts.append(jnp.where(first, one, turn(two, n)))
            return rows_of(parts)

        def low_inv(b):
            acc = [inv[b, qc, :, rows(0, 1)] for qc in range(2)]
            for qc in range(2):
                for p in pairs[1:]:
                    acc[qc] = acc[qc] + inv[b, qc, :, rows(p, 1)]
            return turn(acc[0].reshape(2 * n, 128), -n) + acc[1].reshape(2 * n, 128)

        def temp_rows(temp):
            temp = temp.reshape(shape)
            return rows_of([jnp.where(pair[p], temp[q], 0.0).reshape(n, 128) for p in pairs for q in range(2)])

        def product(lefts, rights):
            if len(lefts) == 1:
                return hdot(lefts[0], rights[0])
            return hdot(jnp.concatenate(lefts, axis=1), twin(*rights))

        here = [(lanes((w, 2, 8, 128)) >> shift) == 2 * p for p in pairs]

        def wide_rows(temp):
            temp = [temp[:, 128 * qc:128 * qc + 128].reshape(shape) for qc in range(2)]
            return rows_of([both(lambda qc: jnp.where(here[p], temp[qc][q], 0.0).reshape(n, 128))
                            for p in pairs for q in range(2)])

        if w < 4:
            temps = [hdot(low_left(b), rows_of([both(lambda qc: inv[b, qc, q, rows(p, 0)].reshape(n, 128))
                                                for p in pairs for q in range(2)])) for b in group]
            for b, temp in zip(group, temps):
                prod = -hdot(low_inv(b), wide_rows(temp))
                for qc in range(2):
                    val = prod[:, 128 * qc:128 * qc + 128].reshape(shape)
                    for p in pairs:
                        inv[b, qc, :, rows(p, 1)] = jnp.where(even[p], val, inv[b, qc, :, rows(p, 1)])
            return
        two_blocks = (group[:2], group[2:])
        temps = [product([low_left(b) for b in bs], [up_inv(b) for b in bs]) for bs in two_blocks]
        for bs, temp in zip(two_blocks, temps):
            prod = -product([low_inv(b) for b in bs],
                            [temp_rows(temp[:, 128 * h:128 * h + 128]) for h in range(len(bs))])
            for h, b in enumerate(bs):
                piece = prod[:, 128 * h:128 * h + 128]
                for qc, val in enumerate((piece, turn(piece, -n))):
                    val = val.reshape(shape)
                    for p in pairs:
                        inv[b, qc, :, rows(p, 1)] = jnp.where(even[p], val, inv[b, qc, :, rows(p, 1)])

    zst = [None] * 6

    def z_diag(j):
        return both(lambda qc: inv[j, qc, c, :, x].reshape(64, 128))

    def emit(i, j, blk):
        out[64 * i:64 * i + 64, 128 * j:128 * j + 128] = blk

    def add_terms(j, ks, acc):
        for k in ks:
            prod = (hdot2 if k == 1 else hdot)(zst[k], low_block(k, j))
            for i in range(k, 6):
                part = prod[64 * (i - k):64 * (i - k) + 64]
                acc[i] = part if acc[i] is None else acc[i] + part

    def finish(j, acc):
        emit(j, j, inv[j, y, c, :, x].reshape(64, 128))
        if j == 5:
            zst[5] = z_diag(5)
            return
        res = -(hdot2 if j < 3 else hdot)(rows_of(acc[j + 1:]), inv_full(j))
        zst[j] = rows_of([z_diag(j), res])
        mine = jnp.where(y == 0, res[:, 0:128], res[:, 128:256])
        for i in range(j + 1, 6):
            emit(i, j, mine[64 * (i - j - 1):64 * (i - j)])

    def empty():
        return [None] * 6

    def finish_first(acc, rows):
        res = -hdot2(rows_of([acc[i] for i in rows]), inv[0, y].reshape(256, 128))
        for n, i in enumerate(rows):
            emit(i, 0, res[64 * n:64 * n + 64])

    def c_block(k, j):
        return cbuf[c_at(k, j)].reshape(256, 128)

    def u_compute_top():
        prod = hdot(z_diag(3), jnp.concatenate([c_block(3, j) for j in range(3)], axis=1))
        for j in range(3):
            utop[y, j] = prod[:, 128 * j:128 * j + 128]

    def u_compute(j):
        both_rows = hdot(zst[3][64:192], c_block(3, j)) + hdot(zst[4], c_block(4, j))
        ubuf[j, y, 0:64] = both_rows[0:64]
        ubuf[j, y, 64:128] = both_rows[64:128] + hdot(zst[5], c_block(5, j))

    def u_rows(i, j, q):
        if i == 3:
            return utop[q, j]
        return ubuf[j, q, 64 * (i - 4):64 * (i - 3)]

    def u_add(j, acc, rows=(3, 4, 5)):
        for i in rows:
            part = both(lambda q: u_rows(i, j, q))
            acc[i] = part if acc[i] is None else acc[i] + part

    pack(DB)
    pl.semaphore_wait(barrier, 3)
    own(DB, "yx")
    ready(BO)
    own(BO, "sx")
    own(DB, "s")
    own(BO, "y")
    from_x(DB)
    pack(DA)
    own(DA, "yx")
    from_y(DB)
    c_own(3)
    from_x(BO)
    c_own(2)
    own(DA, "s")
    c_own(0)
    for i in range(5):
        out[64 * i:64 * i + 64, 128 * (i + 1):768] = jnp.zeros((64, 128 * (5 - i)), F32)
    from_diag(DB)
    wait_sib(DB)
    from_y(DA)
    from_x(DA)
    unpack(DB)
    base(3)
    c_own(1)
    double(DIAG[DB], 1)
    ready(A1)
    own(A1, "y")
    from_y(BO)
    c_relay(3)
    double(DIAG[DB], 2)
    own(A1, "x")
    from_diag(BO)
    ready(A2)
    own(A2, "xy")
    double(DIAG[DB], 4)
    c_wait(3)
    u_compute_top()
    u_send_to(3)
    from_diag(DA)
    wait_sib(BO)
    c_relay(2)
    finish(5, None)
    acc = empty()
    add_terms(4, (5,), acc)
    finish(4, acc)
    acc = empty()
    add_terms(3, (5, 4), acc)
    finish(3, acc)
    c_relay(1)
    from_y(A1)
    c_relay(0)
    wait_sib(DA)
    c_wait(2)
    unpack(DA)
    u_compute(2)
    base(0)
    u_send_to(2)
    own(A1, "s")
    own(A2, "s")
    from_y(A2)
    c_wait(1)
    u_compute(1)
    double(DIAG[DA], 1)
    u_send_to(1)
    c_wait(0)
    from_x(A2)
    from_x(A1)
    u_compute(0)
    double(DIAG[DA], 2)
    last_u = u_copy(0)
    sends.append(last_u)
    pl.when(c == 0)(last_u.start)
    from_diag(A1)
    double(DIAG[DA], 4)
    pl.when(c == 1)(last_u.start)
    emit(0, 0, inv[0, y, c, :, x].reshape(64, 128))
    from_diag(A2)
    u_wait(3)
    u_wait(2)
    acc = empty()
    u_add(2, acc)
    finish(2, acc)
    wait_sib(A1)
    acc = empty()
    add_terms(1, (2,), acc)
    first = empty()
    add_terms(0, (2,), first)
    u_wait(1)
    wait_sib(A2)
    u_add(1, acc)
    finish(1, acc)
    add_terms(0, (1,), first)
    u_add(0, first, (3,))
    finish_first(first, (1, 2, 3))
    u_wait(0)
    u_add(0, first, (4, 5))
    finish_first(first, (4, 5))

    for cp in sends:
        cp.wait_send()


def solution(mesh):
    spec = P(("batch", "row"), "col")

    def body(local_l):
        rows, cols = local_l.shape
        tiles = (2, 8, 2, 8, 128)
        return pl.pallas_call(
            kernel,
            out_shape=jax.ShapeDtypeStruct((rows, cols), F32),
            in_specs=[pl.BlockSpec(memory_space=pltpu.HBM)],
            out_specs=pl.BlockSpec(memory_space=pltpu.VMEM),
            scratch_shapes=[
                pltpu.VMEM((6, 8, 8, 128), F32),
                pltpu.VMEM((2, 2, 2, 2, 14, 8, 128), F32),
                pltpu.VMEM((6, 2, *tiles), F32),
                pltpu.VMEM((6, 2, *tiles), F32),
                pltpu.VMEM((9, *tiles), F32),
                pltpu.VMEM((2, 3, 64, 128), F32),
                pltpu.VMEM((3, 2, 128, 128), F32),
                pltpu.VMEM((6, 2, *tiles), F32),
                pltpu.SemaphoreType.DMA((21,)),
                pltpu.SemaphoreType.DMA((5, 7)),
                pltpu.SemaphoreType.DMA((5, 7)),
                pltpu.SemaphoreType.DMA((4, 3)),
                pltpu.SemaphoreType.DMA((4, 3)),
                pltpu.SemaphoreType.DMA((4,)),
                pltpu.SemaphoreType.DMA((4,)),
            ],
            compiler_params=pltpu.CompilerParams(
                collective_id=0, has_side_effects=True, vmem_limit_bytes=40 * 1024 * 1024),
        )(pltpu.with_memory_space_constraint(local_l.reshape(rows // 8, 8, cols), pltpu.HBM))

    return jax.shard_map(body, mesh=mesh, in_specs=(spec,), out_specs=spec, check_vma=False)
```
